512 devices in a mesh: groups: 2 (over y), gx: 128 (over z, x), gy: 2 (over core).
Axes of the slice: x: 8, y: 2, z: 16, core: 2. Of those that a mesh axis runs over, the one named last changes fastest.
The devices are a block of a 8x8x16 slice.
Arguments:
- forcing: float32 [2, 8192, 3072], P(None, ('groups', 'gx'), 'gy'), parts along dimension 1, may hold values from -6 to 6
- viscosity: float32 [8192, 3072], P(('groups', 'gx'), 'gy'), parts along dimension 0, may hold values from 0.25 to 8
- mass: float32 [8192, 3072], P(('groups', 'gx'), 'gy'), parts along dimension 0, may hold values from 0.5 to 2
- coriolis: float32 [3072], P('gy'), may hold values from 0.1 to 0.45
- land: int32 [4096, 3072], P('gx', 'gy'), may hold values 0 or 1
- ice_tiles: int32 [64, 24], P('groups'), parts along dimension 0, may hold values 0 or 1
Outputs:
- velocity: float32 [2, 8192, 3072], P(None, ('groups', 'gx'), 'gy'), parts along dimension 1
The draws below stay inside these ranges and needn't reach their ends.
There are 2 independent parts, one for each index of `groups`. The reference program is written for one: setup_inputs(seed, part) draws one part's arguments, and reference() takes and returns one part's arrays. A program takes and returns all parts, laid end to end along the dimension named above; an argument that names none is the same for every part. Nothing has to cross between parts.
Inputs may be any that keep to these rules, and one draw needn't show every extreme that they name: 1 marks land. `ice_tiles`: 1 marks a tile with ice.
All inputs are finite; a program needn't handle non-finite values. No bound on the sum of `land` on one device may be relied on, other than what follows from the above.
Results may differ from the reference program's by a relative error of at most 0.00005.
Values sent between devices are 32-bit elements; how exact they have to be, the bound alone decides.
No kernel may reach another device: no remote copies, remote signals or barrier semaphores. Data moves between devices by JAX's collectives and lax.ppermute only.
A program may use at most 64 MiB of HBM per device.

```python
import math
import jax
import jax.numpy as jnp

TILE = 128
LEVELS = 4
PRE = 1
POST = 1
CSWEEPS = 3
CYCLES = 1
NX = 4096
NY = 3072


def touch_ends(array, own_key, smallest, top_value):
    place = [jax.random.randint(jax.random.fold_in(own_key, axis), (), 0, length) for axis, length in enumerate(array.shape)]
    widest = array.shape.index(max(array.shape))
    beside = place[:widest] + [(place[widest] + 1) % array.shape[widest]] + place[widest + 1:]
    return array.at[tuple(place)].set(smallest).at[tuple(beside)].set(top_value)


def level_of(key, shape, cuts, low, largest):
    gain, own = 1.0, jax.random.fold_in(key, 6)
    for dim, blocks in cuts:
        heights = jnp.exp(jax.random.uniform(jax.random.fold_in(own, dim), (blocks,), jnp.float32, low / len(cuts), largest / len(cuts)))
        gain = gain * jnp.repeat(heights, shape[dim] // blocks).reshape([-1 if axis == dim else 1 for axis in range(len(shape))])
    return gain


def noise(own_key, extent, width, limit, cuts=(), kind=jnp.bfloat16):
    values = width * jax.random.normal(own_key, extent, jnp.float32)
    if cuts:
        values = values * level_of(own_key, extent, cuts, -0.22, 0.18)
    return jnp.clip(values, -limit, limit).astype(kind)


def setup_inputs(seed: int = 0, part: int = 0) -> dict:
    arg_keys = jax.random.split(jax.random.key(seed), 7)
    own_keys = jax.random.split(jax.random.fold_in(arg_keys[6], part), 7)
    forcing = noise(own_keys[0], (2, NX, NY), 1.0, 6.0, ((1, 128), (2, 2)), jnp.float32)
    viscosity = jnp.clip(jnp.exp(math.log(8.0) - 3.465736 * jax.random.uniform(own_keys[1], (NX, NY), jnp.float32) ** level_of(own_keys[1], (NX, NY), ((0, 128), (1, 2)), -0.2, 0.2)), 0.25, 8.0)
    mass = jnp.clip(jnp.exp(math.log(2.0) - 1.3862944 * jax.random.uniform(own_keys[2], (NX, NY), jnp.float32) ** level_of(own_keys[2], (NX, NY), ((0, 128), (1, 2)), -0.2, 0.2)), 0.5, 2.0)
    coriolis = jnp.clip(0.1 + 0.35 * jax.random.uniform(arg_keys[3], (NY,), jnp.float32) ** level_of(arg_keys[3], (NY,), ((0, 2),), -0.2, 0.2), 0.1, 0.45)
    land = touch_ends((jax.random.randint(arg_keys[4], (NX, NY), 0, 6) < 1).astype(jnp.int32), jax.random.fold_in(arg_keys[4], 1), 0, 1)
    ice_tiles = touch_ends((jax.random.randint(own_keys[5], (NX // TILE, NY // TILE), 0, 4) < 3).astype(jnp.int32), jax.random.fold_in(own_keys[5], 1), 0, 1)
    return {"forcing": forcing, "viscosity": viscosity, "mass": mass, "coriolis": coriolis, "land": land, "ice_tiles": ice_tiles}


relax_weight = 0.8
land_mass = 4.0


def pair_mean(values):
    return 0.25 * (values[..., 0::2, 0::2] + values[..., 1::2, 0::2] + values[..., 0::2, 1::2] + values[..., 1::2, 1::2])


def build_levels(visc_eff, mass_eff, coriolis):
    east = 0.5 * (visc_eff + jnp.roll(visc_eff, -1, 0))
    west = jnp.roll(east, 1, 0)
    inner = 0.5 * (visc_eff[:, :-1] + visc_eff[:, 1:])
    folded = 0.5 * (visc_eff[:, -1] + visc_eff[::-1, -1])
    north = jnp.concatenate([inner, folded[:, None]], 1)
    south = jnp.concatenate([visc_eff[:, :1], north[:, :-1]], 1)
    mass_now = mass_eff
    rotation = coriolis
    levels = []
    for level in range(LEVELS):
        if level > 0:
            east = 0.25 * (east[1::2, 0::2] + east[1::2, 1::2])
            west = 0.25 * (west[0::2, 0::2] + west[0::2, 1::2])
            north = 0.25 * (north[0::2, 1::2] + north[1::2, 1::2])
            south = 0.25 * (south[0::2, 0::2] + south[1::2, 0::2])
            mass_now = pair_mean(mass_now)
            rotation = 0.5 * (rotation[0::2] + rotation[1::2])
        diagonal = mass_now + east + west + north + south
        levels.append((east, west, north, south, diagonal, rotation))
    return levels


def apply_operator(field, stencil):
    east, west, north, south, diagonal, rotation = stencil
    east_nb = jnp.roll(field, -1, 1)
    west_nb = jnp.roll(field, 1, 1)
    north_nb = jnp.concatenate([field[:, :, 1:], -field[:, ::-1, -1:]], 2)
    south_nb = jnp.concatenate([jnp.zeros_like(field[:, :, :1]), field[:, :, :-1]], 2)
    turned = jnp.stack([-field[1], field[0]]) * rotation
    return diagonal * field - east * east_nb - west * west_nb - north * north_nb - south * south_nb + turned


def smooth(field, source, stencil, count, from_zero):
    for sweep in range(count):
        if from_zero and sweep == 0:
            field = relax_weight * source / stencil[4]
        else:
            field = field + relax_weight * (source - apply_operator(field, stencil)) / stencil[4]
    return field


def vcycle(level, source, field, from_zero, levels):
    stencil = levels[level]
    if level == LEVELS - 1:
        return smooth(field, source, stencil, CSWEEPS, True)
    field = smooth(field, source, stencil, PRE, from_zero)
    residue = source - apply_operator(field, stencil)
    coarse = vcycle(level + 1, pair_mean(residue), None, True, levels)
    field = field + jnp.repeat(jnp.repeat(coarse, 2, 1), 2, 2)
    return smooth(field, source, stencil, POST, False)


def reference(forcing, viscosity, mass, coriolis, land, ice_tiles):
    land_float = land.astype(jnp.float32)
    ocean = 1.0 - land_float
    ice = jnp.repeat(jnp.repeat(ice_tiles.astype(jnp.float32), TILE, 0), TILE, 1)
    visc_eff = viscosity * ice * ocean
    mass_eff = mass * ocean + land_mass * land_float
    source = forcing * ocean
    levels = build_levels(visc_eff, mass_eff, coriolis)
    field = None
    for cycle in range(CYCLES):
        field = vcycle(0, source, field, cycle == 0, levels)
    return field
```

```python
import functools

import jax
import jax.numpy as jnp
from jax import lax
from jax.experimental import pallas as pl
from jax.experimental.pallas import tpu as pltpu
from jax.sharding import PartitionSpec as P

TILE = 128
LEVELS = 4
LANES = 128
SEGS = 4
HALF = LANES // 2
GROUP = 8

relax_weight = 0.8
land_mass = 4.0
f32 = jnp.float32
exact = lax.Precision.HIGHEST


def iota(shape, axis):
    return lax.broadcasted_iota(jnp.int32, shape, axis)


def prepare_kernel(
    ice_ref, forcing_ref, visc_ref, mass_ref, land_ref, cor_ref, packed_ref, edge_ref, mirror_ref, wall_ref
):
    width = visc_ref.shape[0]
    tiles = visc_ref.shape[1] // LANES
    tps = tiles // SEGS
    tile_x = lax.axis_index("gx") * width // TILE
    tile_y = lax.axis_index("gy") * tiles
    lane = iota((8, LANES), 1)
    for i in range(width // 8):
        rows = slice(8 * i, 8 * i + 8)
        ends = []
        for t in range(tiles):
            s, k = divmod(t, tps)
            cols = slice(t * LANES, (t + 1) * LANES)
            ice = ice_ref[tile_x, tile_y + t].astype(f32)
            land = land_ref[rows, cols].astype(f32)
            ocean = 1.0 - land
            values = (
                visc_ref[rows, cols] * ice * ocean,
                mass_ref[rows, cols] * ocean + land_mass * land,
                forcing_ref[0, rows, cols] * ocean,
                forcing_ref[1, rows, cols] * ocean,
            )
            for a, value in enumerate(values):
                tile = 8 * i * 2 * tps + (a // 2) * tps + k
                start = tile * 8 + (a % 2) * SEGS + s
                packed_ref[pl.ds(start, 8, stride=2 * tps * 8), :] = value
            if t in (0, tiles - 1):
                ends.append(values)
        for a in range(4):
            start = 8 * i * 4 + a
            edge_ref[pl.ds(start, 8, stride=4), :] = jnp.where(lane < HALF, ends[0][a], ends[1][a])
            if a == 0:
                wall = jnp.broadcast_to(ends[0][0][:, :1], (8, LANES))
            else:
                wall = jnp.full((8, LANES), 1.0 if a == 1 else 0.0, f32)
            wall_ref[pl.ds(start, 8, stride=4), :] = wall
    main = 4 * width
    first, last = cor_ref[0:1, :], cor_ref[tiles - 1 : tiles, :]
    edge_ref[main : main + 8, :] = jnp.broadcast_to(
        jnp.where(lane[:1] < HALF, first, last), (8, LANES)
    )
    wall_ref[main : main + 8, :] = jnp.zeros((8, LANES), f32)
    flip = (iota((LANES, LANES), 0) + iota((LANES, LANES), 1) == LANES - 1).astype(f32)
    row, col = iota((main, main), 0), iota((main, main), 1)
    sign = jnp.where(row & 2 == 0, 1.0, -1.0)
    turn = jnp.where((row & 3 == col & 3) & ((row >> 2) + (col >> 2) == width - 1), sign, 0.0)
    turned = jnp.dot(turn, edge_ref[0:main, :], precision=exact, preferred_element_type=f32)
    mirror_ref[0:main, :] = jnp.dot(turned, flip, precision=exact, preferred_element_type=f32)
    mirror_ref[main : main + 8, :] = jnp.dot(
        edge_ref[main : main + 8, :], flip, precision=exact, preferred_element_type=f32
    )


def solve_kernel(own_ref, left_ref, right_ref, cor_ref, out_ref, *scratch):
    packed, sems, flat = scratch[:3]
    store = scratch[3:]
    size = own_ref.shape[0]
    width = out_ref.shape[1]
    tiles = cor_ref.shape[0]
    tps = tiles // SEGS
    span = (tps + 1) * LANES
    shape = (8, span)
    copies = [
        pltpu.make_async_copy(ref, packed.at[pl.ds(n * size, size), :], sems.at[n])
        for n, ref in enumerate((left_ref, own_ref, right_ref))
    ]
    for copy in copies:
        copy.start()

    sub1, lane1 = iota((8, LANES), 0), iota((8, LANES), 1)
    low = sub1 < SEGS
    at_north = (sub1 & (SEGS - 1) == SEGS - 1) & (lane1 < HALF)
    at_south = (sub1 & (SEGS - 1) == 0) & (lane1 >= HALF)
    outer = at_north | at_south
    lane = iota(shape, 1)
    bottom = lax.axis_index("gy") == 0
    wall = (iota(shape, 0) & (SEGS - 1) == 0) & (lane >= tps * LANES + HALF) & bottom
    weight = jnp.where(wall, 0.0, relax_weight)

    def roll(value, shift):
        return pltpu.roll(value, shift % span, 1)

    def other(value):
        return pltpu.roll(value, SEGS, 0)

    def pair(value, step, odd):
        return value + jnp.where(odd, roll(value, step), roll(value, -step))

    def with_halo(parts, outside):
        inside = jnp.where(lane1 < HALF, pltpu.roll(parts[0], 7, 0), pltpu.roll(parts[-1], 1, 0))
        return parts + [jnp.where(outer, outside, inside)]

    for copy in copies:
        copy.wait()

    names = ("visc", "north", "mass", "right", "east", "scale", "field", "done")
    levels = []
    place = 0
    for level in range(LEVELS):
        levels.append(dict(zip(names, store[place : place + len(names)])))
        place += len(names)

    line = packed[pl.ds(size + size - 8, 8), :][:1]
    parts = [cor_ref[pl.ds(k, SEGS, stride=tps), :] for k in range(tps)]
    parts = [jnp.concatenate([part, -part], 0) for part in parts]
    line8 = jnp.where(low, jnp.broadcast_to(line, (8, LANES)), -jnp.broadcast_to(line, (8, LANES)))
    rotation = jnp.concatenate(with_halo(parts, line8), 1)

    top = levels[0]

    def unpack(group, carry):
        for j in range(GROUP):
            x = group * GROUP + j
            third = group * GROUP // width
            xi = x - third * width
            base = pl.multiple_of(third * size + xi * (2 * tps * 8), 8)
            if j % 2 == 0:
                ext = packed[pl.ds(pl.multiple_of(third * size + width * 2 * tps * 8 + xi * 4, 8), 8), :]
            rows = [
                jnp.broadcast_to(ext[(j % 2) * 4 + a : (j % 2) * 4 + a + 1], (8, LANES)) for a in range(4)
            ]
            both = with_halo(
                [packed[pl.ds(base + 8 * k, 8), :] for k in range(tps)], jnp.where(low, rows[0], rows[1])
            )
            turned = [other(part) for part in both]
            visc = jnp.concatenate([jnp.where(low, a, b) for a, b in zip(both, turned)], 1)
            mass = jnp.concatenate([jnp.where(low, b, a) for a, b in zip(both, turned)], 1)
            right = jnp.concatenate(
                with_halo(
                    [packed[pl.ds(base + 8 * (tps + k), 8), :] for k in range(tps)],
                    jnp.where(low, rows[2], rows[3]),
                ),
                1,
            )
            top["visc"][x + 1] = visc
            top["mass"][x] = mass
            top["right"][x] = right
            top["north"][x] = 0.5 * (visc + roll(visc, -1))
        return carry

    lax.fori_loop(0, 3 * width // GROUP, unpack, 0)

    def loop(count, body):
        group = GROUP
        while count % group:
            group //= 2
        if count == group:
            body(0, group)
        else:
            lax.fori_loop(0, count // group, lambda g, c: (body(g * group, group), c)[1], 0)

    rotations = []
    for level in range(LEVELS):
        now = levels[level]
        step = 1 << level
        count = 3 * width >> level
        rotations.append(rotation)

        def coefficients(first, group, now=now, step=step, level=level):
            if level == 0:
                visc = [now["visc"][first + j] for j in range(group + 2)]
                east = [0.5 * (visc[j] + visc[j + 1]) for j in range(group + 1)]
                for j in range(group):
                    now["east"][first + j + 1] = east[j + 1]
            else:
                east = [now["east"][first + j] for j in range(group + 1)]
            for j in range(group):
                x = first + j
                north = now["north"][x]
                diag = now["mass"][x] + east[j + 1] + east[j] + north + roll(north, step)
                scale = weight / diag
                now["scale"][x] = scale
                now["field"][x + 1] = scale * now["right"][x]

        loop(count, coefficients)
        if level == LEVELS - 1:
            break
        coarse = levels[level + 1]
        odd = lane & step != 0

        def restrict(first, group, now=now, coarse=coarse, step=step, odd=odd, rotation=rotation):
            first = first * 2
            field = [now["field"][first + j] for j in range(2 * group + 2)]
            east = [now["east"][first + j] for j in range(2 * group + 1)]
            rest = []
            for j in range(2 * group):
                x = first + j
                north = now["north"][x]
                w = field[j + 1]
                rest.append(
                    (1.0 - relax_weight) * now["right"][x]
                    + east[j + 1] * field[j + 2]
                    + east[j] * field[j]
                    + north * roll(w, -step)
                    + roll(north * w, step)
                    + rotation * other(w)
                )
            for j in range(group):
                half = first // 2 + j
                x = first + 2 * j
                coarse["right"][half] = 0.25 * pair(rest[2 * j] + rest[2 * j + 1], step, odd)
                coarse["east"][half + 1] = 0.25 * pair(east[2 * j + 2], step, odd)
                coarse["mass"][half] = 0.25 * pair(now["mass"][x] + now["mass"][x + 1], step, odd)
                north = now["north"][x] + now["north"][x + 1]
                coarse["north"][half] = 0.25 * jnp.where(odd, north, roll(north, -step))

        loop(count // 2, restrict)
        rotation = 0.5 * pair(rotation, step, odd)

    def sweep(level, first, group, value, target, offset):
        now = levels[level]
        step = 1 << level
        field = [value(first + j - 1) for j in range(group + 2)]
        east = [now["east"][first + j] for j in range(group + 1)]
        for j in range(group):
            x = first + j
            north = now["north"][x]
            w = field[j + 1]
            around = (
                now["right"][x]
                + east[j + 1] * field[j + 2]
                + east[j] * field[j]
                + north * roll(w, -step)
                + roll(north * w, step)
                + rotations[level] * other(w)
            )
            result = (1.0 - relax_weight) * w + now["scale"][x] * around
            if target is None:
                for k in range(tps):
                    row = pl.multiple_of(((x - offset) * tps + k) * 8, 8)
                    flat[pl.ds(row, 8), :] = result[:, k * LANES : (k + 1) * LANES]
            else:
                target[x + 1] = result

    last = levels[-1]
    own = width >> (LEVELS - 1)
    sweep(LEVELS - 1, own - 2, own + 4, lambda x: last["field"][x + 1], last["done"], 0)
    sweep(LEVELS - 1, own - 1, own + 2, lambda x: last["done"][x + 1], last["field"], 0)
    solved = last["field"]
    for level in reversed(range(LEVELS - 1)):
        now = levels[level]
        own = width >> level

        def value(x, now=now, solved=solved):
            return now["field"][x + 1] + solved[lax.div(x, 2) + 1]

        if level > 0:
            start, count, target = own - 1, own + 2, now["done"]
        else:
            start, count, target = own, own, None
        loop(
            count,
            lambda first, group, level=level, start=start, value=value, target=target: sweep(
                level, start + first, group, value, target, start
            ),
        )
        solved = now["done"]

    for c in range(2):
        for i in range(width // 8):
            for t in range(tiles):
                s, k = divmod(t, tps)
                row = (8 * i * tps + k) * 8 + c * SEGS + s
                out_ref[c, 8 * i : 8 * i + 8, t * LANES : (t + 1) * LANES] = flat[
                    pl.ds(row, 8, stride=tps * 8), :
                ]


def local(forcing, viscosity, mass, coriolis, land, ice_tiles):
    width, height = viscosity.shape
    tiles = height // LANES
    tps = tiles // SEGS
    main = width * 2 * tps * 8
    outside = 4 * width + 8
    gx, gy = lax.axis_size("gx"), lax.axis_size("gy")
    is_top = lax.axis_index("gy") == gy - 1
    lines = coriolis.reshape(tiles, LANES)
    vmem = pl.BlockSpec(memory_space=pltpu.VMEM)
    anywhere = pl.BlockSpec(memory_space=pl.ANY)

    packed, edge, mirror, wall = pl.pallas_call(
        prepare_kernel,
        out_shape=(
            jax.ShapeDtypeStruct((main + outside, LANES), f32),
            jax.ShapeDtypeStruct((outside, LANES), f32),
            jax.ShapeDtypeStruct((outside, LANES), f32),
            jax.ShapeDtypeStruct((outside, LANES), f32),
        ),
        in_specs=[pl.BlockSpec(memory_space=pltpu.SMEM)] + [vmem] * 5,
        out_specs=(vmem,) * 4,
    )(ice_tiles, forcing, viscosity, mass, land, lines)

    top = gy - 1
    swap = lax.ppermute(edge, "gy", [(i, gy - 1 - i) for i in range(gy)])
    folded = lax.ppermute(
        mirror, ("gx", "gy"), [(i * gy + top, (gx - 1 - i) * gy + top) for i in range(gx)]
    )
    north = iota((outside, LANES), 1) < HALF
    beyond = jnp.where(north, jnp.where(is_top, folded, swap), jnp.where(is_top, swap, wall))
    packed = lax.dynamic_update_slice(packed, beyond, (main, 0))
    up = [(i, (i + 1) % gx) for i in range(gx)]
    from_left = lax.ppermute(packed, "gx", up)
    from_right = lax.ppermute(packed, "gx", [(b, a) for a, b in up])

    store = []
    for level in range(LEVELS):
        columns = (3 * width >> level) + 2
        store += [pltpu.VMEM((columns, 8, (tps + 1) * LANES), f32)] * 8
    return pl.pallas_call(
        solve_kernel,
        out_shape=jax.ShapeDtypeStruct((2, width, height), f32),
        in_specs=[anywhere] * 3 + [vmem],
        out_specs=vmem,
        scratch_shapes=[
            pltpu.VMEM((3 * (main + outside), LANES), f32),
            pltpu.SemaphoreType.DMA((3,)),
            pltpu.VMEM((width * tps * 8, LANES), f32),
        ]
        + store,
        compiler_params=pltpu.CompilerParams(vmem_limit_bytes=48 * 1024 * 1024),
    )(packed, from_left, from_right, lines)


def solution(mesh):
    return jax.shard_map(
        local,
        mesh=mesh,
        in_specs=(
            P(None, ("groups", "gx"), "gy"),
            P(("groups", "gx"), "gy"),
            P(("groups", "gx"), "gy"),
            P("gy"),
            P("gx", "gy"),
            P("groups", None),
        ),
        out_specs=P(None, ("groups", "gx"), "gy"),
        check_vma=False,
    )
```

```python
import functools

import jax
import jax.numpy as jnp
from jax import lax
from jax.experimental import pallas as pl
from jax.experimental.pallas import tpu as pltpu
from jax.sharding import PartitionSpec as P

TILE = 128
LEVELS = 4
LANES = 128
SEGS = 4
HALF = LANES // 2
GROUP = 8

relax_weight = 0.8
land_mass = 4.0
f32 = jnp.float32
exact = lax.Precision.HIGHEST


FINE = 6
SPLIT = 2


def iota(shape, axis):
    return lax.broadcasted_iota(jnp.int32, shape, axis)


def prepare_kernel(
    ice_ref, forcing_ref, visc_ref, mass_ref, land_ref, cor_ref,
    packed_ref, lowest_ref, highest_ref, edge_ref, mirror_ref, wall_ref,
):
    width = visc_ref.shape[0]
    tiles = visc_ref.shape[1] // LANES
    tps = tiles // SEGS
    tile_x = lax.axis_index("gx") * width // TILE
    tile_y = lax.axis_index("gy") * tiles
    lane = iota((8, LANES), 1)
    for i in range(width // 8):
        rows = slice(8 * i, 8 * i + 8)
        ends = []
        for t in range(tiles):
            s, k = divmod(t, tps)
            cols = slice(t * LANES, (t + 1) * LANES)
            ice = ice_ref[tile_y + t, tile_x].astype(f32)
            land = land_ref[rows, cols].astype(f32)
            ocean = 1.0 - land
            values = (
                visc_ref[rows, cols] * ice * ocean,
                mass_ref[rows, cols] * ocean + land_mass * land,
                forcing_ref[0, rows, cols] * ocean,
                forcing_ref[1, rows, cols] * ocean,
            )
            for a, value in enumerate(values):
                tile = 8 * i * 2 * tps + (a // 2) * tps + k
                start = tile * 8 + (a % 2) * SEGS + s
                packed_ref[pl.ds(start, 8, stride=2 * tps * 8), :] = value
            if t in (0, tiles - 1):
                ends.append(values)
        for a in range(4):
            start = 8 * i * 4 + a
            edge_ref[pl.ds(start, 8, stride=4), :] = jnp.where(lane < HALF, ends[0][a], ends[1][a])
            if a == 0:
                wall = jnp.broadcast_to(ends[0][0][:, :1], (8, LANES))
            else:
                wall = jnp.full((8, LANES), 1.0 if a == 1 else 0.0, f32)
            wall_ref[pl.ds(start, 8, stride=4), :] = wall
    side = FINE * 2 * tps * 8
    lowest_ref[...] = packed_ref[0:side, :]
    highest_ref[...] = packed_ref[width * 2 * tps * 8 - side : width * 2 * tps * 8, :]
    main = 4 * width
    first, last = cor_ref[0:1, :], cor_ref[tiles - 1 : tiles, :]
    edge_ref[main : main + 8, :] = jnp.broadcast_to(
        jnp.where(lane[:1] < HALF, first, last), (8, LANES)
    )
    wall_ref[main : main + 8, :] = jnp.zeros((8, LANES), f32)
    flip = (iota((LANES, LANES), 0) + iota((LANES, LANES), 1) == LANES - 1).astype(f32)
    row, col = iota((main, main), 0), iota((main, main), 1)
    sign = jnp.where(row & 2 == 0, 1.0, -1.0)
    turn = jnp.where((row & 3 == col & 3) & ((row >> 2) + (col >> 2) == width - 1), sign, 0.0)
    turned = jnp.dot(turn, edge_ref[0:main, :], precision=exact, preferred_element_type=f32)
    mirror_ref[0:main, :] = jnp.dot(turned, flip, precision=exact, preferred_element_type=f32)
    mirror_ref[main : main + 8, :] = jnp.dot(
        edge_ref[main : main + 8, :], flip, precision=exact, preferred_element_type=f32
    )


def edge_kernel(swap_ref, folded_ref, wall_ref, lowest_ref, highest_ref, ext_ref, low_ref, high_ref):
    is_top = lax.axis_index("gy") == lax.axis_size("gy") - 1
    north = iota(swap_ref.shape, 1) < HALF
    swap = swap_ref[...]
    beyond = jnp.where(
        north, jnp.where(is_top, folded_ref[...], swap), jnp.where(is_top, swap, wall_ref[...])
    )
    ext_ref[...] = beyond
    side = lowest_ref.shape[0]
    main = swap_ref.shape[0] - 8
    low_ref[0:side, :] = lowest_ref[...]
    low_ref[side : side + 4 * FINE, :] = ext_ref[0 : 4 * FINE, :]
    high_ref[0:side, :] = highest_ref[...]
    high_ref[side : side + 4 * FINE, :] = ext_ref[main - 4 * FINE : main, :]


class Shifts:
    def __init__(self, tps):
        self.tps = tps
        self.span = (tps + 1) * LANES
        self.shape = (8, self.span)
        self.lane = iota(self.shape, 1)
        lane = iota((8, LANES), 1)
        row = iota((8, LANES), 0) & (SEGS - 1)
        self.first_half = lane < HALF
        self.low = iota((8, LANES), 0) < SEGS
        self.outer = ((row == SEGS - 1) & (lane < HALF)) | ((row == 0) & (lane >= HALF))
        bottom = lax.axis_index("gy") == 0
        wall = (iota(self.shape, 0) & (SEGS - 1) == 0) & (self.lane >= tps * LANES + HALF) & bottom
        self.weight = jnp.where(wall, 0.0, relax_weight)

    def roll(self, value, shift):
        return pltpu.roll(value, shift % self.span, 1)

    def odd(self, step):
        return self.lane & step != 0

    def pair(self, value, step):
        return value + jnp.where(self.odd(step), self.roll(value, step), self.roll(value, -step))

    def with_halo(self, parts, outside):
        inside = jnp.where(self.first_half, pltpu.roll(parts[0], 7, 0), pltpu.roll(parts[-1], 1, 0))
        return parts + [jnp.where(self.outer, outside, inside)]

    def rotations(self, cor_ref, line):
        parts = [cor_ref[pl.ds(k, SEGS, stride=self.tps), :] for k in range(self.tps)]
        parts = [jnp.concatenate([part, -part], 0) for part in parts]
        line = jnp.broadcast_to(line, (8, LANES))
        rotation = jnp.concatenate(self.with_halo(parts, jnp.where(self.low, line, -line)), 1)
        result = []
        for level in range(LEVELS):
            result.append(rotation)
            rotation = 0.5 * self.pair(rotation, 1 << level)
        return result

    def around(self, now, x, field, east, rotation, step):
        north = now["north"][x]
        west_nb, w, east_nb = field
        return (
            east[1] * east_nb
            + east[0] * west_nb
            + north * self.roll(w, -step)
            + self.roll(north * w, step)
            + rotation * other(w)
        )

    def coefficients(self, now, first, group, step):
        east = [now["east"][first + j - 1] for j in range(group + 1)]
        for j in range(group):
            x = first + j
            north = now["north"][x]
            diag = now["mass"][x] + east[j + 1] + east[j] + north + self.roll(north, step)
            scale = self.weight / diag
            now["scale"][x] = scale
            now["field"][x] = scale * now["right"][x]

    def coarse_east(self, now, fine, target, step):
        target[...] = 0.25 * self.pair(now["east"][fine + 1], step)

    def coarse_sums(self, now, coarse, fine, place, step):
        north = now["north"][fine] + now["north"][fine + 1]
        coarse["north"][place] = 0.25 * jnp.where(self.odd(step), north, self.roll(north, -step))
        coarse["mass"][place] = 0.25 * self.pair(now["mass"][fine] + now["mass"][fine + 1], step)

    def restrict(self, now, coarse, fine, place, group, rotation, step):
        field = [now["field"][fine + j - 1] for j in range(2 * group + 2)]
        east = [now["east"][fine + j - 1] for j in range(2 * group + 1)]
        rest = [
            (1.0 - relax_weight) * now["right"][fine + j]
            + self.around(now, fine + j, field[j : j + 3], east[j : j + 2], rotation, step)
            for j in range(2 * group)
        ]
        for j in range(group):
            coarse["right"][place + j] = 0.25 * self.pair(rest[2 * j] + rest[2 * j + 1], step)

    def sweep(self, now, first, group, value, rotation, step, put):
        field = [value(first + j - 1) for j in range(group + 2)]
        east = [now["east"][first + j - 1] for j in range(group + 1)]
        for j in range(group):
            x = first + j
            near = now["right"][x] + self.around(
                now, x, field[j : j + 3], east[j : j + 2], rotation, step
            )
            put(x, (1.0 - relax_weight) * field[j + 1] + now["scale"][x] * near)


def other(value):
    return pltpu.roll(value, SEGS, 0)


def loop(start, count, body, group=GROUP):
    whole, rest = divmod(count, group)
    if whole == 1:
        body(start, group)
    elif whole:
        lax.fori_loop(0, whole, lambda g, c: (body(start + g * group, group), c)[1], 0)
    if rest:
        body(start + whole * group, rest)


FIRST = ("north", "east", "scale", "right", "field")
COARSE = ("right", "east", "north", "mass")


def first_kernel(own_ref, ext_ref, left_ref, right_ref, cor_ref, *refs):
    width = (ext_ref.shape[0] - 8) // 4
    tps = cor_ref.shape[0] // SEGS
    move = Shifts(tps)
    levels = [dict(zip(FIRST, refs[5 * n : 5 * n + 5])) for n in range(SPLIT)]
    sent_ref, rot_ref = refs[5 * SPLIT : 5 * SPLIT + 2]
    rest = list(refs[5 * SPLIT + 2 :])
    visc = rest.pop(0)
    for level in levels:
        level["mass"] = rest.pop(0)
    bottom = dict(zip(COARSE, rest))
    levels.append(bottom)
    main = ext_ref.shape[0] - 8
    rotations = move.rotations(cor_ref, ext_ref[main : main + 1, :])
    for level in range(LEVELS):
        rot_ref[level] = rotations[level]
    top = levels[0]

    def unpack(ref, base, ext, index, x):
        rows = [jnp.broadcast_to(ext[4 * index + a : 4 * index + a + 1], (8, LANES)) for a in range(4)]
        both = move.with_halo(
            [ref[pl.ds(base + 8 * k, 8), :] for k in range(tps)], jnp.where(move.low, rows[0], rows[1])
        )
        turned = [other(part) for part in both]
        value = jnp.concatenate([jnp.where(move.low, a, b) for a, b in zip(both, turned)], 1)
        visc[x] = value
        top["mass"][x] = jnp.concatenate([jnp.where(move.low, b, a) for a, b in zip(both, turned)], 1)
        top["right"][x] = jnp.concatenate(
            move.with_halo(
                [ref[pl.ds(base + 8 * (tps + k), 8), :] for k in range(tps)],
                jnp.where(move.low, rows[2], rows[3]),
            ),
            1,
        )
        top["north"][x] = 0.5 * (value + move.roll(value, -1))

    each = 2 * tps * 8
    for ref, start in ((left_ref, 0), (right_ref, FINE + width)):
        for j in range(0, FINE, 2):
            ext = ref[FINE * each + 4 * j : FINE * each + 4 * j + 8, :]
            for index in range(2):
                unpack(ref, (j + index) * each, ext, index, start + j + index)

    def own(first, group):
        for j in range(0, group, 2):
            x = first + j
            ext = ext_ref[pl.ds(pl.multiple_of(4 * x, 8), 8), :]
            for index in range(2):
                unpack(own_ref, pl.multiple_of((x + index) * each, 8), ext, index, FINE + x + index)

    loop(0, width, own)
    columns = 2 * FINE + width

    def faces(first, group):
        value = [visc[first + j] for j in range(group + 1)]
        for j in range(group):
            top["east"][first + j] = 0.5 * (value[j] + value[j + 1])

    loop(0, columns - 1, faces, 11)
    loop(1, columns - 2, lambda x, n: move.coefficients(top, x, n, 1), 7)
    half = columns // 2
    level1 = levels[1]

    def east1(first, group):
        for j in range(group):
            level1["east"][first + j] = 0.25 * move.pair(top["east"][2 * (first + j) + 1], 1)

    def sums1(first, group):
        for j in range(group):
            move.coarse_sums(top, level1, 2 * (first + j), first + j, 1)

    loop(0, half - 1, east1, 7)
    loop(0, half, sums1, 11)
    loop(1, half - 2, lambda x, n: move.restrict(top, level1, 2 * x, x, n, rotations[0], 1), 5)
    loop(1, half - 2, lambda x, n: move.coefficients(level1, x, n, 2), 10)
    count = width >> SPLIT
    skip = FINE // 2
    for k in range(count):
        bottom["east"][k] = 0.25 * move.pair(level1["east"][skip + 2 * k + 1], 2)
        move.coarse_sums(level1, bottom, skip + 2 * k, k, 2)
    move.restrict(level1, bottom, skip, 0, count, rotations[1], 2)
    bit0, bit1 = move.odd(1), move.odd(2)
    for k in range(count):
        parts = [bottom[name][k] for name in COARSE]
        sent_ref[k] = jnp.where(
            bit1, jnp.where(bit0, parts[3], parts[2]), jnp.where(bit0, parts[1], parts[0])
        )


SECOND = ("right", "east", "north", "mass", "scale", "field")


def second_kernel(own_ref, left_ref, right_ref, rot_ref, *refs):
    out_refs = 5 * SPLIT
    levels = [dict(zip(FIRST, refs[5 * n : 5 * n + 5])) for n in range(SPLIT)]
    out_ref = refs[out_refs]
    rest = list(refs[out_refs + 1 :])
    flat = rest.pop(0)
    for _ in range(SPLIT, LEVELS):
        levels.append(dict(zip(SECOND, rest[:6])))
        rest = rest[6:]
    done = rest
    width = out_ref.shape[1]
    tps = out_ref.shape[2] // LANES // SEGS
    tiles = tps * SEGS
    move = Shifts(tps)
    rotations = [rot_ref[level] for level in range(LEVELS)]
    count = width >> SPLIT
    now = levels[SPLIT]
    bit0, bit1 = move.odd(1), move.odd(2)
    for start, ref in ((0, left_ref), (count, own_ref), (2 * count, right_ref)):
        for j in range(count):
            value = ref[j]
            evens = jnp.where(bit0, move.roll(value, 1), value)
            odds = jnp.where(bit0, value, move.roll(value, -1))
            for name, part, upper in zip(COARSE, (evens, odds, evens, odds), (0, 0, 1, 1)):
                if upper:
                    now[name][start + j] = jnp.where(bit1, part, move.roll(part, -2))
                else:
                    now[name][start + j] = jnp.where(bit1, move.roll(part, 2), part)
    total = 3 * count
    move.coefficients(now, 1, total - 2, 1 << SPLIT)
    for level in range(SPLIT, LEVELS - 1):
        now, coarse = levels[level], levels[level + 1]
        step = 1 << level
        half = total // 2
        for k in range(half - 1):
            coarse["east"][k] = 0.25 * move.pair(now["east"][2 * k + 1], step)
        for k in range(1, half - 1):
            move.coarse_sums(now, coarse, 2 * k, k, step)
        move.restrict(now, coarse, 2, 1, half - 2, rotations[level], step)
        total = half
        move.coefficients(coarse, 1, total - 2, 2 * step)

    def keep(target):
        def put(x, value):
            target[x] = value

        return put

    level = LEVELS - 1
    last, solved = levels[level], done.pop(0)
    own = width >> level
    move.sweep(
        last, own - 2, own + 4, lambda x: last["field"][x], rotations[level], 1 << level, keep(solved)
    )
    move.sweep(
        last, own - 1, own + 2, lambda x: solved[x], rotations[level], 1 << level, keep(last["field"])
    )
    solved, before = last["field"], own
    for level in reversed(range(LEVELS - 1)):
        now = levels[level]
        own = width >> level
        here = own if level >= SPLIT else FINE >> level
        lead = 2 * before - here if level >= SPLIT - 1 else 0

        def value(x, now=now, solved=solved, lead=lead):
            return now["field"][x] + solved[lax.div(x + lead, 2)]

        if level:
            target = done.pop(0)
            loop(
                here - 1,
                own + 2,
                lambda x, n, now=now, value=value, level=level, target=target: move.sweep(
                    now, x, n, value, rotations[level], 1 << level, keep(target)
                ),
                10,
            )
            solved, before = target, here
        else:

            def put(x, result, here=here):
                for k in range(tps):
                    row = pl.multiple_of(((x - here) * tps + k) * 8, 8)
                    flat[pl.ds(row, 8), :] = result[:, k * LANES : (k + 1) * LANES]

            loop(
                here,
                own,
                lambda x, n, now=now, value=value: move.sweep(now, x, n, value, rotations[0], 1, put),
            )

    for c in range(2):
        for i in range(width // 8):
            for t in range(tiles):
                s, k = divmod(t, tps)
                row = (8 * i * tps + k) * 8 + c * SEGS + s
                out_ref[c, 8 * i : 8 * i + 8, t * LANES : (t + 1) * LANES] = flat[
                    pl.ds(row, 8, stride=tps * 8), :
                ]


def local(forcing, viscosity, mass, coriolis, land, ice_tiles):
    width, height = viscosity.shape
    tiles = height // LANES
    tps = tiles // SEGS
    each = 2 * tps * 8
    outside = 4 * width + 8
    gx, gy = lax.axis_size("gx"), lax.axis_size("gy")
    lines = coriolis.reshape(tiles, LANES)
    vmem = pl.BlockSpec(memory_space=pltpu.VMEM)

    def here(*shape):
        return pltpu.VMEM(shape, f32)

    def call(kernel, outs, args, scratch=(), first=None):
        return pl.pallas_call(
            kernel,
            out_shape=outs,
            in_specs=[first or vmem] + [vmem] * (len(args) - 1),
            out_specs=jax.tree.map(lambda _: vmem, outs),
            scratch_shapes=scratch,
            compiler_params=pltpu.CompilerParams(vmem_limit_bytes=24 * 1024 * 1024),
        )(*args)

    packed, lowest, highest, edge, mirror, wall = call(
        prepare_kernel,
        (
            here(width * each, LANES),
            here(FINE * each, LANES),
            here(FINE * each, LANES),
            here(outside, LANES),
            here(outside, LANES),
            here(outside, LANES),
        ),
        (ice_tiles.T, forcing, viscosity, mass, land, lines),
        first=pl.BlockSpec(memory_space=pltpu.SMEM),
    )
    top = gy - 1
    swap = lax.ppermute(edge, "gy", [(i, gy - 1 - i) for i in range(gy)])
    folded = lax.ppermute(
        mirror, ("gx", "gy"), [(i * gy + top, (gx - 1 - i) * gy + top) for i in range(gx)]
    )
    ext, low, high = call(
        edge_kernel,
        (here(outside, LANES),) + (here(FINE * (each + 4), LANES),) * 2,
        (swap, folded, wall, lowest, highest),
    )
    up = [(i, (i + 1) % gx) for i in range(gx)]
    down = [(b, a) for a, b in up]
    from_left = lax.ppermute(high, "gx", up)
    from_right = lax.ppermute(low, "gx", down)

    span = (tps + 1) * LANES
    columns = [(2 * FINE + width) >> level for level in range(SPLIT)]
    columns += [3 * width >> level for level in range(SPLIT, LEVELS)]
    count = width >> SPLIT

    def lines_of(number):
        return here(number, 8, span)

    state = call(
        first_kernel,
        tuple(lines_of(columns[level]) for level in range(SPLIT) for _ in FIRST)
        + (lines_of(count), lines_of(LEVELS)),
        (packed, ext, from_left, from_right, lines),
        scratch=[lines_of(columns[0])]
        + [lines_of(columns[level]) for level in range(SPLIT)]
        + [lines_of(count)] * len(COARSE),
    )
    *kept, sent, rotation = state
    from_left = lax.ppermute(sent, "gx", up)
    from_right = lax.ppermute(sent, "gx", down)
    return call(
        second_kernel,
        jax.ShapeDtypeStruct((2, width, height), f32),
        (sent, from_left, from_right, rotation, *kept),
        scratch=[pltpu.VMEM((width * tps * 8, LANES), f32)]
        + [lines_of(columns[level]) for level in range(SPLIT, LEVELS) for _ in SECOND]
        + [lines_of(columns[level]) for level in reversed(range(1, LEVELS))],
    )


def solution(mesh):
    return jax.shard_map(
        local,
        mesh=mesh,
        in_specs=(
            P(None, ("groups", "gx"), "gy"),
            P(("groups", "gx"), "gy"),
            P(("groups", "gx"), "gy"),
            P("gy"),
            P("gx", "gy"),
            P("groups", None),
        ),
        out_specs=P(None, ("groups", "gx"), "gy"),
        check_vma=False,
    )
```

```python
import jax
import jax.numpy as jnp
from jax import lax
from jax.experimental import pallas as pl
from jax.experimental.pallas import tpu as pltpu
from jax.sharding import PartitionSpec as P


TILE = 128
LEVELS = 4
LANES = 128
SEGS = 4
HALF = LANES // 2
GROUP = 8

relax_weight = 0.8
land_mass = 4.0
f32 = jnp.float32
exact = lax.Precision.HIGHEST


FINE = 6
SPLIT = 2


def iota(shape, axis):
    return lax.broadcasted_iota(jnp.int32, shape, axis)


def is_even():
    return lax.axis_index("gx") & 1 == 0


def prepare_kernel(*refs):
    sources, outs = refs[:6], refs[6:12]
    held, sems = refs[12:18], refs[18]
    copies = [pltpu.make_async_copy(a, b, sems.at[n]) for n, (a, b) in enumerate(zip(sources, held))]
    for copy in copies:
        copy.start()
    ice_ref, forcing_ref, visc_ref, mass_ref, land_ref, cor_ref = held
    packed_ref, lowest_ref, highest_ref, edge_ref, mirror_ref, wall_ref = outs
    width = visc_ref.shape[0]
    tiles = visc_ref.shape[1] // LANES
    tps = tiles // SEGS
    tile_x = lax.axis_index("gx") * width // TILE
    tile_y = lax.axis_index("gy") * tiles
    lane = iota((8, LANES), 1)
    for copy in copies:
        copy.wait()
    for i in range(width // 8):
        rows = slice(8 * i, 8 * i + 8)
        ends = []
        for t in range(tiles):
            s, k = divmod(t, tps)
            cols = slice(t * LANES, (t + 1) * LANES)
            ice = ice_ref[tile_y + t, tile_x].astype(f32)
            land = land_ref[rows, cols].astype(f32)
            ocean = 1.0 - land
            values = (
                visc_ref[rows, cols] * ice * ocean,
                mass_ref[rows, cols] * ocean + land_mass * land,
                forcing_ref[0, rows, cols] * ocean,
                forcing_ref[1, rows, cols] * ocean,
            )
            for a, value in enumerate(values):
                tile = 8 * i * 2 * tps + (a // 2) * tps + k
                start = tile * 8 + (a % 2) * SEGS + s
                packed_ref[pl.ds(start, 8, stride=2 * tps * 8), :] = value
            if t in (0, tiles - 1):
                ends.append(values)
        for a in range(4):
            start = 8 * i * 4 + a
            edge_ref[pl.ds(start, 8, stride=4), :] = jnp.where(lane < HALF, ends[0][a], ends[1][a])
            if a == 0:
                wall = jnp.broadcast_to(ends[0][0][:, :1], (8, LANES))
            else:
                wall = jnp.full((8, LANES), 1.0 if a == 1 else 0.0, f32)
            wall_ref[pl.ds(start, 8, stride=4), :] = wall
    side = FINE * 2 * tps * 8
    lowest_ref[...] = packed_ref[0:side, :]
    highest_ref[...] = packed_ref[width * 2 * tps * 8 - side : width * 2 * tps * 8, :]
    main = 4 * width
    first, last = cor_ref[0:1, :], cor_ref[tiles - 1 : tiles, :]
    edge_ref[main : main + 8, :] = jnp.broadcast_to(
        jnp.where(lane[:1] < HALF, first, last), (8, LANES)
    )
    wall_ref[main : main + 8, :] = jnp.zeros((8, LANES), f32)
    flip = (iota((LANES, LANES), 0) + iota((LANES, LANES), 1) == LANES - 1).astype(f32)
    row, col = iota((main, main), 0), iota((main, main), 1)
    sign = jnp.where(row & 2 == 0, 1.0, -1.0)
    turn = jnp.where((row & 3 == col & 3) & ((row >> 2) + (col >> 2) == width - 1), sign, 0.0)
    turned = jnp.dot(turn, edge_ref[0:main, :], precision=exact, preferred_element_type=f32)
    mirror_ref[0:main, :] = jnp.dot(turned, flip, precision=exact, preferred_element_type=f32)
    mirror_ref[main : main + 8, :] = jnp.dot(
        edge_ref[main : main + 8, :], flip, precision=exact, preferred_element_type=f32
    )


def edge_kernel(swap_ref, folded_ref, wall_ref, lowest_ref, highest_ref, ext_ref, odd_ref, even_ref):
    is_top = lax.axis_index("gy") == lax.axis_size("gy") - 1
    north = iota(swap_ref.shape, 1) < HALF
    swap = swap_ref[...]
    beyond = jnp.where(
        north, jnp.where(is_top, folded_ref[...], swap), jnp.where(is_top, swap, wall_ref[...])
    )
    ext_ref[...] = beyond
    side = lowest_ref.shape[0]
    main = swap_ref.shape[0] - 8
    even = is_even()
    parts = (
        (slice(0, side), lowest_ref[...], highest_ref[...]),
        (
            slice(side, side + 4 * FINE),
            ext_ref[0 : 4 * FINE, :],
            ext_ref[main - 4 * FINE : main, :],
        ),
    )
    for rows, low, high in parts:
        odd_ref[rows, :] = jnp.where(even, low, high)
        even_ref[rows, :] = jnp.where(even, high, low)


class Shifts:
    def __init__(self, tps):
        self.tps = tps
        self.span = (tps + 1) * LANES
        self.shape = (8, self.span)
        self.lane = iota(self.shape, 1)
        lane = iota((8, LANES), 1)
        row = iota((8, LANES), 0) & (SEGS - 1)
        self.first_half = lane < HALF
        self.low = iota((8, LANES), 0) < SEGS
        self.outer = ((row == SEGS - 1) & (lane < HALF)) | ((row == 0) & (lane >= HALF))
        bottom = lax.axis_index("gy") == 0
        wall = (iota(self.shape, 0) & (SEGS - 1) == 0) & (self.lane >= tps * LANES + HALF) & bottom
        self.weight = jnp.where(wall, 0.0, relax_weight)

    def roll(self, value, shift):
        return pltpu.roll(value, shift % self.span, 1)

    def odd(self, step):
        return self.lane & step != 0

    def pair(self, value, step):
        return value + jnp.where(self.odd(step), self.roll(value, step), self.roll(value, -step))

    def with_halo(self, parts, outside):
        inside = jnp.where(self.first_half, pltpu.roll(parts[0], 7, 0), pltpu.roll(parts[-1], 1, 0))
        return parts + [jnp.where(self.outer, outside, inside)]

    def rotations(self, cor_ref, line):
        parts = [cor_ref[pl.ds(k, SEGS, stride=self.tps), :] for k in range(self.tps)]
        parts = [jnp.concatenate([part, -part], 0) for part in parts]
        line = jnp.broadcast_to(line, (8, LANES))
        rotation = jnp.concatenate(self.with_halo(parts, jnp.where(self.low, line, -line)), 1)
        result = []
        for level in range(LEVELS):
            result.append(rotation)
            rotation = 0.5 * self.pair(rotation, 1 << level)
        return result

    def around(self, now, x, field, east, rotation, step):
        north = now["north"][x]
        west_nb, w, east_nb = field
        return (
            east[1] * east_nb
            + east[0] * west_nb
            + north * self.roll(w, -step)
            + self.roll(north * w, step)
            + rotation * other(w)
        )

    def coefficients(self, now, first, group, step):
        east = [now["east"][first + j - 1] for j in range(group + 1)]
        for j in range(group):
            x = first + j
            north = now["north"][x]
            diag = now["mass"][x] + east[j + 1] + east[j] + north + self.roll(north, step)
            scale = self.weight / diag
            now["scale"][x] = scale
            now["field"][x] = scale * now["right"][x]

    def coarse_east(self, now, fine, target, step):
        target[...] = 0.25 * self.pair(now["east"][fine + 1], step)

    def coarse_sums(self, now, coarse, fine, place, step):
        north = now["north"][fine] + now["north"][fine + 1]
        coarse["north"][place] = 0.25 * jnp.where(self.odd(step), north, self.roll(north, -step))
        coarse["mass"][place] = 0.25 * self.pair(now["mass"][fine] + now["mass"][fine + 1], step)

    def restrict(self, now, coarse, fine, place, group, rotation, step):
        field = [now["field"][fine + j - 1] for j in range(2 * group + 2)]
        east = [now["east"][fine + j - 1] for j in range(2 * group + 1)]
        rest = [
            (1.0 - relax_weight) * now["right"][fine + j]
            + self.around(now, fine + j, field[j : j + 3], east[j : j + 2], rotation, step)
            for j in range(2 * group)
        ]
        for j in range(group):
            coarse["right"][place + j] = 0.25 * self.pair(rest[2 * j] + rest[2 * j + 1], step)

    def sweep(self, now, first, group, value, rotation, step, put):
        field = [value(first + j - 1) for j in range(group + 2)]
        east = [now["east"][first + j - 1] for j in range(group + 1)]
        for j in range(group):
            x = first + j
            near = now["right"][x] + self.around(
                now, x, field[j : j + 3], east[j : j + 2], rotation, step
            )
            put(x, (1.0 - relax_weight) * field[j + 1] + now["scale"][x] * near)


def other(value):
    return pltpu.roll(value, SEGS, 0)


def loop(start, count, body, group=GROUP):
    whole, rest = divmod(count, group)
    if whole == 1:
        body(start, group)
    elif whole:
        lax.fori_loop(0, whole, lambda g, c: (body(start + g * group, group), c)[1], 0)
    if rest:
        body(start + whole * group, rest)


FIRST = ("north", "east", "scale", "right", "field")
COARSE = ("right", "east", "north", "mass")


def first_kernel(own_ref, ext_ref, odd_ref, even_ref, cor_ref, *refs):
    width = (ext_ref.shape[0] - 8) // 4
    tps = cor_ref.shape[0] // SEGS
    move = Shifts(tps)
    levels = [dict(zip(FIRST, refs[5 * n : 5 * n + 5])) for n in range(SPLIT)]
    sent_ref, rot_ref = refs[5 * SPLIT : 5 * SPLIT + 2]
    rest = list(refs[5 * SPLIT + 2 :])
    visc = rest.pop(0)
    for level in levels:
        level["mass"] = rest.pop(0)
    bottom = dict(zip(COARSE, rest))
    levels.append(bottom)
    main = ext_ref.shape[0] - 8
    rotations = move.rotations(cor_ref, ext_ref[main : main + 1, :])
    for level in range(LEVELS):
        rot_ref[level] = rotations[level]
    top = levels[0]

    even = is_even()

    def from_left(rows):
        return jnp.where(even, odd_ref[rows, :], even_ref[rows, :])

    def from_right(rows):
        return jnp.where(even, even_ref[rows, :], odd_ref[rows, :])

    def unpack(load, base, ext, index, x):
        rows = [jnp.broadcast_to(ext[4 * index + a : 4 * index + a + 1], (8, LANES)) for a in range(4)]
        both = move.with_halo(
            [load(pl.ds(base + 8 * k, 8)) for k in range(tps)], jnp.where(move.low, rows[0], rows[1])
        )
        turned = [other(part) for part in both]
        value = jnp.concatenate([jnp.where(move.low, a, b) for a, b in zip(both, turned)], 1)
        visc[x] = value
        top["mass"][x] = jnp.concatenate([jnp.where(move.low, b, a) for a, b in zip(both, turned)], 1)
        top["right"][x] = jnp.concatenate(
            move.with_halo(
                [load(pl.ds(base + 8 * (tps + k), 8)) for k in range(tps)],
                jnp.where(move.low, rows[2], rows[3]),
            ),
            1,
        )
        top["north"][x] = 0.5 * (value + move.roll(value, -1))

    each = 2 * tps * 8
    for load, start in ((from_left, 0), (from_right, FINE + width)):
        for j in range(0, FINE, 2):
            ext = load(pl.ds(FINE * each + 4 * j, 8))
            for index in range(2):
                unpack(load, (j + index) * each, ext, index, start + j + index)

    def own(first, group):
        for j in range(0, group, 2):
            x = first + j
            ext = ext_ref[pl.ds(pl.multiple_of(4 * x, 8), 8), :]
            for index in range(2):
                unpack(
                    lambda rows: own_ref[rows, :],
                    pl.multiple_of((x + index) * each, 8),
                    ext,
                    index,
                    FINE + x + index,
                )

    loop(0, width, own)
    columns = 2 * FINE + width

    def faces(first, group):
        value = [visc[first + j] for j in range(group + 1)]
        for j in range(group):
            top["east"][first + j] = 0.5 * (value[j] + value[j + 1])

    loop(0, columns - 1, faces, 11)
    loop(1, columns - 2, lambda x, n: move.coefficients(top, x, n, 1), 7)
    half = columns // 2
    level1 = levels[1]

    def east1(first, group):
        for j in range(group):
            level1["east"][first + j] = 0.25 * move.pair(top["east"][2 * (first + j) + 1], 1)

    def sums1(first, group):
        for j in range(group):
            move.coarse_sums(top, level1, 2 * (first + j), first + j, 1)

    loop(0, half - 1, east1, 7)
    loop(0, half, sums1, 11)
    loop(1, half - 2, lambda x, n: move.restrict(top, level1, 2 * x, x, n, rotations[0], 1), 5)
    loop(1, half - 2, lambda x, n: move.coefficients(level1, x, n, 2), 10)
    count = width >> SPLIT
    skip = FINE // 2
    for k in range(count):
        bottom["east"][k] = 0.25 * move.pair(level1["east"][skip + 2 * k + 1], 2)
        move.coarse_sums(level1, bottom, skip + 2 * k, k, 2)
    move.restrict(level1, bottom, skip, 0, count, rotations[1], 2)
    bit0, bit1 = move.odd(1), move.odd(2)
    for k in range(count):
        parts = [bottom[name][k] for name in COARSE]
        sent_ref[k] = jnp.where(
            bit1, jnp.where(bit0, parts[3], parts[2]), jnp.where(bit0, parts[1], parts[0])
        )


SECOND = ("right", "east", "north", "mass", "scale", "field")


def second_kernel(own_ref, odd_ref, even_ref, rot_ref, *refs):
    out_refs = 5 * SPLIT
    levels = [dict(zip(FIRST, refs[5 * n : 5 * n + 5])) for n in range(SPLIT)]
    out_ref = refs[out_refs]
    rest = list(refs[out_refs + 1 :])
    flat = rest.pop(0)
    for _ in range(SPLIT, LEVELS):
        levels.append(dict(zip(SECOND, rest[:6])))
        rest = rest[6:]
    done = rest
    width = out_ref.shape[1]
    tps = out_ref.shape[2] // LANES // SEGS
    tiles = tps * SEGS
    move = Shifts(tps)
    rotations = [rot_ref[level] for level in range(LEVELS)]
    count = width >> SPLIT
    now = levels[SPLIT]
    bit0, bit1 = move.odd(1), move.odd(2)
    even = is_even()
    loads = (
        lambda j: jnp.where(even, odd_ref[j], even_ref[j]),
        lambda j: own_ref[j],
        lambda j: jnp.where(even, even_ref[j], odd_ref[j]),
    )
    for third, load in enumerate(loads):
        start = third * count
        for j in range(count):
            value = load(j)
            evens = jnp.where(bit0, move.roll(value, 1), value)
            odds = jnp.where(bit0, value, move.roll(value, -1))
            for name, part, upper in zip(COARSE, (evens, odds, evens, odds), (0, 0, 1, 1)):
                if upper:
                    now[name][start + j] = jnp.where(bit1, part, move.roll(part, -2))
                else:
                    now[name][start + j] = jnp.where(bit1, move.roll(part, 2), part)
    total = 3 * count
    move.coefficients(now, 1, total - 2, 1 << SPLIT)
    for level in range(SPLIT, LEVELS - 1):
        now, coarse = levels[level], levels[level + 1]
        step = 1 << level
        half = total // 2
        for k in range(half - 1):
            coarse["east"][k] = 0.25 * move.pair(now["east"][2 * k + 1], step)
        for k in range(1, half - 1):
            move.coarse_sums(now, coarse, 2 * k, k, step)
        move.restrict(now, coarse, 2, 1, half - 2, rotations[level], step)
        total = half
        move.coefficients(coarse, 1, total - 2, 2 * step)

    def keep(target):
        def put(x, value):
            target[x] = value

        return put

    level = LEVELS - 1
    last, solved = levels[level], done.pop(0)
    own = width >> level
    move.sweep(
        last, own - 2, own + 4, lambda x: last["field"][x], rotations[level], 1 << level, keep(solved)
    )
    move.sweep(
        last, own - 1, own + 2, lambda x: solved[x], rotations[level], 1 << level, keep(last["field"])
    )
    solved, before = last["field"], own
    for level in reversed(range(LEVELS - 1)):
        now = levels[level]
        own = width >> level
        here = own if level >= SPLIT else FINE >> level
        lead = 2 * before - here if level >= SPLIT - 1 else 0

        def value(x, now=now, solved=solved, lead=lead):
            return now["field"][x] + solved[lax.div(x + lead, 2)]

        if level:
            target = done.pop(0)
            loop(
                here - 1,
                own + 2,
                lambda x, n, now=now, value=value, level=level, target=target: move.sweep(
                    now, x, n, value, rotations[level], 1 << level, keep(target)
                ),
                10,
            )
            solved, before = target, here
        else:

            def put(x, result, here=here):
                for k in range(tps):
                    row = pl.multiple_of(((x - here) * tps + k) * 8, 8)
                    flat[pl.ds(row, 8), :] = result[:, k * LANES : (k + 1) * LANES]

            loop(
                here,
                own,
                lambda x, n, now=now, value=value: move.sweep(now, x, n, value, rotations[0], 1, put),
            )

    for c in range(2):
        for i in range(width // 8):
            for t in range(tiles):
                s, k = divmod(t, tps)
                row = (8 * i * tps + k) * 8 + c * SEGS + s
                out_ref[c, 8 * i : 8 * i + 8, t * LANES : (t + 1) * LANES] = flat[
                    pl.ds(row, 8, stride=tps * 8), :
                ]


def local(forcing, viscosity, mass, coriolis, land, ice_tiles):
    width, height = viscosity.shape
    tiles = height // LANES
    tps = tiles // SEGS
    each = 2 * tps * 8
    outside = 4 * width + 8
    gx, gy = lax.axis_size("gx"), lax.axis_size("gy")
    lines = coriolis.reshape(tiles, LANES)
    vmem = pl.BlockSpec(memory_space=pltpu.VMEM)

    def here(*shape):
        return pltpu.VMEM(shape, f32)

    def call(kernel, outs, args, scratch=(), space=pltpu.VMEM):
        return pl.pallas_call(
            kernel,
            out_shape=outs,
            in_specs=[pl.BlockSpec(memory_space=space)] * len(args),
            out_specs=jax.tree.map(lambda _: vmem, outs),
            scratch_shapes=scratch,
            compiler_params=pltpu.CompilerParams(vmem_limit_bytes=24 * 1024 * 1024),
        )(*(pltpu.with_memory_space_constraint(arg, space) for arg in args))

    sources = (ice_tiles.T, forcing, viscosity, mass, land, lines)
    packed, lowest, highest, edge, mirror, wall = call(
        prepare_kernel,
        (
            here(width * each, LANES),
            here(FINE * each, LANES),
            here(FINE * each, LANES),
            here(outside, LANES),
            here(outside, LANES),
            here(outside, LANES),
        ),
        sources,
        scratch=[pltpu.SMEM(sources[0].shape, sources[0].dtype)]
        + [pltpu.VMEM(source.shape, source.dtype) for source in sources[1:]]
        + [pltpu.SemaphoreType.DMA((len(sources),))],
        space=pltpu.HBM,
    )
    top = gy - 1
    folded = lax.ppermute(
        mirror, ("gx", "gy"), [(i * gy + top, (gx - 1 - i) * gy + top) for i in range(gx)]
    )
    swap = lax.ppermute(edge, "gy", [(i, gy - 1 - i) for i in range(gy)])
    ext, odd, even = call(
        edge_kernel,
        (here(outside, LANES),) + (here(FINE * (each + 4), LANES),) * 2,
        (swap, folded, wall, lowest, highest),
    )
    odd_pairs = [(i, (i + (1 if i % 2 else gx - 1)) % gx) for i in range(gx)]
    even_pairs = [(i, i ^ 1) for i in range(gx)]
    by_odd = lax.ppermute(odd, "gx", odd_pairs)
    by_even = lax.ppermute(even, "gx", even_pairs)

    span = (tps + 1) * LANES
    columns = [(2 * FINE + width) >> level for level in range(SPLIT)]
    columns += [3 * width >> level for level in range(SPLIT, LEVELS)]
    count = width >> SPLIT

    def lines_of(number):
        return here(number, 8, span)

    state = call(
        first_kernel,
        tuple(lines_of(columns[level]) for level in range(SPLIT) for _ in FIRST)
        + (lines_of(count), lines_of(LEVELS)),
        (packed, ext, by_odd, by_even, lines),
        scratch=[lines_of(columns[0])]
        + [lines_of(columns[level]) for level in range(SPLIT)]
        + [lines_of(count)] * len(COARSE),
    )
    *kept, sent, rotation = state
    by_odd = lax.ppermute(sent, "gx", odd_pairs)
    by_even = lax.ppermute(sent, "gx", even_pairs)
    return call(
        second_kernel,
        jax.ShapeDtypeStruct((2, width, height), f32),
        (sent, by_odd, by_even, rotation, *kept),
        scratch=[pltpu.VMEM((width * tps * 8, LANES), f32)]
        + [lines_of(columns[level]) for level in range(SPLIT, LEVELS) for _ in SECOND]
        + [lines_of(columns[level]) for level in reversed(range(1, LEVELS))],
    )


def solution(mesh):
    return jax.shard_map(
        local,
        mesh=mesh,
        in_specs=(
            P(None, ("groups", "gx"), "gy"),
            P(("groups", "gx"), "gy"),
            P(("groups", "gx"), "gy"),
            P("gy"),
            P("gx", "gy"),
            P("groups", None),
        ),
        out_specs=P(None, ("groups", "gx"), "gy"),
        check_vma=False,
    )
```

```python
import jax
import jax.numpy as jnp
from jax import lax
from jax.experimental import pallas as pl
from jax.experimental.pallas import tpu as pltpu
from jax.sharding import PartitionSpec as P


TILE = 128
LEVELS = 4
LANES = 128
SEGS = 4
HALF = LANES // 2
GROUP = 8

relax_weight = 0.8
land_mass = 4.0
f32 = jnp.float32
exact = lax.Precision.HIGHEST


FINE = 6
SPLIT = 2


def iota(shape, axis):
    return lax.broadcasted_iota(jnp.int32, shape, axis)


def is_even():
    return lax.axis_index("gx") & 1 == 0


def masked(ice, visc, mass, land, forcing):
    land = land.astype(f32)
    ocean = 1.0 - land
    return (
        visc * ice * ocean,
        mass * ocean + land_mass * land,
        forcing[0] * ocean,
        forcing[1] * ocean,
    )


def fetch(sources, held, sems):
    copies = [pltpu.make_async_copy(a, b, sems.at[n]) for n, (a, b) in enumerate(zip(sources, held))]
    for copy in copies:
        copy.start()
    return copies


def ends_kernel(
    ice_hbm, forcing_hbm, visc_hbm, mass_hbm, land_hbm, cor_hbm, edge_ref, mirror_ref, wall_ref,
    ice_ref, cor_ref, forcing_ref, visc_ref, mass_ref, land_ref, sems,
):
    width = visc_hbm.shape[0]
    tiles = visc_hbm.shape[1] // LANES
    sources, held = [ice_hbm, cor_hbm], [ice_ref, cor_ref]
    for n, t in enumerate((0, tiles - 1)):
        cols = pl.ds(t * LANES, LANES)
        sources += [forcing_hbm.at[:, :, cols]] + [a.at[:, cols] for a in (visc_hbm, mass_hbm, land_hbm)]
        held += [a.at[n] for a in (forcing_ref, visc_ref, mass_ref, land_ref)]
    copies = fetch(sources, held, sems)
    tile_x = lax.axis_index("gx") * width // TILE
    tile_y = lax.axis_index("gy") * tiles
    lane = iota((8, LANES), 1)
    main = 4 * width
    flip = (iota((LANES, LANES), 0) + iota((LANES, LANES), 1) == LANES - 1).astype(f32)
    row, col = iota((main, main), 0), iota((main, main), 1)
    sign = jnp.where(row & 2 == 0, 1.0, -1.0)
    turn = jnp.where((row & 3 == col & 3) & ((row >> 2) + (col >> 2) == width - 1), sign, 0.0)
    wall_ref[main : main + 8, :] = jnp.zeros((8, LANES), f32)
    for copy in copies:
        copy.wait()
    for i in range(width // 8):
        rows = slice(8 * i, 8 * i + 8)
        ends = [
            masked(
                ice_ref[tile_y + t, tile_x].astype(f32),
                visc_ref[n, rows, :],
                mass_ref[n, rows, :],
                land_ref[n, rows, :],
                [forcing_ref[n, c, rows, :] for c in range(2)],
            )
            for n, t in enumerate((0, tiles - 1))
        ]
        for a in range(4):
            start = 8 * i * 4 + a
            edge_ref[pl.ds(start, 8, stride=4), :] = jnp.where(lane < HALF, ends[0][a], ends[1][a])
            if a == 0:
                wall = jnp.broadcast_to(ends[0][0][:, :1], (8, LANES))
            else:
                wall = jnp.full((8, LANES), 1.0 if a == 1 else 0.0, f32)
            wall_ref[pl.ds(start, 8, stride=4), :] = wall
    first, last = cor_ref[0:1, :], cor_ref[tiles - 1 : tiles, :]
    edge_ref[main : main + 8, :] = jnp.broadcast_to(
        jnp.where(lane[:1] < HALF, first, last), (8, LANES)
    )
    turned = jnp.dot(turn, edge_ref[0:main, :], precision=exact, preferred_element_type=f32)
    mirror_ref[0:main, :] = jnp.dot(turned, flip, precision=exact, preferred_element_type=f32)
    mirror_ref[main : main + 8, :] = jnp.dot(
        edge_ref[main : main + 8, :], flip, precision=exact, preferred_element_type=f32
    )


def pack_kernel(
    ice_hbm, forcing_hbm, visc_hbm, mass_hbm, land_hbm, packed_ref, lowest_ref, highest_ref,
    ice_ref, forcing_ref, visc_ref, mass_ref, land_ref, sems,
):
    copies = fetch(
        (ice_hbm, forcing_hbm, visc_hbm, mass_hbm, land_hbm),
        (ice_ref, forcing_ref, visc_ref, mass_ref, land_ref),
        sems,
    )
    width = visc_ref.shape[0]
    tiles = visc_ref.shape[1] // LANES
    tps = tiles // SEGS
    tile_x = lax.axis_index("gx") * width // TILE
    tile_y = lax.axis_index("gy") * tiles
    for copy in copies:
        copy.wait()
    for i in range(width // 8):
        rows = slice(8 * i, 8 * i + 8)
        for t in range(tiles):
            s, k = divmod(t, tps)
            cols = slice(t * LANES, (t + 1) * LANES)
            values = masked(
                ice_ref[tile_y + t, tile_x].astype(f32),
                visc_ref[rows, cols],
                mass_ref[rows, cols],
                land_ref[rows, cols],
                [forcing_ref[c, rows, cols] for c in range(2)],
            )
            for a, value in enumerate(values):
                tile = 8 * i * 2 * tps + (a // 2) * tps + k
                start = tile * 8 + (a % 2) * SEGS + s
                packed_ref[pl.ds(start, 8, stride=2 * tps * 8), :] = value
    side = FINE * 2 * tps * 8
    lowest_ref[...] = packed_ref[0:side, :]
    highest_ref[...] = packed_ref[width * 2 * tps * 8 - side : width * 2 * tps * 8, :]


def edge_kernel(swap_ref, folded_ref, wall_ref, lowest_ref, highest_ref, ext_ref, odd_ref, even_ref):
    is_top = lax.axis_index("gy") == lax.axis_size("gy") - 1
    north = iota(swap_ref.shape, 1) < HALF
    swap = swap_ref[...]
    beyond = jnp.where(
        north, jnp.where(is_top, folded_ref[...], swap), jnp.where(is_top, swap, wall_ref[...])
    )
    ext_ref[...] = beyond
    side = lowest_ref.shape[0]
    main = swap_ref.shape[0] - 8
    even = is_even()
    parts = (
        (slice(0, side), lowest_ref[...], highest_ref[...]),
        (
            slice(side, side + 4 * FINE),
            ext_ref[0 : 4 * FINE, :],
            ext_ref[main - 4 * FINE : main, :],
        ),
    )
    for rows, low, high in parts:
        odd_ref[rows, :] = jnp.where(even, low, high)
        even_ref[rows, :] = jnp.where(even, high, low)


class Shifts:
    def __init__(self, tps):
        self.tps = tps
        self.span = (tps + 1) * LANES
        self.shape = (8, self.span)
        self.lane = iota(self.shape, 1)
        lane = iota((8, LANES), 1)
        row = iota((8, LANES), 0) & (SEGS - 1)
        self.first_half = lane < HALF
        self.low = iota((8, LANES), 0) < SEGS
        self.outer = ((row == SEGS - 1) & (lane < HALF)) | ((row == 0) & (lane >= HALF))
        bottom = lax.axis_index("gy") == 0
        wall = (iota(self.shape, 0) & (SEGS - 1) == 0) & (self.lane >= tps * LANES + HALF) & bottom
        self.weight = jnp.where(wall, 0.0, relax_weight)

    def roll(self, value, shift):
        return pltpu.roll(value, shift % self.span, 1)

    def odd(self, step):
        return self.lane & step != 0

    def pair(self, value, step):
        return value + jnp.where(self.odd(step), self.roll(value, step), self.roll(value, -step))

    def with_halo(self, parts, outside):
        inside = jnp.where(self.first_half, pltpu.roll(parts[0], 7, 0), pltpu.roll(parts[-1], 1, 0))
        return parts + [jnp.where(self.outer, outside, inside)]

    def rotations(self, cor_ref, line):
        parts = [cor_ref[pl.ds(k, SEGS, stride=self.tps), :] for k in range(self.tps)]
        parts = [jnp.concatenate([part, -part], 0) for part in parts]
        line = jnp.broadcast_to(line, (8, LANES))
        rotation = jnp.concatenate(self.with_halo(parts, jnp.where(self.low, line, -line)), 1)
        result = []
        for level in range(LEVELS):
            result.append(rotation)
            rotation = 0.5 * self.pair(rotation, 1 << level)
        return result

    def around(self, now, x, field, east, rotation, step):
        north = now["north"][x]
        west_nb, w, east_nb = field
        return (
            east[1] * east_nb
            + east[0] * west_nb
            + north * self.roll(w, -step)
            + self.roll(north * w, step)
            + rotation * other(w)
        )

    def coefficients(self, now, first, group, step):
        east = [now["east"][first + j - 1] for j in range(group + 1)]
        for j in range(group):
            x = first + j
            north = now["north"][x]
            diag = now["mass"][x] + east[j + 1] + east[j] + north + self.roll(north, step)
            scale = self.weight / diag
            now["scale"][x] = scale
            now["field"][x] = scale * now["right"][x]

    def coarse_east(self, now, fine, target, step):
        target[...] = 0.25 * self.pair(now["east"][fine + 1], step)

    def coarse_sums(self, now, coarse, fine, place, step):
        north = now["north"][fine] + now["north"][fine + 1]
        coarse["north"][place] = 0.25 * jnp.where(self.odd(step), north, self.roll(north, -step))
        coarse["mass"][place] = 0.25 * self.pair(now["mass"][fine] + now["mass"][fine + 1], step)

    def restrict(self, now, coarse, fine, place, group, rotation, step):
        field = [now["field"][fine + j - 1] for j in range(2 * group + 2)]
        east = [now["east"][fine + j - 1] for j in range(2 * group + 1)]
        rest = [
            (1.0 - relax_weight) * now["right"][fine + j]
            + self.around(now, fine + j, field[j : j + 3], east[j : j + 2], rotation, step)
            for j in range(2 * group)
        ]
        for j in range(group):
            coarse["right"][place + j] = 0.25 * self.pair(rest[2 * j] + rest[2 * j + 1], step)

    def sweep(self, now, first, group, value, rotation, step, put):
        field = [value(first + j - 1) for j in range(group + 2)]
        east = [now["east"][first + j - 1] for j in range(group + 1)]
        for j in range(group):
            x = first + j
            near = now["right"][x] + self.around(
                now, x, field[j : j + 3], east[j : j + 2], rotation, step
            )
            put(x, (1.0 - relax_weight) * field[j + 1] + now["scale"][x] * near)


def other(value):
    return pltpu.roll(value, SEGS, 0)


def loop(start, count, body, group=GROUP):
    whole, rest = divmod(count, group)
    if whole == 1:
        body(start, group)
    elif whole:
        lax.fori_loop(0, whole, lambda g, c: (body(start + g * group, group), c)[1], 0)
    if rest:
        body(start + whole * group, rest)


FIRST = ("north", "east", "scale", "right", "field")
STATE = FIRST + ("mass",)
COARSE = ("right", "east", "north", "mass")
AHEAD = ("done", "same", "side", "up", "down", "turn")


def faces(visc, east, first, group):
    value = [visc[first + j] for j in range(group + 1)]
    for j in range(group):
        east[first + j] = 0.5 * (value[j] + value[j + 1])


def unpack(move, visc, top, load, base, ext, index, x):
    tps = move.tps
    rows = [jnp.broadcast_to(ext[4 * index + a : 4 * index + a + 1], (8, LANES)) for a in range(4)]
    both = move.with_halo(
        [load(pl.ds(base + 8 * k, 8)) for k in range(tps)], jnp.where(move.low, rows[0], rows[1])
    )
    turned = [other(part) for part in both]
    value = jnp.concatenate([jnp.where(move.low, a, b) for a, b in zip(both, turned)], 1)
    visc[x] = value
    top["mass"][x] = jnp.concatenate([jnp.where(move.low, b, a) for a, b in zip(both, turned)], 1)
    top["right"][x] = jnp.concatenate(
        move.with_halo(
            [load(pl.ds(base + 8 * (tps + k), 8)) for k in range(tps)],
            jnp.where(move.low, rows[2], rows[3]),
        ),
        1,
    )
    top["north"][x] = 0.5 * (value + move.roll(value, -1))


def coarsen(move, now, coarse, first, group, skip, step, with_east=True, with_sums=True):
    for j in range(group):
        x = 2 * (first + j) + skip
        if with_east:
            coarse["east"][first + j] = 0.25 * move.pair(now["east"][x + 1], step)
        if with_sums:
            move.coarse_sums(now, coarse, x, first + j, step)


def send(move, bottom, sent_ref, columns):
    bit0, bit1 = move.odd(1), move.odd(2)
    for k in columns:
        parts = [bottom[name][k] for name in COARSE]
        sent_ref[k] = jnp.where(
            bit1, jnp.where(bit0, parts[3], parts[2]), jnp.where(bit0, parts[1], parts[0])
        )


def grouped(refs):
    levels = [dict(zip(STATE, refs[6 * n : 6 * n + 6])) for n in range(SPLIT)]
    return levels, refs[6 * SPLIT], refs[6 * SPLIT + 1]


def own_kernel(own_ref, ext_ref, cor_ref, *refs):
    width = (ext_ref.shape[0] - 8) // 4
    tps = cor_ref.shape[0] // SEGS
    move = Shifts(tps)
    (top, level1), visc, sent_ref = grouped(refs)
    rot_ref = refs[6 * SPLIT + 2]
    bottom = dict(zip(COARSE, refs[6 * SPLIT + 3 :]))
    main = ext_ref.shape[0] - 8
    rotations = move.rotations(cor_ref, ext_ref[main : main + 1, :])
    for level in range(LEVELS):
        rot_ref[level] = rotations[level]
    each = 2 * tps * 8

    def own(first, group):
        for j in range(0, group, 2):
            x = first + j
            ext = ext_ref[pl.ds(pl.multiple_of(4 * x, 8), 8), :]
            for index in range(2):
                base = pl.multiple_of((x + index) * each, 8)
                unpack(
                    move, visc, top, lambda rows: own_ref[rows, :], base, ext, index, FINE + x + index
                )

    loop(0, width, own)
    loop(FINE, width - 1, lambda x, n: faces(visc, top["east"], x, n), 16)
    loop(FINE + 1, width - 2, lambda x, n: move.coefficients(top, x, n, 1), 10)
    skip, half, count = FINE // 2, width // 2, width >> SPLIT
    loop(skip, half - 1, lambda x, n: coarsen(move, top, level1, x, n, 0, 1), 15)
    coarsen(move, top, level1, skip + half - 1, 1, 0, 1, with_east=False)
    loop(
        skip + 1, half - 2, lambda x, n: move.restrict(top, level1, 2 * x, x, n, rotations[0], 1), 7
    )
    move.coefficients(level1, skip + 1, half - 2, 2)
    coarsen(move, level1, bottom, 1, count - 2, skip, 2)
    move.restrict(level1, bottom, skip + 2, 1, count - 2, rotations[1], 2)
    send(move, bottom, sent_ref, range(1, count - 1))


def sides_kernel(odd_ref, even_ref, rot_ref, *refs):
    (top, level1), visc, sent_ref = grouped(refs[6 * SPLIT + 2 : 12 * SPLIT + 4])
    bottom = dict(zip(COARSE, refs[12 * SPLIT + 4 :]))
    columns, _, span = visc.shape
    width = columns - 2 * FINE
    tps = span // LANES - 1
    move = Shifts(tps)
    each = 2 * tps * 8
    even = is_even()
    skip, half, count = FINE // 2, columns // 2, width >> SPLIT

    def from_left(rows):
        return jnp.where(even, odd_ref[rows, :], even_ref[rows, :])

    def from_right(rows):
        return jnp.where(even, even_ref[rows, :], odd_ref[rows, :])

    for load, start in ((from_left, 0), (from_right, FINE + width)):
        for j in range(0, FINE, 2):
            ext = load(pl.ds(FINE * each + 4 * j, 8))
            for index in range(2):
                unpack(move, visc, top, load, (j + index) * each, ext, index, start + j + index)
    for start in (0, columns - 1 - FINE):
        faces(visc, top["east"], start, FINE)
    for start in (1, columns - 1 - FINE):
        move.coefficients(top, start, FINE, 1)
    for start in (0, half - 1 - skip):
        coarsen(move, top, level1, start, skip, 0, 1, with_sums=False)
    for start in (1, half - skip):
        coarsen(move, top, level1, start, skip - 1, 0, 1, with_east=False)
    for start in (1, half - 1 - skip):
        move.restrict(top, level1, 2 * start, start, skip, rot_ref[0], 1)
        move.coefficients(level1, start, skip, 2)
    for k in (0, count - 1):
        coarsen(move, level1, bottom, k, 1, skip, 2)
        move.restrict(level1, bottom, skip + 2 * k, k, 1, rot_ref[1], 2)
    send(move, bottom, sent_ref, (0, count - 1))


def ahead_kernel(rot_ref, *refs):
    levels = [dict(zip(FIRST, refs[5 * n : 5 * n + 5])) for n in range(SPLIT)]
    outs = refs[5 * SPLIT :]
    move = Shifts(rot_ref.shape[2] // LANES - 1)
    for level, now in enumerate(levels):
        step = 1 << level
        ahead = dict(zip(AHEAD, outs[6 * level : 6 * level + 6]))
        start = FINE if level == 0 else (FINE >> level) - 1
        count = ahead["done"].shape[0]
        rotation = rot_ref[level]

        def body(first, group, now=now, ahead=ahead, step=step, start=start, level=level, rotation=rotation):
            x0 = first + start
            field = [now["field"][x0 + j - 1] for j in range(group + 2)]
            east = [now["east"][x0 + j - 1] for j in range(group + 1)]
            for j in range(group):
                x, place = x0 + j, first + j
                scale = now["scale"][x]
                north = now["north"][x]
                near = now["right"][x] + move.around(
                    now, x, field[j : j + 3], east[j : j + 2], rotation, step
                )
                ahead["done"][place] = (1.0 - relax_weight) * field[j + 1] + scale * near
                inner, outer = east[j + 1], east[j]
                if (j + level) % 2:
                    inner, outer = outer, inner
                ahead["same"][place] = (1.0 - relax_weight) + scale * inner
                ahead["side"][place] = scale * outer
                ahead["up"][place] = scale * north
                ahead["down"][place] = scale * move.roll(north, step)
                ahead["turn"][place] = scale * rotation

        loop(0, count, body, 8 if level == 0 else 6)


SECOND = ("right", "east", "north", "mass", "scale", "field")


def second_kernel(own_ref, odd_ref, even_ref, rot_ref, *refs):
    aheads = [dict(zip(AHEAD, refs[6 * n : 6 * n + 6])) for n in range(SPLIT)]
    out_hbm = refs[6 * SPLIT]
    rest = list(refs[6 * SPLIT + 1 :])
    flat, out_ref, sems = rest[:3]
    rest = rest[3:]
    levels = [None] * SPLIT
    for _ in range(SPLIT, LEVELS):
        levels.append(dict(zip(SECOND, rest[:6])))
        rest = rest[6:]
    done = rest
    width = out_ref.shape[1]
    tps = out_ref.shape[2] // LANES // SEGS
    tiles = tps * SEGS
    move = Shifts(tps)
    rotations = [rot_ref[level] for level in range(LEVELS)]
    count = width >> SPLIT
    now = levels[SPLIT]
    bit0, bit1 = move.odd(1), move.odd(2)
    even = is_even()
    loads = (
        lambda j: jnp.where(even, odd_ref[j], even_ref[j]),
        lambda j: own_ref[j],
        lambda j: jnp.where(even, even_ref[j], odd_ref[j]),
    )
    for third, load in enumerate(loads):
        start = third * count
        for j in range(count):
            value = load(j)
            evens = jnp.where(bit0, move.roll(value, 1), value)
            odds = jnp.where(bit0, value, move.roll(value, -1))
            for name, part, upper in zip(COARSE, (evens, odds, evens, odds), (0, 0, 1, 1)):
                if upper:
                    now[name][start + j] = jnp.where(bit1, part, move.roll(part, -2))
                else:
                    now[name][start + j] = jnp.where(bit1, move.roll(part, 2), part)
    total = 3 * count
    move.coefficients(now, 1, total - 2, 1 << SPLIT)
    for level in range(SPLIT, LEVELS - 1):
        now, coarse = levels[level], levels[level + 1]
        step = 1 << level
        half = total // 2
        for k in range(half - 1):
            coarse["east"][k] = 0.25 * move.pair(now["east"][2 * k + 1], step)
        for k in range(1, half - 1):
            move.coarse_sums(now, coarse, 2 * k, k, step)
        move.restrict(now, coarse, 2, 1, half - 2, rotations[level], step)
        total = half
        move.coefficients(coarse, 1, total - 2, 2 * step)

    def keep(target):
        def put(x, value):
            target[x] = value

        return put

    level = LEVELS - 1
    last, solved = levels[level], done.pop(0)
    own = width >> level
    move.sweep(
        last, own - 2, own + 4, lambda x: last["field"][x], rotations[level], 1 << level, keep(solved)
    )
    move.sweep(
        last, own - 1, own + 2, lambda x: solved[x], rotations[level], 1 << level, keep(last["field"])
    )
    solved, before = last["field"], own
    for level in reversed(range(SPLIT, LEVELS - 1)):
        now = levels[level]
        own = width >> level

        def value(x, now=now, solved=solved):
            return now["field"][x] + solved[lax.div(x, 2)]

        target = done.pop(0)
        move.sweep(now, own - 1, own + 2, value, rotations[level], 1 << level, keep(target))
        solved, before = target, own

    def correct(ahead, solved, first, count, place, step, put):
        for j in range(count):
            middle = solved[first + j]
            moved = (move.roll(middle, -step), move.roll(middle, step), other(middle))
            for child in range(2):
                x = place + 2 * j + child
                if isinstance(x, int) and not 0 <= x < ahead["done"].shape[0]:
                    continue
                result = (
                    ahead["done"][x]
                    + ahead["same"][x] * middle
                    + ahead["side"][x] * solved[first + j + 2 * child - 1]
                    + ahead["up"][x] * moved[0]
                    + ahead["down"][x] * moved[1]
                    + ahead["turn"][x] * moved[2]
                )
                put(x, result)

    target = done.pop(0)
    correct(aheads[1], solved, before - 1, (width >> SPLIT) + 2, -1, 2, keep(target))

    def put(x, result):
        for k in range(tps):
            row = pl.multiple_of((x * tps + k) * 8, 8)
            flat[pl.ds(row, 8), :] = result[:, k * LANES : (k + 1) * LANES]

    copies = []
    for i in range(width // 8):
        correct(aheads[0], target, 4 * i + 1, 4, 8 * i, 1, put)
        rows = pl.ds(8 * i, 8)
        for c in range(2):
            for t in range(tiles):
                s, k = divmod(t, tps)
                row = (8 * i * tps + k) * 8 + c * SEGS + s
                out_ref[c, rows, t * LANES : (t + 1) * LANES] = flat[pl.ds(row, 8, stride=tps * 8), :]
        copies.append(pltpu.make_async_copy(out_ref.at[:, rows, :], out_hbm.at[:, rows, :], sems.at[i]))
        copies[-1].start()
    for copy in copies:
        copy.wait()


def local(forcing, viscosity, mass, coriolis, land, ice_tiles):
    width, height = viscosity.shape
    tiles = height // LANES
    tps = tiles // SEGS
    each = 2 * tps * 8
    outside = 4 * width + 8
    gx, gy = lax.axis_size("gx"), lax.axis_size("gy")
    lines = coriolis.reshape(tiles, LANES)

    def here(*shape):
        return pltpu.VMEM(shape, f32)

    def call(kernel, outs, args, scratch=(), space=pltpu.VMEM, out_space=pltpu.VMEM, aliases={}):
        return pl.pallas_call(
            kernel,
            out_shape=outs,
            in_specs=[pl.BlockSpec(memory_space=space)] * len(args),
            out_specs=jax.tree.map(lambda _: pl.BlockSpec(memory_space=out_space), outs),
            scratch_shapes=scratch,
            input_output_aliases=aliases,
            compiler_params=pltpu.CompilerParams(vmem_limit_bytes=24 * 1024 * 1024),
        )(*(pltpu.with_memory_space_constraint(arg, space) for arg in args))

    sources = (ice_tiles.T, forcing, viscosity, mass, land, lines)
    ice_space = pltpu.SMEM(sources[0].shape, sources[0].dtype)
    edge, mirror, wall = call(
        ends_kernel,
        (here(outside, LANES),) * 3,
        sources,
        scratch=[ice_space, pltpu.VMEM(lines.shape, f32), pltpu.VMEM((2, 2, width, LANES), f32)]
        + [pltpu.VMEM((2, width, LANES), source.dtype) for source in sources[2:5]]
        + [pltpu.SemaphoreType.DMA((10,))],
        space=pltpu.HBM,
    )
    top = gy - 1
    folded = lax.ppermute(
        mirror, ("gx", "gy"), [(i * gy + top, (gx - 1 - i) * gy + top) for i in range(gx)]
    )
    swap = lax.ppermute(edge, "gy", [(i, gy - 1 - i) for i in range(gy)])
    packed, lowest, highest = call(
        pack_kernel,
        (here(width * each, LANES), here(FINE * each, LANES), here(FINE * each, LANES)),
        sources[:5],
        scratch=[ice_space]
        + [pltpu.VMEM(source.shape, source.dtype) for source in sources[1:5]]
        + [pltpu.SemaphoreType.DMA((5,))],
        space=pltpu.HBM,
    )
    ext, odd, even = call(
        edge_kernel,
        (here(outside, LANES),) + (here(FINE * (each + 4), LANES),) * 2,
        (swap, folded, wall, lowest, highest),
    )
    odd_pairs = [(i, (i + (1 if i % 2 else gx - 1)) % gx) for i in range(gx)]
    even_pairs = [(i, i ^ 1) for i in range(gx)]
    by_odd = lax.ppermute(odd, "gx", odd_pairs)
    by_even = lax.ppermute(even, "gx", even_pairs)

    span = (tps + 1) * LANES
    columns = [(2 * FINE + width) >> level for level in range(SPLIT)]
    columns += [3 * width >> level for level in range(SPLIT, LEVELS)]
    count = width >> SPLIT

    def lines_of(number):
        return here(number, 8, span)

    kept = tuple(lines_of(columns[level]) for level in range(SPLIT) for _ in STATE)
    kept += (lines_of(columns[0]), lines_of(count))
    coarse = [lines_of(count)] * len(COARSE)
    *state, rotation = call(
        own_kernel, kept + (lines_of(LEVELS),), (packed, ext, lines), scratch=coarse
    )
    state = call(
        sides_kernel,
        kept,
        (by_odd, by_even, rotation, *state),
        scratch=coarse,
        aliases={3 + n: n for n in range(len(kept))},
    )
    sent = state[-1]
    by_odd = lax.ppermute(sent, "gx", odd_pairs)
    by_even = lax.ppermute(sent, "gx", even_pairs)
    ahead = call(
        ahead_kernel,
        (lines_of(width),) * len(AHEAD) + (lines_of(width // 2 + 2),) * len(AHEAD),
        (rotation, *(state[len(STATE) * level + n] for level in range(SPLIT) for n in range(len(FIRST)))),
    )
    return call(
        second_kernel,
        jax.ShapeDtypeStruct((2, width, height), f32),
        (sent, by_odd, by_even, rotation, *ahead),
        scratch=[
            pltpu.VMEM((width * tps * 8, LANES), f32),
            pltpu.VMEM((2, width, height), f32),
            pltpu.SemaphoreType.DMA((width // 8,)),
        ]
        + [lines_of(columns[level]) for level in range(SPLIT, LEVELS) for _ in SECOND]
        + [lines_of(columns[level]) for level in reversed(range(SPLIT, LEVELS))]
        + [lines_of(width // 2 + 2)],
        out_space=pltpu.HBM,
    )


def solution(mesh):
    return jax.shard_map(
        local,
        mesh=mesh,
        in_specs=(
            P(None, ("groups", "gx"), "gy"),
            P(("groups", "gx"), "gy"),
            P(("groups", "gx"), "gy"),
            P("gy"),
            P("gx", "gy"),
            P("groups", None),
        ),
        out_specs=P(None, ("groups", "gx"), "gy"),
        check_vma=False,
    )
```

```python
import jax
import jax.numpy as jnp
from jax import lax
from jax.experimental import pallas as pl
from jax.experimental.pallas import tpu as pltpu
from jax.sharding import PartitionSpec as P


TILE = 128
LEVELS = 4
LANES = 128
SEGS = 4
HALF = LANES // 2
GROUP = 8

relax_weight = 0.8
land_mass = 4.0
f32 = jnp.float32
exact = lax.Precision.HIGHEST


FINE = 8
SPLIT = 2


def iota(shape, axis):
    return lax.broadcasted_iota(jnp.int32, shape, axis)


def is_even():
    return lax.axis_index("gx") & 1 == 0


def masked(ice, visc, mass, land, forcing):
    land = land.astype(f32)
    ocean = 1.0 - land
    return (
        visc * ice * ocean,
        mass * ocean + land_mass * land,
        forcing[0] * ocean,
        forcing[1] * ocean,
    )


def fetch(sources, held, sems):
    copies = [pltpu.make_async_copy(a, b, sems.at[n]) for n, (a, b) in enumerate(zip(sources, held))]
    for copy in copies:
        copy.start()
    return copies


def ends_kernel(
    ice_hbm, forcing_hbm, visc_hbm, mass_hbm, land_hbm, cor_hbm, edge_ref, mirror_ref, wall_ref,
    ice_ref, cor_ref, forcing_ref, visc_ref, mass_ref, land_ref, sems,
):
    width = visc_hbm.shape[0]
    tiles = visc_hbm.shape[1] // LANES
    sources, held = [ice_hbm, cor_hbm], [ice_ref, cor_ref]
    for n, t in enumerate((0, tiles - 1)):
        cols = pl.ds(t * LANES, LANES)
        sources += [forcing_hbm.at[:, :, cols]] + [a.at[:, cols] for a in (visc_hbm, mass_hbm, land_hbm)]
        held += [a.at[n] for a in (forcing_ref, visc_ref, mass_ref, land_ref)]
    copies = fetch(sources, held, sems)
    tile_x = lax.axis_index("gx") * width // TILE
    tile_y = lax.axis_index("gy") * tiles
    lane = iota((8, LANES), 1)
    main = 4 * width
    flip = (iota((LANES, LANES), 0) + iota((LANES, LANES), 1) == LANES - 1).astype(f32)
    row, col = iota((main, main), 0), iota((main, main), 1)
    sign = jnp.where(row & 2 == 0, 1.0, -1.0)
    turn = jnp.where((row & 3 == col & 3) & ((row >> 2) + (col >> 2) == width - 1), sign, 0.0)
    wall_ref[main : main + 8, :] = jnp.zeros((8, LANES), f32)
    for copy in copies:
        copy.wait()
    for i in range(width // 8):
        rows = slice(8 * i, 8 * i + 8)
        ends = [
            masked(
                ice_ref[tile_y + t, tile_x].astype(f32),
                visc_ref[n, rows, :],
                mass_ref[n, rows, :],
                land_ref[n, rows, :],
                [forcing_ref[n, c, rows, :] for c in range(2)],
            )
            for n, t in enumerate((0, tiles - 1))
        ]
        for a in range(4):
            start = 8 * i * 4 + a
            edge_ref[pl.ds(start, 8, stride=4), :] = jnp.where(lane < HALF, ends[0][a], ends[1][a])
            if a == 0:
                wall = jnp.broadcast_to(ends[0][0][:, :1], (8, LANES))
            else:
                wall = jnp.full((8, LANES), 1.0 if a == 1 else 0.0, f32)
            wall_ref[pl.ds(start, 8, stride=4), :] = wall
    first, last = cor_ref[0:1, :], cor_ref[tiles - 1 : tiles, :]
    edge_ref[main : main + 8, :] = jnp.broadcast_to(
        jnp.where(lane[:1] < HALF, first, last), (8, LANES)
    )
    turned = jnp.dot(turn, edge_ref[0:main, :], precision=exact, preferred_element_type=f32)
    mirror_ref[0:main, :] = jnp.dot(turned, flip, precision=exact, preferred_element_type=f32)
    mirror_ref[main : main + 8, :] = jnp.dot(
        edge_ref[main : main + 8, :], flip, precision=exact, preferred_element_type=f32
    )


def pack_kernel(
    ice_hbm, forcing_hbm, visc_hbm, mass_hbm, land_hbm, packed_ref,
    ice_ref, forcing_ref, visc_ref, mass_ref, land_ref, sems,
):
    copies = fetch(
        (ice_hbm, forcing_hbm, visc_hbm, mass_hbm, land_hbm),
        (ice_ref, forcing_ref, visc_ref, mass_ref, land_ref),
        sems,
    )
    width = visc_ref.shape[0]
    tiles = visc_ref.shape[1] // LANES
    tps = tiles // SEGS
    tile_x = lax.axis_index("gx") * width // TILE
    tile_y = lax.axis_index("gy") * tiles
    for copy in copies:
        copy.wait()
    for i in range(width // 8):
        rows = slice(8 * i, 8 * i + 8)
        for t in range(tiles):
            s, k = divmod(t, tps)
            cols = slice(t * LANES, (t + 1) * LANES)
            values = masked(
                ice_ref[tile_y + t, tile_x].astype(f32),
                visc_ref[rows, cols],
                mass_ref[rows, cols],
                land_ref[rows, cols],
                [forcing_ref[c, rows, cols] for c in range(2)],
            )
            for a, value in enumerate(values):
                tile = 8 * i * 2 * tps + (a // 2) * tps + k
                start = tile * 8 + (a % 2) * SEGS + s
                packed_ref[pl.ds(start, 8, stride=2 * tps * 8), :] = value


class Shifts:
    def __init__(self, tps):
        self.tps = tps
        self.span = (tps + 1) * LANES
        self.shape = (8, self.span)
        self.lane = iota(self.shape, 1)
        lane = iota((8, LANES), 1)
        row = iota((8, LANES), 0) & (SEGS - 1)
        self.first_half = lane < HALF
        self.low = iota((8, LANES), 0) < SEGS
        self.outer = ((row == SEGS - 1) & (lane < HALF)) | ((row == 0) & (lane >= HALF))
        bottom = lax.axis_index("gy") == 0
        wall = (iota(self.shape, 0) & (SEGS - 1) == 0) & (self.lane >= tps * LANES + HALF) & bottom
        self.weight = jnp.where(wall, 0.0, relax_weight)

    def roll(self, value, shift):
        return pltpu.roll(value, shift % self.span, 1)

    def odd(self, step):
        return self.lane & step != 0

    def pair(self, value, step):
        return value + jnp.where(self.odd(step), self.roll(value, step), self.roll(value, -step))

    def with_halo(self, parts, outside):
        inside = jnp.where(self.first_half, pltpu.roll(parts[0], 7, 0), pltpu.roll(parts[-1], 1, 0))
        return parts + [jnp.where(self.outer, outside, inside)]

    def rotations(self, cor_ref, line):
        parts = [cor_ref[pl.ds(k, SEGS, stride=self.tps), :] for k in range(self.tps)]
        parts = [jnp.concatenate([part, -part], 0) for part in parts]
        line = jnp.broadcast_to(line, (8, LANES))
        rotation = jnp.concatenate(self.with_halo(parts, jnp.where(self.low, line, -line)), 1)
        result = []
        for level in range(LEVELS):
            result.append(rotation)
            rotation = 0.5 * self.pair(rotation, 1 << level)
        return result

    def around(self, now, x, field, east, rotation, step):
        north = now["north"][x]
        west_nb, w, east_nb = field
        return (
            east[1] * east_nb
            + east[0] * west_nb
            + north * self.roll(w, -step)
            + self.roll(north * w, step)
            + rotation * other(w)
        )

    def coefficients(self, now, first, group, step):
        east = [now["east"][first + j - 1] for j in range(group + 1)]
        for j in range(group):
            x = first + j
            north = now["north"][x]
            diag = now["mass"][x] + east[j + 1] + east[j] + north + self.roll(north, step)
            scale = self.weight / diag
            now["scale"][x] = scale
            now["field"][x] = scale * now["right"][x]

    def coarse_east(self, now, fine, target, step):
        target[...] = 0.25 * self.pair(now["east"][fine + 1], step)

    def coarse_sums(self, now, coarse, fine, place, step):
        north = now["north"][fine] + now["north"][fine + 1]
        coarse["north"][place] = 0.25 * jnp.where(self.odd(step), north, self.roll(north, -step))
        coarse["mass"][place] = 0.25 * self.pair(now["mass"][fine] + now["mass"][fine + 1], step)

    def restrict(self, now, coarse, fine, place, group, rotation, step):
        field = [now["field"][fine + j - 1] for j in range(2 * group + 2)]
        east = [now["east"][fine + j - 1] for j in range(2 * group + 1)]
        rest = [
            (1.0 - relax_weight) * now["right"][fine + j]
            + self.around(now, fine + j, field[j : j + 3], east[j : j + 2], rotation, step)
            for j in range(2 * group)
        ]
        for j in range(group):
            coarse["right"][place + j] = 0.25 * self.pair(rest[2 * j] + rest[2 * j + 1], step)

    def sweep(self, now, first, group, value, rotation, step, put):
        field = [value(first + j - 1) for j in range(group + 2)]
        east = [now["east"][first + j - 1] for j in range(group + 1)]
        for j in range(group):
            x = first + j
            near = now["right"][x] + self.around(
                now, x, field[j : j + 3], east[j : j + 2], rotation, step
            )
            put(x, (1.0 - relax_weight) * field[j + 1] + now["scale"][x] * near)


def other(value):
    return pltpu.roll(value, SEGS, 0)


def loop(start, count, body, group=GROUP):
    whole, rest = divmod(count, group)
    if whole == 1:
        body(start, group)
    elif whole:
        lax.fori_loop(0, whole, lambda g, c: (body(start + g * group, group), c)[1], 0)
    if rest:
        body(start + whole * group, rest)


FIRST = ("north", "east", "scale", "right", "field")
STATE = FIRST + ("mass",)
COARSE = ("right", "east", "north", "mass")
AHEAD = ("done", "same", "side", "up", "down", "turn")


def faces(visc, east, first, group):
    value = [visc[first + j] for j in range(group + 1)]
    for j in range(group):
        east[first + j] = 0.5 * (value[j] + value[j + 1])


def unpack(move, visc, top, load, base, ext, index, x):
    tps = move.tps
    rows = [jnp.broadcast_to(ext[4 * index + a : 4 * index + a + 1], (8, LANES)) for a in range(4)]
    both = move.with_halo(
        [load(pl.ds(base + 8 * k, 8)) for k in range(tps)], jnp.where(move.low, rows[0], rows[1])
    )
    turned = [other(part) for part in both]
    value = jnp.concatenate([jnp.where(move.low, a, b) for a, b in zip(both, turned)], 1)
    visc[x] = value
    top["mass"][x] = jnp.concatenate([jnp.where(move.low, b, a) for a, b in zip(both, turned)], 1)
    top["right"][x] = jnp.concatenate(
        move.with_halo(
            [load(pl.ds(base + 8 * (tps + k), 8)) for k in range(tps)],
            jnp.where(move.low, rows[2], rows[3]),
        ),
        1,
    )
    top["north"][x] = 0.5 * (value + move.roll(value, -1))


def coarsen(move, now, coarse, first, group, skip, step, with_east=True, with_sums=True):
    for j in range(group):
        x = 2 * (first + j) + skip
        if with_east:
            coarse["east"][first + j] = 0.25 * move.pair(now["east"][x + 1], step)
        if with_sums:
            move.coarse_sums(now, coarse, x, first + j, step)


def put_packed(move, bottom, column, first, put):
    bit0, bit1 = move.odd(1), move.odd(2)
    names = ("east", "north", "mass")
    east, north, mass = (bottom[name][column] for name in names)
    right = jnp.zeros(move.shape, f32) if first else bottom["right"][column]
    value = jnp.where(bit1, jnp.where(bit0, mass, north), jnp.where(bit0, east, right))
    for k in range(move.tps + 1):
        put(k, value[:, k * LANES : (k + 1) * LANES])


def from_packed(move, value):
    bit0, bit1 = move.odd(1), move.odd(2)
    evens = jnp.where(bit0, move.roll(value, 1), value)
    odds = jnp.where(bit0, value, move.roll(value, -1))
    for name, part, upper in zip(COARSE, (evens, odds, evens, odds), (0, 0, 1, 1)):
        if upper:
            yield name, jnp.where(bit1, part, move.roll(part, -2))
        else:
            yield name, jnp.where(bit1, move.roll(part, 2), part)


def grouped(refs):
    levels = [dict(zip(STATE, refs[6 * n : 6 * n + 6])) for n in range(SPLIT)]
    levels.append(dict(zip(COARSE, refs[6 * SPLIT : 6 * SPLIT + 4])))
    return levels, refs[6 * SPLIT + 4]


KEPT = 6 * SPLIT + 5


def own_kernel(own_ref, swap_ref, folded_ref, wall_ref, cor_ref, *refs):
    tps = cor_ref.shape[0] // SEGS
    move = Shifts(tps)
    (top, level1, bottom), visc = grouped(refs)
    rot_ref, odd_ref, even_ref, ext_ref = refs[KEPT:]
    main = swap_ref.shape[0] - 8
    width = main // 4
    is_top = lax.axis_index("gy") == lax.axis_size("gy") - 1
    north = iota(swap_ref.shape, 1) < HALF
    swap = swap_ref[...]
    ext_ref[...] = jnp.where(
        north, jnp.where(is_top, folded_ref[...], swap), jnp.where(is_top, swap, wall_ref[...])
    )
    even = is_even()
    each = 2 * tps * 8
    side, total = FINE * each, width * each
    parts = (
        (slice(0, side), own_ref[0:side, :], own_ref[total - side : total, :]),
        (
            slice(side, side + 4 * FINE),
            ext_ref[0 : 4 * FINE, :],
            ext_ref[main - 4 * FINE : main, :],
        ),
    )
    for rows, low, high in parts:
        odd_ref[rows, :] = jnp.where(even, low, high)
        even_ref[rows, :] = jnp.where(even, high, low)
    rotations = move.rotations(cor_ref, ext_ref[main : main + 1, :])
    for level in range(LEVELS):
        rot_ref[level] = rotations[level]

    def own(first, group):
        for j in range(0, group, 2):
            x = first + j
            ext = ext_ref[pl.ds(pl.multiple_of(4 * x, 8), 8), :]
            for index in range(2):
                base = pl.multiple_of((x + index) * each, 8)
                unpack(
                    move, visc, top, lambda rows: own_ref[rows, :], base, ext, index, FINE + x + index
                )

    loop(0, width, own)
    loop(FINE, width - 1, lambda x, n: faces(visc, top["east"], x, n), 16)
    loop(FINE + 1, width - 2, lambda x, n: move.coefficients(top, x, n, 1), 10)
    skip, half, count = FINE // 2, width // 2, width >> SPLIT
    loop(skip, half - 1, lambda x, n: coarsen(move, top, level1, x, n, 0, 1), 15)
    coarsen(move, top, level1, skip + half - 1, 1, 0, 1, with_east=False)
    loop(
        skip + 1, half - 2, lambda x, n: move.restrict(top, level1, 2 * x, x, n, rotations[0], 1), 7
    )
    move.coefficients(level1, skip + 1, half - 2, 2)
    coarsen(move, level1, bottom, count, count - 1, skip - 2 * count, 2)
    coarsen(move, level1, bottom, 2 * count - 1, 1, skip - 2 * count, 2, with_east=False)
    move.restrict(level1, bottom, skip + 2, count + 1, count - 2, rotations[1], 2)
    for column in range(count - 1):

        def put(k, tile, column=column):
            row = side + 4 * FINE + (column * (tps + 1) + k) * 8
            odd_ref[row : row + 8, :] = tile
            even_ref[row : row + 8, :] = tile

        put_packed(move, bottom, count + column, column == 0, put)


def ahead_columns(move, now, ahead, rotation, level, place, group, parity=None):
    step = 1 << level
    parity = place % 2 if parity is None else parity
    x0 = place + (FINE >> level) - level
    field = [now["field"][x0 + j - 1] for j in range(group + 2)]
    east = [now["east"][x0 + j - 1] for j in range(group + 1)]
    for j in range(group):
        x, at = x0 + j, place + j
        scale = now["scale"][x]
        north = now["north"][x]
        near = now["right"][x] + move.around(now, x, field[j : j + 3], east[j : j + 2], rotation, step)
        ahead["done"][at] = (1.0 - relax_weight) * field[j + 1] + scale * near
        inner, outer = east[j + 1], east[j]
        if (parity + j + level) % 2:
            inner, outer = outer, inner
        ahead["same"][at] = (1.0 - relax_weight) + scale * inner
        ahead["side"][at] = scale * outer
        ahead["up"][at] = scale * north
        ahead["down"][at] = scale * move.roll(north, step)
        ahead["turn"][at] = scale * rotation


def aheads_of(refs):
    return [dict(zip(AHEAD, refs[6 * n : 6 * n + 6])) for n in range(SPLIT)]


def ahead_kernel(rot_ref, *refs):
    levels = [dict(zip(FIRST, refs[5 * n : 5 * n + 5])) for n in range(SPLIT)]
    aheads = aheads_of(refs[5 * SPLIT :])
    move = Shifts(rot_ref.shape[2] // LANES - 1)
    width = aheads[0]["done"].shape[0]
    loop(
        2,
        width - 4,
        lambda x, n: ahead_columns(move, levels[0], aheads[0], rot_ref[0], 0, x, n, parity=0),
        14,
    )
    loop(
        3,
        width // 2 - 4,
        lambda x, n: ahead_columns(move, levels[1], aheads[1], rot_ref[1], 1, x, n, parity=1),
        6,
    )


SECOND = ("scale", "field")
THIRD = ("right", "east", "north", "mass", "scale", "field")


def second_kernel(odd_ref, even_ref, rot_ref, *refs):
    out_hbm = refs[KEPT + 12]
    refs = list(refs[KEPT + 13 :])
    levels, visc = grouped(refs)
    aheads = aheads_of(refs[KEPT:])
    rest = refs[KEPT + 12 :]
    flat, out_ref, sems = rest[:3]
    levels[SPLIT].update(zip(SECOND, rest[3:5]))
    rest = rest[5:]
    for _ in range(SPLIT + 1, LEVELS):
        levels.append(dict(zip(THIRD, rest[:6])))
        rest = rest[6:]
    done = rest
    width = out_ref.shape[1]
    tps = out_ref.shape[2] // LANES // SEGS
    tiles = tps * SEGS
    move = Shifts(tps)
    rotations = [rot_ref[level] for level in range(LEVELS)]
    each = 2 * tps * 8
    even = is_even()
    columns = visc.shape[0]
    skip, half, count = FINE // 2, columns // 2, width >> SPLIT
    top, level1, now = levels[: SPLIT + 1]

    def from_left(rows):
        return jnp.where(even, odd_ref[rows, :], even_ref[rows, :])

    def from_right(rows):
        return jnp.where(even, even_ref[rows, :], odd_ref[rows, :])

    for load, start in ((from_left, 0), (from_right, FINE + width)):
        for j in range(0, FINE, 2):
            ext = load(pl.ds(FINE * each + 4 * j, 8))
            for index in range(2):
                unpack(move, visc, top, load, (j + index) * each, ext, index, start + j + index)
    for load, start, columns_sent in (
        (from_left, 0, range(count - 1)),
        (from_right, 2 * count, range(1, count - 1)),
    ):
        for column in columns_sent:
            row = FINE * (each + 4) + column * (tps + 1) * 8
            value = jnp.concatenate([load(pl.ds(row + 8 * k, 8)) for k in range(tps + 1)], 1)
            for name, part in from_packed(move, value):
                now[name][start + column] = part
    for start in (0, columns - 1 - FINE):
        faces(visc, top["east"], start, FINE)
    for start in (1, columns - 1 - FINE):
        move.coefficients(top, start, FINE, 1)
    for start in (0, half - 1 - skip):
        coarsen(move, top, level1, start, skip, 0, 1, with_sums=False)
    for start in (1, half - skip):
        coarsen(move, top, level1, start, skip - 1, 0, 1, with_east=False)
    for start in (1, half - 1 - skip):
        move.restrict(top, level1, 2 * start, start, skip, rotations[0], 1)
        move.coefficients(level1, start, skip, 2)
    for column in (count - 1, 2 * count):
        coarsen(move, level1, now, column, 1, skip - 2 * count, 2)
    coarsen(move, level1, now, 2 * count - 1, 1, skip - 2 * count, 2, with_sums=False)
    for column in (count - 1, 2 * count - 1):
        move.restrict(level1, now, 2 * column + skip - 2 * count, column, 2, rotations[1], 2)
    for place in (0, width - 2):
        ahead_columns(move, top, aheads[0], rotations[0], 0, place, 2)
    for place in (0, width // 2 - 1):
        ahead_columns(move, level1, aheads[1], rotations[1], 1, place, 3)
    total = 3 * count
    move.coefficients(now, 1, total - 2, 1 << SPLIT)
    for level in range(SPLIT, LEVELS - 1):
        now, coarse = levels[level], levels[level + 1]
        step = 1 << level
        half = total // 2
        for k in range(half - 1):
            coarse["east"][k] = 0.25 * move.pair(now["east"][2 * k + 1], step)
        for k in range(1, half - 1):
            move.coarse_sums(now, coarse, 2 * k, k, step)
        move.restrict(now, coarse, 2, 1, half - 2, rotations[level], step)
        total = half
        move.coefficients(coarse, 1, total - 2, 2 * step)

    def keep(target):
        def put(x, value):
            target[x] = value

        return put

    level = LEVELS - 1
    last, solved = levels[level], done.pop(0)
    own = width >> level
    move.sweep(
        last, own - 2, own + 4, lambda x: last["field"][x], rotations[level], 1 << level, keep(solved)
    )
    move.sweep(
        last, own - 1, own + 2, lambda x: solved[x], rotations[level], 1 << level, keep(last["field"])
    )
    solved, before = last["field"], own
    for level in reversed(range(SPLIT, LEVELS - 1)):
        now = levels[level]
        own = width >> level

        def value(x, now=now, solved=solved):
            return now["field"][x] + solved[lax.div(x, 2)]

        target = done.pop(0)
        move.sweep(now, own - 1, own + 2, value, rotations[level], 1 << level, keep(target))
        solved, before = target, own

    def correct(ahead, solved, first, count, place, step, put):
        for j in range(count):
            middle = solved[first + j]
            moved = (move.roll(middle, -step), move.roll(middle, step), other(middle))
            for child in range(2):
                x = place + 2 * j + child
                if isinstance(x, int) and not 0 <= x < ahead["done"].shape[0]:
                    continue
                result = (
                    ahead["done"][x]
                    + ahead["same"][x] * middle
                    + ahead["side"][x] * solved[first + j + 2 * child - 1]
                    + ahead["up"][x] * moved[0]
                    + ahead["down"][x] * moved[1]
                    + ahead["turn"][x] * moved[2]
                )
                put(x, result)

    target = done.pop(0)
    correct(aheads[1], solved, before - 1, (width >> SPLIT) + 2, -1, 2, keep(target))

    def put(x, result):
        for k in range(tps):
            row = pl.multiple_of((x * tps + k) * 8, 8)
            flat[pl.ds(row, 8), :] = result[:, k * LANES : (k + 1) * LANES]

    copies = []
    for i in range(width // 8):
        correct(aheads[0], target, 4 * i + 1, 4, 8 * i, 1, put)
        rows = pl.ds(8 * i, 8)
        for c in range(2):
            for t in range(tiles):
                s, k = divmod(t, tps)
                row = (8 * i * tps + k) * 8 + c * SEGS + s
                out_ref[c, rows, t * LANES : (t + 1) * LANES] = flat[pl.ds(row, 8, stride=tps * 8), :]
        copies.append(pltpu.make_async_copy(out_ref.at[:, rows, :], out_hbm.at[:, rows, :], sems.at[i]))
        copies[-1].start()
    for copy in copies:
        copy.wait()


def local(forcing, viscosity, mass, coriolis, land, ice_tiles):
    width, height = viscosity.shape
    tiles = height // LANES
    tps = tiles // SEGS
    each = 2 * tps * 8
    outside = 4 * width + 8
    gx, gy = lax.axis_size("gx"), lax.axis_size("gy")
    lines = coriolis.reshape(tiles, LANES)

    def here(*shape):
        return pltpu.VMEM(shape, f32)

    def call(kernel, outs, args, scratch=(), space=pltpu.VMEM, out_spaces=None, aliases={}):
        return pl.pallas_call(
            kernel,
            out_shape=outs,
            in_specs=[pl.BlockSpec(memory_space=space)] * len(args),
            out_specs=jax.tree.map(
                lambda _, where: pl.BlockSpec(memory_space=where),
                outs,
                out_spaces or jax.tree.map(lambda _: pltpu.VMEM, outs),
            ),
            scratch_shapes=scratch,
            input_output_aliases=aliases,
            compiler_params=pltpu.CompilerParams(vmem_limit_bytes=24 * 1024 * 1024),
        )(*(pltpu.with_memory_space_constraint(arg, space) for arg in args))

    sources = (ice_tiles.T, forcing, viscosity, mass, land, lines)
    ice_space = pltpu.SMEM(sources[0].shape, sources[0].dtype)
    edge, mirror, wall = call(
        ends_kernel,
        (here(outside, LANES),) * 3,
        sources,
        scratch=[ice_space, pltpu.VMEM(lines.shape, f32), pltpu.VMEM((2, 2, width, LANES), f32)]
        + [pltpu.VMEM((2, width, LANES), source.dtype) for source in sources[2:5]]
        + [pltpu.SemaphoreType.DMA((10,))],
        space=pltpu.HBM,
    )
    top = gy - 1
    folded = lax.ppermute(
        mirror, ("gx", "gy"), [(i * gy + top, (gx - 1 - i) * gy + top) for i in range(gx)]
    )
    swap = lax.ppermute(edge, "gy", [(i, gy - 1 - i) for i in range(gy)])
    packed = call(
        pack_kernel,
        here(width * each, LANES),
        sources[:5],
        scratch=[ice_space]
        + [pltpu.VMEM(source.shape, source.dtype) for source in sources[1:5]]
        + [pltpu.SemaphoreType.DMA((5,))],
        space=pltpu.HBM,
    )
    odd_pairs = [(i, (i + (1 if i % 2 else gx - 1)) % gx) for i in range(gx)]
    even_pairs = [(i, i ^ 1) for i in range(gx)]
    span = (tps + 1) * LANES
    columns = [(2 * FINE + width) >> level for level in range(SPLIT)]
    columns += [3 * width >> level for level in range(SPLIT, LEVELS)]
    count = width >> SPLIT

    def lines_of(number):
        return here(number, 8, span)

    kept = tuple(lines_of(columns[level]) for level in range(SPLIT) for _ in STATE)
    kept += (lines_of(columns[SPLIT]),) * len(COARSE) + (lines_of(columns[0]),)
    message = here(FINE * (each + 4) + (count - 1) * (tps + 1) * 8, LANES)
    *state, rotation, odd, even = call(
        own_kernel,
        kept + (lines_of(LEVELS), message, message),
        (packed, swap, folded, wall, lines),
        scratch=[here(outside, LANES)],
    )
    by_odd = lax.ppermute(odd, "gx", odd_pairs)
    by_even = lax.ppermute(even, "gx", even_pairs)
    ahead_shapes = (lines_of(width),) * len(AHEAD) + (lines_of(width // 2 + 2),) * len(AHEAD)
    ahead = call(
        ahead_kernel,
        ahead_shapes,
        (rotation, *(state[len(STATE) * level + n] for level in range(SPLIT) for n in range(len(FIRST)))),
    )
    out = jax.ShapeDtypeStruct((2, width, height), f32)
    return call(
        second_kernel,
        (out,) + kept + ahead_shapes,
        (by_odd, by_even, rotation, *state, *ahead),
        scratch=[
            pltpu.VMEM((width * tps * 8, LANES), f32),
            pltpu.VMEM((2, width, height), f32),
            pltpu.SemaphoreType.DMA((width // 8,)),
        ]
        + [lines_of(columns[SPLIT]) for _ in SECOND]
        + [lines_of(columns[level]) for level in range(SPLIT + 1, LEVELS) for _ in THIRD]
        + [lines_of(columns[level]) for level in reversed(range(SPLIT, LEVELS))]
        + [lines_of(width // 2 + 2)],
        out_spaces=(pltpu.HBM,) + (pltpu.VMEM,) * (KEPT + 12),
        aliases={3 + n: 1 + n for n in range(KEPT + 12)},
    )[0]


def solution(mesh):
    return jax.shard_map(
        local,
        mesh=mesh,
        in_specs=(
            P(None, ("groups", "gx"), "gy"),
            P(("groups", "gx"), "gy"),
            P(("groups", "gx"), "gy"),
            P("gy"),
            P("gx", "gy"),
            P("groups", None),
        ),
        out_specs=P(None, ("groups", "gx"), "gy"),
        check_vma=False,
    )
```

```python
import jax
import jax.numpy as jnp
from jax import lax
from jax.experimental import pallas as pl
from jax.experimental.pallas import tpu as pltpu
from jax.sharding import PartitionSpec as P


TILE = 128
LEVELS = 4
LANES = 128
SEGS = 4
HALF = LANES // 2
GROUP = 8

relax_weight = 0.8
land_mass = 4.0
f32 = jnp.float32
exact = lax.Precision.HIGHEST


FINE = 4
LEAD = 4
SPLIT = 2


def iota(shape, axis):
    return lax.broadcasted_iota(jnp.int32, shape, axis)


def is_even():
    return lax.axis_index("gx") & 1 == 0


def masked(ice, visc, mass, land, forcing):
    land = land.astype(f32)
    ocean = 1.0 - land
    return (
        visc * ice * ocean,
        mass * ocean + land_mass * land,
        forcing[0] * ocean,
        forcing[1] * ocean,
    )


def fetch(sources, held, sems):
    copies = [pltpu.make_async_copy(a, b, sems.at[n]) for n, (a, b) in enumerate(zip(sources, held))]
    for copy in copies:
        copy.start()
    return copies


def prepare_kernel(*refs):
    copies = fetch(refs[:6], refs[10:16], refs[16])
    packed_ref, edge_ref, mirror_ref, wall_ref = refs[6:10]
    ice_ref, forcing_ref, visc_ref, mass_ref, land_ref, cor_ref = refs[10:16]
    width = visc_ref.shape[0]
    tiles = visc_ref.shape[1] // LANES
    tps = tiles // SEGS
    tile_x = lax.axis_index("gx") * width // TILE
    tile_y = lax.axis_index("gy") * tiles
    lane = iota((8, LANES), 1)
    main = 4 * width
    flip = (iota((LANES, LANES), 0) + iota((LANES, LANES), 1) == LANES - 1).astype(f32)
    row, col = iota((main, main), 0), iota((main, main), 1)
    sign = jnp.where(row & 2 == 0, 1.0, -1.0)
    turn = jnp.where((row & 3 == col & 3) & ((row >> 2) + (col >> 2) == width - 1), sign, 0.0)
    wall_ref[main : main + 8, :] = jnp.zeros((8, LANES), f32)
    for copy in copies:
        copy.wait()
    for i in range(width // 8):
        rows = slice(8 * i, 8 * i + 8)
        ends = []
        for t in range(tiles):
            s, k = divmod(t, tps)
            cols = slice(t * LANES, (t + 1) * LANES)
            values = masked(
                ice_ref[tile_y + t, tile_x].astype(f32),
                visc_ref[rows, cols],
                mass_ref[rows, cols],
                land_ref[rows, cols],
                [forcing_ref[c, rows, cols] for c in range(2)],
            )
            for a, value in enumerate(values):
                tile = 8 * i * 2 * tps + (a // 2) * tps + k
                start = tile * 8 + (a % 2) * SEGS + s
                packed_ref[pl.ds(start, 8, stride=2 * tps * 8), :] = value
            if t in (0, tiles - 1):
                ends.append(values)
        for a in range(4):
            start = 8 * i * 4 + a
            edge_ref[pl.ds(start, 8, stride=4), :] = jnp.where(lane < HALF, ends[0][a], ends[1][a])
            if a == 0:
                wall = jnp.broadcast_to(ends[0][0][:, :1], (8, LANES))
            else:
                wall = jnp.full((8, LANES), 1.0 if a == 1 else 0.0, f32)
            wall_ref[pl.ds(start, 8, stride=4), :] = wall
    first, last = cor_ref[0:1, :], cor_ref[tiles - 1 : tiles, :]
    edge_ref[main : main + 8, :] = jnp.broadcast_to(
        jnp.where(lane[:1] < HALF, first, last), (8, LANES)
    )
    turned = jnp.dot(turn, edge_ref[0:main, :], precision=exact, preferred_element_type=f32)
    mirror_ref[0:main, :] = jnp.dot(turned, flip, precision=exact, preferred_element_type=f32)
    mirror_ref[main : main + 8, :] = jnp.dot(
        edge_ref[main : main + 8, :], flip, precision=exact, preferred_element_type=f32
    )


class Shifts:
    def __init__(self, tps):
        self.tps = tps
        self.span = (tps + 1) * LANES
        self.shape = (8, self.span)
        self.lane = iota(self.shape, 1)
        self.upper = iota(self.shape, 0) >= SEGS
        lane = iota((8, LANES), 1)
        row = iota((8, LANES), 0) & (SEGS - 1)
        self.first_half = lane < HALF
        self.low = iota((8, LANES), 0) < SEGS
        self.outer = ((row == SEGS - 1) & (lane < HALF)) | ((row == 0) & (lane >= HALF))
        bottom = lax.axis_index("gy") == 0
        wall = (iota(self.shape, 0) & (SEGS - 1) == 0) & (self.lane >= tps * LANES + HALF) & bottom
        self.weight = jnp.where(wall, 0.0, relax_weight)

    def roll(self, value, shift):
        return pltpu.roll(value, shift % self.span, 1)

    def odd(self, step):
        return self.lane & step != 0

    def pair(self, value, step):
        return value + jnp.where(self.odd(step), self.roll(value, step), self.roll(value, -step))

    def with_halo(self, parts, outside):
        inside = jnp.where(self.first_half, pltpu.roll(parts[0], 7, 0), pltpu.roll(parts[-1], 1, 0))
        return parts + [jnp.where(self.outer, outside, inside)]

    def rotations(self, cor_ref, line):
        parts = [cor_ref[pl.ds(k, SEGS, stride=self.tps), :] for k in range(self.tps)]
        parts = [jnp.concatenate([part, -part], 0) for part in parts]
        line = jnp.broadcast_to(line, (8, LANES))
        rotation = jnp.concatenate(self.with_halo(parts, jnp.where(self.low, line, -line)), 1)
        result = []
        for level in range(LEVELS):
            result.append(rotation)
            rotation = 0.5 * self.pair(rotation, 1 << level)
        return result

    def around(self, now, x, field, east, rotation, step):
        north = now["north"][x]
        west_nb, w, east_nb = field
        return (
            east[1] * east_nb
            + east[0] * west_nb
            + north * self.roll(w, -step)
            + self.roll(north * w, step)
            + rotation * other(w)
        )

    def coefficients(self, now, first, group, step):
        east = [now["east"][first + j - 1] for j in range(group + 1)]
        for j in range(group):
            x = first + j
            north = now["north"][x]
            diag = now["mass"][x] + east[j + 1] + east[j] + north + self.roll(north, step)
            scale = self.weight / diag
            now["scale"][x] = scale
            now["field"][x] = scale * now["right"][x]

    def coarse_east(self, now, fine, target, step):
        target[...] = 0.25 * self.pair(now["east"][fine + 1], step)

    def coarse_sums(self, now, coarse, fine, place, step):
        north = now["north"][fine] + now["north"][fine + 1]
        coarse["north"][place] = 0.25 * jnp.where(self.odd(step), north, self.roll(north, -step))
        coarse["mass"][place] = 0.25 * self.pair(now["mass"][fine] + now["mass"][fine + 1], step)

    def restrict(self, now, coarse, fine, place, group, rotation, step):
        field = [now["field"][fine + j - 1] for j in range(2 * group + 2)]
        east = [now["east"][fine + j - 1] for j in range(2 * group + 1)]
        rest = [
            (1.0 - relax_weight) * now["right"][fine + j]
            + self.around(now, fine + j, field[j : j + 3], east[j : j + 2], rotation, step)
            for j in range(2 * group)
        ]
        for j in range(group):
            coarse["right"][place + j] = 0.25 * self.pair(rest[2 * j] + rest[2 * j + 1], step)

    def sweep(self, now, first, group, value, rotation, step, put):
        field = [value(first + j - 1) for j in range(group + 2)]
        east = [now["east"][first + j - 1] for j in range(group + 1)]
        for j in range(group):
            x = first + j
            near = now["right"][x] + self.around(
                now, x, field[j : j + 3], east[j : j + 2], rotation, step
            )
            put(x, (1.0 - relax_weight) * field[j + 1] + now["scale"][x] * near)


def other(value):
    return pltpu.roll(value, SEGS, 0)


def loop(start, count, body, group=GROUP):
    whole, rest = divmod(count, group)
    if whole == 1:
        body(start, group)
    elif whole:
        lax.fori_loop(0, whole, lambda g, c: (body(start + g * group, group), c)[1], 0)
    if rest:
        body(start + whole * group, rest)


FIRST = ("north", "east", "scale", "right", "field")
STATE = FIRST + ("mass",)
COARSE = ("right", "east", "north", "mass")
AHEAD = ("done", "same", "side", "up", "down", "turn")


def faces(visc, east, first, group):
    value = [visc[first + j] for j in range(group + 1)]
    for j in range(group):
        east[first + j] = 0.5 * (value[j] + value[j + 1])


def unpack(move, visc, top, load, base, ext, index, x):
    tps = move.tps
    rows = [jnp.broadcast_to(ext[4 * index + a : 4 * index + a + 1], (8, LANES)) for a in range(4)]
    both = move.with_halo(
        [load(pl.ds(base + 8 * k, 8)) for k in range(tps)], jnp.where(move.low, rows[0], rows[1])
    )
    turned = [other(part) for part in both]
    value = jnp.concatenate([jnp.where(move.low, a, b) for a, b in zip(both, turned)], 1)
    visc[x] = value
    top["mass"][x] = jnp.concatenate([jnp.where(move.low, b, a) for a, b in zip(both, turned)], 1)
    top["right"][x] = jnp.concatenate(
        move.with_halo(
            [load(pl.ds(base + 8 * (tps + k), 8)) for k in range(tps)],
            jnp.where(move.low, rows[2], rows[3]),
        ),
        1,
    )
    top["north"][x] = 0.5 * (value + move.roll(value, -1))


def coarsen(move, now, coarse, first, group, skip, step, with_east=True, with_sums=True):
    for j in range(group):
        x = 2 * (first + j) + skip
        if with_east:
            coarse["east"][first + j] = 0.25 * move.pair(now["east"][x + 1], step)
        if with_sums:
            move.coarse_sums(now, coarse, x, first + j, step)


def evens_of(move, value):
    return jnp.where(move.odd(1), move.roll(value, 1), value)


def odds_of(move, value):
    return jnp.where(move.odd(1), value, move.roll(value, -1))


def put_packed(move, bottom, column, first, put):
    bit0, bit1 = move.odd(1), move.odd(2)
    names = ("east", "north", "mass")
    east, north, mass = (bottom[name][column] for name in names)
    right = jnp.zeros(move.shape, f32) if first else bottom["right"][column]
    put(jnp.where(bit1, jnp.where(bit0, mass, north), jnp.where(bit0, east, right)))


def from_packed(move, value):
    bit1 = move.odd(2)
    evens, odds = evens_of(move, value), odds_of(move, value)
    for name, part, upper in zip(COARSE, (evens, odds, evens, odds), (0, 0, 1, 1)):
        if upper:
            yield name, jnp.where(bit1, part, move.roll(part, -2))
        else:
            yield name, jnp.where(bit1, move.roll(part, 2), part)


def middle_packed(move, level1, column):
    bit0 = move.odd(1)
    values = []
    for x in (column, column + 1):
        coefficients = jnp.where(move.upper, level1["north"][x], level1["east"][x])
        values.append(jnp.where(bit0, coefficients, level1["right"][x]))
    masses = jnp.where(move.upper, level1["mass"][column + 1], level1["mass"][column])
    return values + [jnp.where(bit0, level1["east"][column - 1], masses)]


def middle_unpacked(move, level1, column, values, west):
    for x, value in zip((column, column + 1), values):
        level1["right"][x] = evens_of(move, value)
        both = odds_of(move, value)
        turned = other(both)
        level1["east"][x] = jnp.where(move.upper, turned, both)
        level1["north"][x] = jnp.where(move.upper, both, turned)
    both = evens_of(move, values[2])
    turned = other(both)
    level1["mass"][column] = jnp.where(move.upper, turned, both)
    level1["mass"][column + 1] = jnp.where(move.upper, both, turned)
    if west:
        level1["east"][column - 1] = odds_of(move, values[2])


def grouped(refs):
    levels = [dict(zip(STATE, refs[6 * n : 6 * n + 6])) for n in range(SPLIT)]
    levels.append(dict(zip(COARSE, refs[6 * SPLIT : 6 * SPLIT + 4])))
    return levels, refs[6 * SPLIT + 4]


KEPT = 6 * SPLIT + 5


def own_kernel(own_ref, swap_ref, folded_ref, wall_ref, cor_ref, *refs):
    tps = cor_ref.shape[0] // SEGS
    move = Shifts(tps)
    (top, level1, bottom), visc = grouped(refs)
    rot_ref, odd_ref, even_ref, ext_ref = refs[KEPT:]
    main = swap_ref.shape[0] - 8
    width = main // 4
    is_top = lax.axis_index("gy") == lax.axis_size("gy") - 1
    north = iota(swap_ref.shape, 1) < HALF
    swap = swap_ref[...]
    ext_ref[...] = jnp.where(
        north, jnp.where(is_top, folded_ref[...], swap), jnp.where(is_top, swap, wall_ref[...])
    )
    even = is_even()
    each = 2 * tps * 8
    side, total = FINE * each, width * each
    parts = (
        (slice(0, side), own_ref[0:side, :], own_ref[total - side : total, :]),
        (
            slice(side, side + 4 * FINE),
            ext_ref[0 : 4 * FINE, :],
            ext_ref[main - 4 * FINE : main, :],
        ),
    )
    for rows, low, high in parts:
        odd_ref[rows, :] = jnp.where(even, low, high)
        even_ref[rows, :] = jnp.where(even, high, low)
    rotations = move.rotations(cor_ref, ext_ref[main : main + 1, :])
    for level in range(LEVELS):
        rot_ref[level] = rotations[level]

    def own(first, group):
        for j in range(0, group, 2):
            x = first + j
            ext = ext_ref[pl.ds(pl.multiple_of(4 * x, 8), 8), :]
            for index in range(2):
                base = pl.multiple_of((x + index) * each, 8)
                unpack(
                    move, visc, top, lambda rows: own_ref[rows, :], base, ext, index, FINE + x + index
                )

    loop(0, width, own)
    loop(FINE, width - 1, lambda x, n: faces(visc, top["east"], x, n), 16)
    loop(FINE + 1, width - 2, lambda x, n: move.coefficients(top, x, n, 1), 10)
    skip, half, count = FINE - 2 * LEAD, width // 2, width >> SPLIT
    loop(LEAD, half - 1, lambda x, n: coarsen(move, top, level1, x, n, skip, 1), 15)
    coarsen(move, top, level1, LEAD + half - 1, 1, skip, 1, with_east=False)
    loop(
        LEAD + 1,
        half - 2,
        lambda x, n: move.restrict(top, level1, 2 * x + skip, x, n, rotations[0], 1),
        7,
    )
    move.coefficients(level1, LEAD + 1, half - 2, 2)
    skip = LEAD - 2 * count
    coarsen(move, level1, bottom, count, count - 1, skip, 2)
    coarsen(move, level1, bottom, 2 * count - 1, 1, skip, 2, with_east=False)
    move.restrict(level1, bottom, LEAD + 2, count + 1, count - 2, rotations[1], 2)

    def put(ref, column, value):
        for k in range(tps + 1):
            row = side + 4 * FINE + (column * (tps + 1) + k) * 8
            ref[row : row + 8, :] = value[:, k * LANES : (k + 1) * LANES]

    lows = middle_packed(move, level1, LEAD + 1)
    highs = middle_packed(move, level1, LEAD + half - 3)
    for n, (low, high) in enumerate(zip(lows, highs)):
        put(odd_ref, n, jnp.where(even, low, high))
        put(even_ref, n, jnp.where(even, high, low))
    for column in range(count - 1):

        def put_both(value, column=column):
            put(odd_ref, 3 + column, value)
            put(even_ref, 3 + column, value)

        put_packed(move, bottom, count + column, column == 0, put_both)


def ahead_columns(move, now, ahead, rotation, level, place, group, parity=None):
    step = 1 << level
    parity = place % 2 if parity is None else parity
    x0 = place + (FINE, LEAD - 1)[level]
    field = [now["field"][x0 + j - 1] for j in range(group + 2)]
    east = [now["east"][x0 + j - 1] for j in range(group + 1)]
    for j in range(group):
        x, at = x0 + j, place + j
        scale = now["scale"][x]
        north = now["north"][x]
        near = now["right"][x] + move.around(now, x, field[j : j + 3], east[j : j + 2], rotation, step)
        ahead["done"][at] = (1.0 - relax_weight) * field[j + 1] + scale * near
        inner, outer = east[j + 1], east[j]
        if (parity + j + level) % 2:
            inner, outer = outer, inner
        ahead["same"][at] = (1.0 - relax_weight) + scale * inner
        ahead["side"][at] = scale * outer
        ahead["up"][at] = scale * north
        ahead["down"][at] = scale * move.roll(north, step)
        ahead["turn"][at] = scale * rotation


def aheads_of(refs):
    return [dict(zip(AHEAD, refs[6 * n : 6 * n + 6])) for n in range(SPLIT)]


def ahead_kernel(rot_ref, *refs):
    levels = [dict(zip(FIRST, refs[5 * n : 5 * n + 5])) for n in range(SPLIT)]
    aheads = aheads_of(refs[5 * SPLIT :])
    move = Shifts(rot_ref.shape[2] // LANES - 1)
    width = aheads[0]["done"].shape[0]
    loop(
        2,
        width - 4,
        lambda x, n: ahead_columns(move, levels[0], aheads[0], rot_ref[0], 0, x, n, parity=0),
        14,
    )
    loop(
        3,
        width // 2 - 4,
        lambda x, n: ahead_columns(move, levels[1], aheads[1], rot_ref[1], 1, x, n, parity=1),
        6,
    )


SECOND = ("scale", "field")
THIRD = ("right", "east", "north", "mass", "scale", "field")


def second_kernel(odd_ref, even_ref, rot_ref, *refs):
    out_hbm = refs[KEPT + 12]
    refs = list(refs[KEPT + 13 :])
    levels, visc = grouped(refs)
    aheads = aheads_of(refs[KEPT:])
    rest = refs[KEPT + 12 :]
    flat, out_ref, sems = rest[:3]
    levels[SPLIT].update(zip(SECOND, rest[3:5]))
    rest = rest[5:]
    for _ in range(SPLIT + 1, LEVELS):
        levels.append(dict(zip(THIRD, rest[:6])))
        rest = rest[6:]
    done = rest
    width = out_ref.shape[1]
    tps = out_ref.shape[2] // LANES // SEGS
    tiles = tps * SEGS
    move = Shifts(tps)
    rotations = [rot_ref[level] for level in range(LEVELS)]
    each = 2 * tps * 8
    even = is_even()
    columns, count, half = visc.shape[0], width >> SPLIT, width // 2
    top, level1, now = levels[: SPLIT + 1]

    def from_left(rows):
        return jnp.where(even, odd_ref[rows, :], even_ref[rows, :])

    def from_right(rows):
        return jnp.where(even, even_ref[rows, :], odd_ref[rows, :])

    for load, start in ((from_left, 0), (from_right, FINE + width)):
        for j in range(0, FINE, 2):
            ext = load(pl.ds(FINE * each + 4 * j, 8))
            for index in range(2):
                unpack(move, visc, top, load, (j + index) * each, ext, index, start + j + index)

    def received(load, column):
        row = FINE * (each + 4) + column * (tps + 1) * 8
        return jnp.concatenate([load(pl.ds(row + 8 * k, 8)) for k in range(tps + 1)], 1)

    middle_unpacked(move, level1, 1, [received(from_left, n) for n in range(3)], True)
    middle_unpacked(
        move, level1, LEAD + half + 1, [received(from_right, n) for n in range(3)], False
    )
    for load, start, columns_sent in (
        (from_left, 0, range(count - 1)),
        (from_right, 2 * count, range(1, count - 1)),
    ):
        for column in columns_sent:
            for name, part in from_packed(move, received(load, 3 + column)):
                now[name][start + column] = part
    for start in (0, columns - 1 - FINE):
        faces(visc, top["east"], start, FINE)
    for start in (1, columns - 1 - FINE):
        move.coefficients(top, start, FINE, 1)
    skip = FINE - 2 * LEAD
    for column in (LEAD - 1, LEAD + half):
        coarsen(move, top, level1, column, 1, skip, 1)
    coarsen(move, top, level1, LEAD + half - 1, 1, skip, 1, with_sums=False)
    for column in (LEAD - 1, LEAD + half - 1):
        move.restrict(top, level1, 2 * column + skip, column, 2, rotations[0], 1)
    for column in (1, LEAD + half - 1):
        move.coefficients(level1, column, 4, 2)
    skip = LEAD - 2 * count
    for column in (count - 1, 2 * count):
        coarsen(move, level1, now, column, 1, skip, 2)
    coarsen(move, level1, now, 2 * count - 1, 1, skip, 2, with_sums=False)
    for column in (count - 1, 2 * count - 1):
        move.restrict(level1, now, 2 * column + skip, column, 2, rotations[1], 2)
    for place in (0, width - 2):
        ahead_columns(move, top, aheads[0], rotations[0], 0, place, 2)
    for place in (0, width // 2 - 1):
        ahead_columns(move, level1, aheads[1], rotations[1], 1, place, 3)
    total = 3 * count
    move.coefficients(now, 1, total - 2, 1 << SPLIT)
    for level in range(SPLIT, LEVELS - 1):
        now, coarse = levels[level], levels[level + 1]
        step = 1 << level
        half = total // 2
        for k in range(half - 1):
            coarse["east"][k] = 0.25 * move.pair(now["east"][2 * k + 1], step)
        for k in range(1, half - 1):
            move.coarse_sums(now, coarse, 2 * k, k, step)
        move.restrict(now, coarse, 2, 1, half - 2, rotations[level], step)
        total = half
        move.coefficients(coarse, 1, total - 2, 2 * step)

    def keep(target):
        def put(x, value):
            target[x] = value

        return put

    level = LEVELS - 1
    last, solved = levels[level], done.pop(0)
    own = width >> level
    move.sweep(
        last, own - 2, own + 4, lambda x: last["field"][x], rotations[level], 1 << level, keep(solved)
    )
    move.sweep(
        last, own - 1, own + 2, lambda x: solved[x], rotations[level], 1 << level, keep(last["field"])
    )
    solved, before = last["field"], own
    for level in reversed(range(SPLIT, LEVELS - 1)):
        now = levels[level]
        own = width >> level

        def value(x, now=now, solved=solved):
            return now["field"][x] + solved[lax.div(x, 2)]

        target = done.pop(0)
        move.sweep(now, own - 1, own + 2, value, rotations[level], 1 << level, keep(target))
        solved, before = target, own

    def correct(ahead, solved, first, count, place, step, put):
        for j in range(count):
            middle = solved[first + j]
            moved = (move.roll(middle, -step), move.roll(middle, step), other(middle))
            for child in range(2):
                x = place + 2 * j + child
                if isinstance(x, int) and not 0 <= x < ahead["done"].shape[0]:
                    continue
                result = (
                    ahead["done"][x]
                    + ahead["same"][x] * middle
                    + ahead["side"][x] * solved[first + j + 2 * child - 1]
                    + ahead["up"][x] * moved[0]
                    + ahead["down"][x] * moved[1]
                    + ahead["turn"][x] * moved[2]
                )
                put(x, result)

    target = done.pop(0)
    correct(aheads[1], solved, before - 1, (width >> SPLIT) + 2, -1, 2, keep(target))

    def put(x, result):
        for k in range(tps):
            row = pl.multiple_of((x * tps + k) * 8, 8)
            flat[pl.ds(row, 8), :] = result[:, k * LANES : (k + 1) * LANES]

    copies = []
    for i in range(width // 8):
        correct(aheads[0], target, 4 * i + 1, 4, 8 * i, 1, put)
        rows = pl.ds(8 * i, 8)
        for c in range(2):
            for t in range(tiles):
                s, k = divmod(t, tps)
                row = (8 * i * tps + k) * 8 + c * SEGS + s
                out_ref[c, rows, t * LANES : (t + 1) * LANES] = flat[pl.ds(row, 8, stride=tps * 8), :]
        copies.append(pltpu.make_async_copy(out_ref.at[:, rows, :], out_hbm.at[:, rows, :], sems.at[i]))
        copies[-1].start()
    for copy in copies:
        copy.wait()


def local(forcing, viscosity, mass, coriolis, land, ice_tiles):
    width, height = viscosity.shape
    tiles = height // LANES
    tps = tiles // SEGS
    each = 2 * tps * 8
    outside = 4 * width + 8
    gx, gy = lax.axis_size("gx"), lax.axis_size("gy")
    lines = coriolis.reshape(tiles, LANES)

    def here(*shape):
        return pltpu.VMEM(shape, f32)

    def call(kernel, outs, args, scratch=(), space=pltpu.VMEM, out_spaces=None, aliases={}):
        return pl.pallas_call(
            kernel,
            out_shape=outs,
            in_specs=[pl.BlockSpec(memory_space=space)] * len(args),
            out_specs=jax.tree.map(
                lambda _, where: pl.BlockSpec(memory_space=where),
                outs,
                out_spaces or jax.tree.map(lambda _: pltpu.VMEM, outs),
            ),
            scratch_shapes=scratch,
            input_output_aliases=aliases,
            compiler_params=pltpu.CompilerParams(vmem_limit_bytes=24 * 1024 * 1024),
        )(*(pltpu.with_memory_space_constraint(arg, space) for arg in args))

    sources = (ice_tiles.T, forcing, viscosity, mass, land, lines)
    packed, edge, mirror, wall = call(
        prepare_kernel,
        (here(width * each, LANES),) + (here(outside, LANES),) * 3,
        sources,
        scratch=[pltpu.SMEM(sources[0].shape, sources[0].dtype)]
        + [pltpu.VMEM(source.shape, source.dtype) for source in sources[1:]]
        + [pltpu.SemaphoreType.DMA((len(sources),))],
        space=pltpu.HBM,
    )
    top = gy - 1
    folded = lax.ppermute(
        mirror, ("gx", "gy"), [(i * gy + top, (gx - 1 - i) * gy + top) for i in range(gx)]
    )
    swap = lax.ppermute(edge, "gy", [(i, gy - 1 - i) for i in range(gy)])
    odd_pairs = [(i, (i + (1 if i % 2 else gx - 1)) % gx) for i in range(gx)]
    even_pairs = [(i, i ^ 1) for i in range(gx)]
    span = (tps + 1) * LANES
    columns = [2 * FINE + width, 2 * LEAD + width // 2]
    columns += [3 * width >> level for level in range(SPLIT, LEVELS)]
    count = width >> SPLIT

    def lines_of(number):
        return here(number, 8, span)

    kept = tuple(lines_of(columns[level]) for level in range(SPLIT) for _ in STATE)
    kept += (lines_of(columns[SPLIT]),) * len(COARSE) + (lines_of(columns[0]),)
    message = here(FINE * (each + 4) + (count + 2) * (tps + 1) * 8, LANES)
    *state, rotation, odd, even = call(
        own_kernel,
        kept + (lines_of(LEVELS), message, message),
        (packed, swap, folded, wall, lines),
        scratch=[here(outside, LANES)],
    )
    by_odd = lax.ppermute(odd, "gx", odd_pairs)
    by_even = lax.ppermute(even, "gx", even_pairs)
    ahead_shapes = (lines_of(width),) * len(AHEAD) + (lines_of(width // 2 + 2),) * len(AHEAD)
    ahead = call(
        ahead_kernel,
        ahead_shapes,
        (rotation, *(state[len(STATE) * level + n] for level in range(SPLIT) for n in range(len(FIRST)))),
    )
    out = jax.ShapeDtypeStruct((2, width, height), f32)
    return call(
        second_kernel,
        (out,) + kept + ahead_shapes,
        (by_odd, by_even, rotation, *state, *ahead),
        scratch=[
            pltpu.VMEM((width * tps * 8, LANES), f32),
            pltpu.VMEM((2, width, height), f32),
            pltpu.SemaphoreType.DMA((width // 8,)),
        ]
        + [lines_of(columns[SPLIT]) for _ in SECOND]
        + [lines_of(columns[level]) for level in range(SPLIT + 1, LEVELS) for _ in THIRD]
        + [lines_of(columns[level]) for level in reversed(range(SPLIT, LEVELS))]
        + [lines_of(width // 2 + 2)],
        out_spaces=(pltpu.HBM,) + (pltpu.VMEM,) * (KEPT + 12),
        aliases={3 + n: 1 + n for n in range(KEPT + 12)},
    )[0]


def solution(mesh):
    return jax.shard_map(
        local,
        mesh=mesh,
        in_specs=(
            P(None, ("groups", "gx"), "gy"),
            P(("groups", "gx"), "gy"),
            P(("groups", "gx"), "gy"),
            P("gy"),
            P("gx", "gy"),
            P("groups", None),
        ),
        out_specs=P(None, ("groups", "gx"), "gy"),
        check_vma=False,
    )
```

```python
import jax
import jax.numpy as jnp
from jax import lax
from jax.experimental import pallas as pl
from jax.experimental.pallas import tpu as pltpu
from jax.sharding import PartitionSpec as P


TILE = 128
LEVELS = 4
LANES = 128
SEGS = 4
HALF = LANES // 2
GROUP = 8

relax_weight = 0.8
land_mass = 4.0
f32 = jnp.float32
exact = lax.Precision.HIGHEST


FINE = 4
LEAD = 4
SPLIT = 2


def iota(shape, axis):
    return lax.broadcasted_iota(jnp.int32, shape, axis)


def is_even():
    return lax.axis_index("gx") & 1 == 0


def masked(ice, visc, mass, land, forcing):
    land = land.astype(f32)
    ocean = 1.0 - land
    return (
        visc * ice * ocean,
        mass * ocean + land_mass * land,
        forcing[0] * ocean,
        forcing[1] * ocean,
    )


def fetch(sources, held, sems):
    copies = [pltpu.make_async_copy(a, b, sems.at[n]) for n, (a, b) in enumerate(zip(sources, held))]
    for copy in copies:
        copy.start()
    return copies


def prepare_kernel(*refs):
    held = (refs[15],) + refs[9:14]
    copies = fetch(refs[:6], held, refs[16])
    edge_ref, mirror_ref, wall_ref, ice_ref = refs[6:9] + refs[14:15]
    forcing_ref, visc_ref, mass_ref, land_ref, cor_ref = refs[9:14]
    ice_place = refs[15]
    width = visc_ref.shape[0]
    tiles = visc_ref.shape[1] // LANES
    tile_x = lax.axis_index("gx") * width // TILE
    tile_y = lax.axis_index("gy") * tiles
    lane = iota((8, LANES), 1)
    main = 4 * width
    flip = (iota((LANES, LANES), 0) + iota((LANES, LANES), 1) == LANES - 1).astype(f32)
    row, col = iota((main, main), 0), iota((main, main), 1)
    sign = jnp.where(row & 2 == 0, 1.0, -1.0)
    turn = jnp.where((row & 3 == col & 3) & ((row >> 2) + (col >> 2) == width - 1), sign, 0.0)
    wall_ref[main : main + 8, :] = jnp.zeros((8, LANES), f32)
    for copy in copies:
        copy.wait()
    for t in range(tiles):
        ice_ref[8 * t : 8 * t + 8, :] = jnp.full((8, LANES), ice_place[tile_y + t, tile_x].astype(f32), f32)
    for i in range(width // 8):
        rows = slice(8 * i, 8 * i + 8)
        ends = []
        for t in (0, tiles - 1):
            cols = slice(t * LANES, (t + 1) * LANES)
            ends.append(
                masked(
                    ice_place[tile_y + t, tile_x].astype(f32),
                    visc_ref[rows, cols],
                    mass_ref[rows, cols],
                    land_ref[rows, cols],
                    [forcing_ref[c, rows, cols] for c in range(2)],
                )
            )
        for a in range(4):
            start = 8 * i * 4 + a
            edge_ref[pl.ds(start, 8, stride=4), :] = jnp.where(lane < HALF, ends[0][a], ends[1][a])
            if a == 0:
                wall = jnp.broadcast_to(ends[0][0][:, :1], (8, LANES))
            else:
                wall = jnp.full((8, LANES), 1.0 if a == 1 else 0.0, f32)
            wall_ref[pl.ds(start, 8, stride=4), :] = wall
    first, last = cor_ref[0:1, :], cor_ref[tiles - 1 : tiles, :]
    edge_ref[main : main + 8, :] = jnp.broadcast_to(
        jnp.where(lane[:1] < HALF, first, last), (8, LANES)
    )
    turned = jnp.dot(turn, edge_ref[0:main, :], precision=exact, preferred_element_type=f32)
    mirror_ref[0:main, :] = jnp.dot(turned, flip, precision=exact, preferred_element_type=f32)
    mirror_ref[main : main + 8, :] = jnp.dot(
        edge_ref[main : main + 8, :], flip, precision=exact, preferred_element_type=f32
    )


def pack_kernel(forcing_ref, visc_ref, mass_ref, land_ref, ice_ref, packed_ref):
    width = visc_ref.shape[0]
    tiles = visc_ref.shape[1] // LANES
    tps = tiles // SEGS
    for i in range(width // 8):
        rows = slice(8 * i, 8 * i + 8)
        for t in range(tiles):
            s, k = divmod(t, tps)
            cols = slice(t * LANES, (t + 1) * LANES)
            values = masked(
                ice_ref[8 * t : 8 * t + 8, :],
                visc_ref[rows, cols],
                mass_ref[rows, cols],
                land_ref[rows, cols],
                [forcing_ref[c, rows, cols] for c in range(2)],
            )
            for a, value in enumerate(values):
                tile = 8 * i * 2 * tps + (a // 2) * tps + k
                start = tile * 8 + (a % 2) * SEGS + s
                packed_ref[pl.ds(start, 8, stride=2 * tps * 8), :] = value


class Shifts:
    def __init__(self, tps):
        self.tps = tps
        self.span = (tps + 1) * LANES
        self.shape = (8, self.span)
        self.lane = iota(self.shape, 1)
        self.upper = iota(self.shape, 0) >= SEGS
        lane = self.lane1 = iota((8, LANES), 1)
        row = iota((8, LANES), 0) & (SEGS - 1)
        self.first_half = lane < HALF
        self.low = iota((8, LANES), 0) < SEGS
        self.outer = ((row == SEGS - 1) & (lane < HALF)) | ((row == 0) & (lane >= HALF))
        bottom = lax.axis_index("gy") == 0
        wall = (iota(self.shape, 0) & (SEGS - 1) == 0) & (self.lane >= tps * LANES + HALF) & bottom
        self.weight = jnp.where(wall, 0.0, relax_weight)

    def roll(self, value, shift):
        return pltpu.roll(value, shift % self.span, 1)

    def odd(self, step):
        return self.lane & step != 0

    def take(self, value, index):
        tiles = [value[:, k * LANES : (k + 1) * LANES] for k in range(self.tps + 1)]
        return jnp.concatenate([jnp.take_along_axis(tile, index, axis=1) for tile in tiles], 1)

    def pair(self, value, step):
        return value + self.take(value, self.lane1 ^ step)

    def with_halo(self, parts, outside):
        inside = jnp.where(self.first_half, pltpu.roll(parts[0], 7, 0), pltpu.roll(parts[-1], 1, 0))
        return parts + [jnp.where(self.outer, outside, inside)]

    def rotations(self, cor_ref, line):
        parts = [cor_ref[pl.ds(k, SEGS, stride=self.tps), :] for k in range(self.tps)]
        parts = [jnp.concatenate([part, -part], 0) for part in parts]
        line = jnp.broadcast_to(line, (8, LANES))
        rotation = jnp.concatenate(self.with_halo(parts, jnp.where(self.low, line, -line)), 1)
        result = []
        for level in range(LEVELS):
            result.append(rotation)
            rotation = 0.5 * self.pair(rotation, 1 << level)
        return result

    def around(self, now, x, field, east, rotation, step):
        north = now["north"][x]
        west_nb, w, east_nb = field
        return (
            east[1] * east_nb
            + east[0] * west_nb
            + north * self.roll(w, -step)
            + self.roll(north * w, step)
            + rotation * other(w)
        )

    def coefficients(self, now, first, group, step):
        east = [now["east"][first + j - 1] for j in range(group + 1)]
        for j in range(group):
            x = first + j
            north = now["north"][x]
            diag = now["mass"][x] + east[j + 1] + east[j] + north + self.roll(north, step)
            scale = self.weight / diag
            now["scale"][x] = scale
            now["field"][x] = scale * now["right"][x]

    def coarse_east(self, now, fine, target, step):
        target[...] = 0.25 * self.pair(now["east"][fine + 1], step)

    def coarse_sums(self, now, coarse, fine, place, step):
        north = now["north"][fine] + now["north"][fine + 1]
        coarse["north"][place] = 0.25 * self.take(north, self.lane1 | step)
        coarse["mass"][place] = 0.25 * self.pair(now["mass"][fine] + now["mass"][fine + 1], step)

    def restrict(self, now, coarse, fine, place, group, rotation, step):
        field = [now["field"][fine + j - 1] for j in range(2 * group + 2)]
        east = [now["east"][fine + j - 1] for j in range(2 * group + 1)]
        rest = [
            (1.0 - relax_weight) * now["right"][fine + j]
            + self.around(now, fine + j, field[j : j + 3], east[j : j + 2], rotation, step)
            for j in range(2 * group)
        ]
        for j in range(group):
            coarse["right"][place + j] = 0.25 * self.pair(rest[2 * j] + rest[2 * j + 1], step)

    def sweep(self, now, first, group, value, rotation, step, put):
        field = [value(first + j - 1) for j in range(group + 2)]
        east = [now["east"][first + j - 1] for j in range(group + 1)]
        for j in range(group):
            x = first + j
            near = now["right"][x] + self.around(
                now, x, field[j : j + 3], east[j : j + 2], rotation, step
            )
            put(x, (1.0 - relax_weight) * field[j + 1] + now["scale"][x] * near)


def other(value):
    return pltpu.roll(value, SEGS, 0)


def loop(start, count, body, group=GROUP):
    whole, rest = divmod(count, group)
    if whole == 1:
        body(start, group)
    elif whole:
        lax.fori_loop(0, whole, lambda g, c: (body(start + g * group, group), c)[1], 0)
    if rest:
        body(start + whole * group, rest)


FIRST = ("north", "east", "scale", "right", "field")
STATE = FIRST + ("mass",)
COARSE = ("right", "east", "north", "mass")
AHEAD = ("done", "same", "side", "up", "down", "turn")


def faces(visc, east, first, group):
    value = [visc[first + j] for j in range(group + 1)]
    for j in range(group):
        east[first + j] = 0.5 * (value[j] + value[j + 1])


def unpack(move, visc, top, load, base, ext, index, x):
    tps = move.tps
    rows = [jnp.broadcast_to(ext[4 * index + a : 4 * index + a + 1], (8, LANES)) for a in range(4)]
    both = move.with_halo(
        [load(pl.ds(base + 8 * k, 8)) for k in range(tps)], jnp.where(move.low, rows[0], rows[1])
    )
    turned = [other(part) for part in both]
    value = jnp.concatenate([jnp.where(move.low, a, b) for a, b in zip(both, turned)], 1)
    visc[x] = value
    top["mass"][x] = jnp.concatenate([jnp.where(move.low, b, a) for a, b in zip(both, turned)], 1)
    top["right"][x] = jnp.concatenate(
        move.with_halo(
            [load(pl.ds(base + 8 * (tps + k), 8)) for k in range(tps)],
            jnp.where(move.low, rows[2], rows[3]),
        ),
        1,
    )
    top["north"][x] = 0.5 * (value + move.roll(value, -1))


def coarsen(move, now, coarse, first, group, skip, step, with_east=True, with_sums=True):
    for j in range(group):
        x = 2 * (first + j) + skip
        if with_east:
            coarse["east"][first + j] = 0.25 * move.pair(now["east"][x + 1], step)
        if with_sums:
            move.coarse_sums(now, coarse, x, first + j, step)


def evens_of(move, value):
    return move.take(value, move.lane1 & ~1)


def odds_of(move, value):
    return move.take(value, move.lane1 | 1)


def put_packed(move, bottom, column, first, put):
    bit0, bit1 = move.odd(1), move.odd(2)
    names = ("east", "north", "mass")
    east, north, mass = (bottom[name][column] for name in names)
    right = jnp.zeros(move.shape, f32) if first else bottom["right"][column]
    put(jnp.where(bit1, jnp.where(bit0, mass, north), jnp.where(bit0, east, right)))


def from_packed(move, value):
    for n, name in enumerate(COARSE):
        yield name, move.take(value, (move.lane1 & ~3) | n)


def middle_packed(move, level1, column):
    bit0 = move.odd(1)
    values = []
    for x in (column, column + 1):
        coefficients = jnp.where(move.upper, level1["north"][x], level1["east"][x])
        values.append(jnp.where(bit0, coefficients, level1["right"][x]))
    masses = jnp.where(move.upper, level1["mass"][column + 1], level1["mass"][column])
    return values + [jnp.where(bit0, level1["east"][column - 1], masses)]


def middle_unpacked(move, level1, column, values, west):
    for x, value in zip((column, column + 1), values):
        level1["right"][x] = evens_of(move, value)
        both = odds_of(move, value)
        turned = other(both)
        level1["east"][x] = jnp.where(move.upper, turned, both)
        level1["north"][x] = jnp.where(move.upper, both, turned)
    both = evens_of(move, values[2])
    turned = other(both)
    level1["mass"][column] = jnp.where(move.upper, turned, both)
    level1["mass"][column + 1] = jnp.where(move.upper, both, turned)
    if west:
        level1["east"][column - 1] = odds_of(move, values[2])


def grouped(refs):
    levels = [dict(zip(STATE, refs[6 * n : 6 * n + 6])) for n in range(SPLIT)]
    levels.append(dict(zip(COARSE, refs[6 * SPLIT : 6 * SPLIT + 4])))
    return levels, refs[6 * SPLIT + 4]


KEPT = 6 * SPLIT + 5


def own_kernel(own_ref, swap_ref, folded_ref, wall_ref, cor_ref, *refs):
    tps = cor_ref.shape[0] // SEGS
    move = Shifts(tps)
    (top, level1, bottom), visc = grouped(refs)
    rot_ref, odd_ref, even_ref, ext_ref = refs[KEPT:]
    main = swap_ref.shape[0] - 8
    width = main // 4
    is_top = lax.axis_index("gy") == lax.axis_size("gy") - 1
    north = iota(swap_ref.shape, 1) < HALF
    swap = swap_ref[...]
    ext_ref[...] = jnp.where(
        north, jnp.where(is_top, folded_ref[...], swap), jnp.where(is_top, swap, wall_ref[...])
    )
    even = is_even()
    each = 2 * tps * 8
    side, total = FINE * each, width * each
    parts = (
        (slice(0, side), own_ref[0:side, :], own_ref[total - side : total, :]),
        (
            slice(side, side + 4 * FINE),
            ext_ref[0 : 4 * FINE, :],
            ext_ref[main - 4 * FINE : main, :],
        ),
    )
    for rows, low, high in parts:
        odd_ref[rows, :] = jnp.where(even, low, high)
        even_ref[rows, :] = jnp.where(even, high, low)
    rotations = move.rotations(cor_ref, ext_ref[main : main + 1, :])
    for level in range(LEVELS):
        rot_ref[level] = rotations[level]

    def own(first, group):
        for j in range(0, group, 2):
            x = first + j
            ext = ext_ref[pl.ds(pl.multiple_of(4 * x, 8), 8), :]
            for index in range(2):
                base = pl.multiple_of((x + index) * each, 8)
                unpack(
                    move, visc, top, lambda rows: own_ref[rows, :], base, ext, index, FINE + x + index
                )

    loop(0, width, own, width)
    loop(FINE, width - 1, lambda x, n: faces(visc, top["east"], x, n), 31)
    loop(FINE + 1, width - 2, lambda x, n: move.coefficients(top, x, n, 1), width - 2)
    skip, half, count = FINE - 2 * LEAD, width // 2, width >> SPLIT
    loop(LEAD, half - 1, lambda x, n: coarsen(move, top, level1, x, n, skip, 1), 15)
    coarsen(move, top, level1, LEAD + half - 1, 1, skip, 1, with_east=False)
    loop(
        LEAD + 1,
        half - 2,
        lambda x, n: move.restrict(top, level1, 2 * x + skip, x, n, rotations[0], 1),
        14,
    )
    move.coefficients(level1, LEAD + 1, half - 2, 2)
    skip = LEAD - 2 * count
    coarsen(move, level1, bottom, count, count - 1, skip, 2)
    coarsen(move, level1, bottom, 2 * count - 1, 1, skip, 2, with_east=False)
    move.restrict(level1, bottom, LEAD + 2, count + 1, count - 2, rotations[1], 2)

    def put(ref, column, value):
        for k in range(tps + 1):
            row = side + 4 * FINE + (column * (tps + 1) + k) * 8
            ref[row : row + 8, :] = value[:, k * LANES : (k + 1) * LANES]

    lows = middle_packed(move, level1, LEAD + 1)
    highs = middle_packed(move, level1, LEAD + half - 3)
    for n, (low, high) in enumerate(zip(lows, highs)):
        put(odd_ref, n, jnp.where(even, low, high))
        put(even_ref, n, jnp.where(even, high, low))
    for column in range(count - 1):

        def put_both(value, column=column):
            put(odd_ref, 3 + column, value)
            put(even_ref, 3 + column, value)

        put_packed(move, bottom, count + column, column == 0, put_both)


def ahead_columns(move, now, ahead, rotation, level, place, group, parity=None):
    step = 1 << level
    parity = place % 2 if parity is None else parity
    x0 = place + (FINE, LEAD - 1)[level]
    field = [now["field"][x0 + j - 1] for j in range(group + 2)]
    east = [now["east"][x0 + j - 1] for j in range(group + 1)]
    for j in range(group):
        x, at = x0 + j, place + j
        scale = now["scale"][x]
        north = now["north"][x]
        near = now["right"][x] + move.around(now, x, field[j : j + 3], east[j : j + 2], rotation, step)
        ahead["done"][at] = (1.0 - relax_weight) * field[j + 1] + scale * near
        inner, outer = east[j + 1], east[j]
        if (parity + j + level) % 2:
            inner, outer = outer, inner
        ahead["same"][at] = (1.0 - relax_weight) + scale * inner
        ahead["side"][at] = scale * outer
        ahead["up"][at] = scale * north
        ahead["down"][at] = scale * move.roll(north, step)
        ahead["turn"][at] = scale * rotation


def aheads_of(refs):
    return [dict(zip(AHEAD, refs[6 * n : 6 * n + 6])) for n in range(SPLIT)]


def ahead_kernel(rot_ref, *refs):
    levels = [dict(zip(FIRST, refs[5 * n : 5 * n + 5])) for n in range(SPLIT)]
    aheads = aheads_of(refs[5 * SPLIT :])
    move = Shifts(rot_ref.shape[2] // LANES - 1)
    width = aheads[0]["done"].shape[0]
    loop(
        2,
        width - 4,
        lambda x, n: ahead_columns(move, levels[0], aheads[0], rot_ref[0], 0, x, n, parity=0),
        14,
    )
    loop(
        3,
        width // 2 - 4,
        lambda x, n: ahead_columns(move, levels[1], aheads[1], rot_ref[1], 1, x, n, parity=1),
        6,
    )


SECOND = ("scale", "field")
THIRD = ("right", "east", "north", "mass", "scale", "field")


def second_kernel(odd_ref, even_ref, rot_ref, *refs):
    out_hbm = refs[KEPT + 12]
    refs = list(refs[KEPT + 13 :])
    levels, visc = grouped(refs)
    aheads = aheads_of(refs[KEPT:])
    rest = refs[KEPT + 12 :]
    flat, out_ref, sems = rest[:3]
    levels[SPLIT].update(zip(SECOND, rest[3:5]))
    rest = rest[5:]
    for _ in range(SPLIT + 1, LEVELS):
        levels.append(dict(zip(THIRD, rest[:6])))
        rest = rest[6:]
    done = rest
    width = out_ref.shape[1]
    tps = out_ref.shape[2] // LANES // SEGS
    tiles = tps * SEGS
    move = Shifts(tps)
    rotations = [rot_ref[level] for level in range(LEVELS)]
    each = 2 * tps * 8
    even = is_even()
    columns, count, half = visc.shape[0], width >> SPLIT, width // 2
    top, level1, now = levels[: SPLIT + 1]

    def from_left(rows):
        return jnp.where(even, odd_ref[rows, :], even_ref[rows, :])

    def from_right(rows):
        return jnp.where(even, even_ref[rows, :], odd_ref[rows, :])

    for load, start in ((from_left, 0), (from_right, FINE + width)):
        for j in range(0, FINE, 2):
            ext = load(pl.ds(FINE * each + 4 * j, 8))
            for index in range(2):
                unpack(move, visc, top, load, (j + index) * each, ext, index, start + j + index)

    def received(load, column):
        row = FINE * (each + 4) + column * (tps + 1) * 8
        return jnp.concatenate([load(pl.ds(row + 8 * k, 8)) for k in range(tps + 1)], 1)

    middle_unpacked(move, level1, 1, [received(from_left, n) for n in range(3)], True)
    middle_unpacked(
        move, level1, LEAD + half + 1, [received(from_right, n) for n in range(3)], False
    )
    for load, start, columns_sent in (
        (from_left, 0, range(count - 1)),
        (from_right, 2 * count, range(1, count - 1)),
    ):
        for column in columns_sent:
            for name, part in from_packed(move, received(load, 3 + column)):
                now[name][start + column] = part
    for start in (0, columns - 1 - FINE):
        faces(visc, top["east"], start, FINE)
    for start in (1, columns - 1 - FINE):
        move.coefficients(top, start, FINE, 1)
    skip = FINE - 2 * LEAD
    for column in (LEAD - 1, LEAD + half):
        coarsen(move, top, level1, column, 1, skip, 1)
    coarsen(move, top, level1, LEAD + half - 1, 1, skip, 1, with_sums=False)
    for column in (LEAD - 1, LEAD + half - 1):
        move.restrict(top, level1, 2 * column + skip, column, 2, rotations[0], 1)
    for column in (1, LEAD + half - 1):
        move.coefficients(level1, column, 4, 2)
    skip = LEAD - 2 * count
    for column in (count - 1, 2 * count):
        coarsen(move, level1, now, column, 1, skip, 2)
    coarsen(move, level1, now, 2 * count - 1, 1, skip, 2, with_sums=False)
    for column in (count - 1, 2 * count - 1):
        move.restrict(level1, now, 2 * column + skip, column, 2, rotations[1], 2)
    for place in (0, width - 2):
        ahead_columns(move, top, aheads[0], rotations[0], 0, place, 2)
    for place in (0, width // 2 - 1):
        ahead_columns(move, level1, aheads[1], rotations[1], 1, place, 3)
    total = 3 * count
    move.coefficients(now, 1, total - 2, 1 << SPLIT)
    for level in range(SPLIT, LEVELS - 1):
        now, coarse = levels[level], levels[level + 1]
        step = 1 << level
        half = total // 2
        for k in range(half - 1):
            coarse["east"][k] = 0.25 * move.pair(now["east"][2 * k + 1], step)
        for k in range(1, half - 1):
            move.coarse_sums(now, coarse, 2 * k, k, step)
        move.restrict(now, coarse, 2, 1, half - 2, rotations[level], step)
        total = half
        move.coefficients(coarse, 1, total - 2, 2 * step)

    def keep(target):
        def put(x, value):
            target[x] = value

        return put

    level = LEVELS - 1
    last, solved = levels[level], done.pop(0)
    own = width >> level
    move.sweep(
        last, own - 2, own + 4, lambda x: last["field"][x], rotations[level], 1 << level, keep(solved)
    )
    move.sweep(
        last, own - 1, own + 2, lambda x: solved[x], rotations[level], 1 << level, keep(last["field"])
    )
    solved, before = last["field"], own
    for level in reversed(range(SPLIT, LEVELS - 1)):
        now = levels[level]
        own = width >> level

        def value(x, now=now, solved=solved):
            return now["field"][x] + solved[lax.div(x, 2)]

        target = done.pop(0)
        move.sweep(now, own - 1, own + 2, value, rotations[level], 1 << level, keep(target))
        solved, before = target, own

    def correct(ahead, solved, first, count, place, step, put):
        for j in range(count):
            middle = solved[first + j]
            moved = (move.roll(middle, -step), move.roll(middle, step), other(middle))
            for child in range(2):
                x = place + 2 * j + child
                if isinstance(x, int) and not 0 <= x < ahead["done"].shape[0]:
                    continue
                result = (
                    ahead["done"][x]
                    + ahead["same"][x] * middle
                    + ahead["side"][x] * solved[first + j + 2 * child - 1]
                    + ahead["up"][x] * moved[0]
                    + ahead["down"][x] * moved[1]
                    + ahead["turn"][x] * moved[2]
                )
                put(x, result)

    target = done.pop(0)
    correct(aheads[1], solved, before - 1, (width >> SPLIT) + 2, -1, 2, keep(target))

    def put(x, result):
        for k in range(tps):
            row = pl.multiple_of((x * tps + k) * 8, 8)
            flat[pl.ds(row, 8), :] = result[:, k * LANES : (k + 1) * LANES]

    copies = []
    for i in range(width // 8):
        correct(aheads[0], target, 4 * i + 1, 4, 8 * i, 1, put)
        rows = pl.ds(8 * i, 8)
        for c in range(2):
            for t in range(tiles):
                s, k = divmod(t, tps)
                row = (8 * i * tps + k) * 8 + c * SEGS + s
                out_ref[c, rows, t * LANES : (t + 1) * LANES] = flat[pl.ds(row, 8, stride=tps * 8), :]
        copies.append(pltpu.make_async_copy(out_ref.at[:, rows, :], out_hbm.at[:, rows, :], sems.at[i]))
        copies[-1].start()
    for copy in copies:
        copy.wait()


def local(forcing, viscosity, mass, coriolis, land, ice_tiles):
    width, height = viscosity.shape
    tiles = height // LANES
    tps = tiles // SEGS
    each = 2 * tps * 8
    outside = 4 * width + 8
    gx, gy = lax.axis_size("gx"), lax.axis_size("gy")
    lines = coriolis.reshape(tiles, LANES)

    def here(*shape):
        return pltpu.VMEM(shape, f32)

    def call(kernel, outs, args, scratch=(), space=pltpu.VMEM, out_spaces=None, aliases={}):
        return pl.pallas_call(
            kernel,
            out_shape=outs,
            in_specs=[pl.BlockSpec(memory_space=space)] * len(args),
            out_specs=jax.tree.map(
                lambda _, where: pl.BlockSpec(memory_space=where),
                outs,
                out_spaces or jax.tree.map(lambda _: pltpu.VMEM, outs),
            ),
            scratch_shapes=scratch,
            input_output_aliases=aliases,
            compiler_params=pltpu.CompilerParams(vmem_limit_bytes=24 * 1024 * 1024),
        )(*(pltpu.with_memory_space_constraint(arg, space) for arg in args))

    sources = (ice_tiles.T, forcing, viscosity, mass, land, lines)
    edge, mirror, wall, *fields, lines, ice = call(
        prepare_kernel,
        (here(outside, LANES),) * 3
        + tuple(pltpu.VMEM(source.shape, source.dtype) for source in sources[1:])
        + (here(8 * tiles, LANES),),
        sources,
        scratch=[
            pltpu.SMEM(sources[0].shape, sources[0].dtype),
            pltpu.SemaphoreType.DMA((len(sources),)),
        ],
        space=pltpu.HBM,
    )
    top = gy - 1
    folded = lax.ppermute(
        mirror, ("gx", "gy"), [(i * gy + top, (gx - 1 - i) * gy + top) for i in range(gx)]
    )
    swap = lax.ppermute(edge, "gy", [(i, gy - 1 - i) for i in range(gy)])
    packed = call(pack_kernel, here(width * each, LANES), (*fields, ice))
    odd_pairs = [(i, (i + (1 if i % 2 else gx - 1)) % gx) for i in range(gx)]
    even_pairs = [(i, i ^ 1) for i in range(gx)]
    span = (tps + 1) * LANES
    columns = [2 * FINE + width, 2 * LEAD + width // 2]
    columns += [3 * width >> level for level in range(SPLIT, LEVELS)]
    count = width >> SPLIT

    def lines_of(number):
        return here(number, 8, span)

    kept = tuple(lines_of(columns[level]) for level in range(SPLIT) for _ in STATE)
    kept += (lines_of(columns[SPLIT]),) * len(COARSE) + (lines_of(columns[0]),)
    message = here(FINE * (each + 4) + (count + 2) * (tps + 1) * 8, LANES)
    *state, rotation, odd, even = call(
        own_kernel,
        kept + (lines_of(LEVELS), message, message),
        (packed, swap, folded, wall, lines),
        scratch=[here(outside, LANES)],
    )
    by_odd = lax.ppermute(odd, "gx", odd_pairs)
    by_even = lax.ppermute(even, "gx", even_pairs)
    ahead_shapes = (lines_of(width),) * len(AHEAD) + (lines_of(width // 2 + 2),) * len(AHEAD)
    ahead = call(
        ahead_kernel,
        ahead_shapes,
        (rotation, *(state[len(STATE) * level + n] for level in range(SPLIT) for n in range(len(FIRST)))),
    )
    out = jax.ShapeDtypeStruct((2, width, height), f32)
    return call(
        second_kernel,
        (out,) + kept + ahead_shapes,
        (by_odd, by_even, rotation, *state, *ahead),
        scratch=[
            pltpu.VMEM((width * tps * 8, LANES), f32),
            pltpu.VMEM((2, width, height), f32),
            pltpu.SemaphoreType.DMA((width // 8,)),
        ]
        + [lines_of(columns[SPLIT]) for _ in SECOND]
        + [lines_of(columns[level]) for level in range(SPLIT + 1, LEVELS) for _ in THIRD]
        + [lines_of(columns[level]) for level in reversed(range(SPLIT, LEVELS))]
        + [lines_of(width // 2 + 2)],
        out_spaces=(pltpu.HBM,) + (pltpu.VMEM,) * (KEPT + 12),
        aliases={3 + n: 1 + n for n in range(KEPT + 12)},
    )[0]


def solution(mesh):
    return jax.shard_map(
        local,
        mesh=mesh,
        in_specs=(
            P(None, ("groups", "gx"), "gy"),
            P(("groups", "gx"), "gy"),
            P(("groups", "gx"), "gy"),
            P("gy"),
            P("gx", "gy"),
            P("groups", None),
        ),
        out_specs=P(None, ("groups", "gx"), "gy"),
        check_vma=False,
    )
```

```python
import jax
import jax.numpy as jnp
from jax import lax
from jax.experimental import pallas as pl
from jax.experimental.pallas import tpu as pltpu
from jax.sharding import PartitionSpec as P


TILE = 128
LEVELS = 4
LANES = 128
SEGS = 4
HALF = LANES // 2
GROUP = 8

relax_weight = 0.8
land_mass = 4.0
f32 = jnp.float32
exact = lax.Precision.HIGHEST


FINE = 4
LEAD = 4
SPLIT = 2


def iota(shape, axis):
    return lax.broadcasted_iota(jnp.int32, shape, axis)


def is_even():
    return lax.axis_index("gx") & 1 == 0


def masked(ice, visc, mass, land, forcing):
    land = land.astype(f32)
    ocean = 1.0 - land
    return (
        visc * ice * ocean,
        mass * ocean + land_mass * land,
        forcing[0] * ocean,
        forcing[1] * ocean,
    )


def fetch(sources, held, sems):
    copies = [pltpu.make_async_copy(a, b, sems.at[n]) for n, (a, b) in enumerate(zip(sources, held))]
    for copy in copies:
        copy.start()
    return copies


def prepare_kernel(*refs):
    held = (refs[15],) + refs[9:14]
    copies = fetch(refs[:6], held, refs[16])
    edge_ref, mirror_ref, wall_ref, ice_ref = refs[6:9] + refs[14:15]
    forcing_ref, visc_ref, mass_ref, land_ref, cor_ref = refs[9:14]
    ice_place = refs[15]
    width = visc_ref.shape[0]
    tiles = visc_ref.shape[1] // LANES
    tile_x = lax.axis_index("gx") * width // TILE
    tile_y = lax.axis_index("gy") * tiles
    lane = iota((8, LANES), 1)
    main = 4 * width
    flip = (iota((LANES, LANES), 0) + iota((LANES, LANES), 1) == LANES - 1).astype(f32)
    row, col = iota((main, main), 0), iota((main, main), 1)
    sign = jnp.where(row & 2 == 0, 1.0, -1.0)
    turn = jnp.where((row & 3 == col & 3) & ((row >> 2) + (col >> 2) == width - 1), sign, 0.0)
    wall_ref[main : main + 8, :] = jnp.zeros((8, LANES), f32)
    for copy in copies:
        copy.wait()
    for t in range(tiles):
        ice_ref[8 * t : 8 * t + 8, :] = jnp.full((8, LANES), ice_place[tile_y + t, tile_x].astype(f32), f32)
    for i in range(width // 8):
        rows = slice(8 * i, 8 * i + 8)
        ends = []
        for t in (0, tiles - 1):
            cols = slice(t * LANES, (t + 1) * LANES)
            ends.append(
                masked(
                    ice_place[tile_y + t, tile_x].astype(f32),
                    visc_ref[rows, cols],
                    mass_ref[rows, cols],
                    land_ref[rows, cols],
                    [forcing_ref[c, rows, cols] for c in range(2)],
                )
            )
        for a in range(4):
            start = 8 * i * 4 + a
            edge_ref[pl.ds(start, 8, stride=4), :] = jnp.where(lane < HALF, ends[0][a], ends[1][a])
            if a == 0:
                wall = jnp.broadcast_to(ends[0][0][:, :1], (8, LANES))
            else:
                wall = jnp.full((8, LANES), 1.0 if a == 1 else 0.0, f32)
            wall_ref[pl.ds(start, 8, stride=4), :] = wall
    first, last = cor_ref[0:1, :], cor_ref[tiles - 1 : tiles, :]
    edge_ref[main : main + 8, :] = jnp.broadcast_to(
        jnp.where(lane[:1] < HALF, first, last), (8, LANES)
    )
    turned = jnp.dot(turn, edge_ref[0:main, :], precision=exact, preferred_element_type=f32)
    mirror_ref[0:main, :] = jnp.dot(turned, flip, precision=exact, preferred_element_type=f32)
    mirror_ref[main : main + 8, :] = jnp.dot(
        edge_ref[main : main + 8, :], flip, precision=exact, preferred_element_type=f32
    )


def pack_kernel(forcing_ref, visc_ref, mass_ref, land_ref, ice_ref, packed_ref):
    width = visc_ref.shape[0]
    tiles = visc_ref.shape[1] // LANES
    tps = tiles // SEGS
    for i in range(width // 8):
        rows = slice(8 * i, 8 * i + 8)
        for t in range(tiles):
            s, k = divmod(t, tps)
            cols = slice(t * LANES, (t + 1) * LANES)
            values = masked(
                ice_ref[8 * t : 8 * t + 8, :],
                visc_ref[rows, cols],
                mass_ref[rows, cols],
                land_ref[rows, cols],
                [forcing_ref[c, rows, cols] for c in range(2)],
            )
            for a, value in enumerate(values):
                tile = 8 * i * 2 * tps + (a // 2) * tps + k
                start = tile * 8 + (a % 2) * SEGS + s
                packed_ref[pl.ds(start, 8, stride=2 * tps * 8), :] = value


class Shifts:
    def __init__(self, tps):
        self.tps = tps
        self.span = (tps + 1) * LANES
        self.shape = (8, self.span)
        self.lane = iota(self.shape, 1)
        self.upper = iota(self.shape, 0) >= SEGS
        lane = self.lane1 = iota((8, LANES), 1)
        row = iota((8, LANES), 0) & (SEGS - 1)
        self.first_half = lane < HALF
        self.low = iota((8, LANES), 0) < SEGS
        self.outer = ((row == SEGS - 1) & (lane < HALF)) | ((row == 0) & (lane >= HALF))
        bottom = lax.axis_index("gy") == 0
        wall = (iota(self.shape, 0) & (SEGS - 1) == 0) & (self.lane >= tps * LANES + HALF) & bottom
        self.weight = jnp.where(wall, 0.0, relax_weight)

    def roll(self, value, shift):
        return pltpu.roll(value, shift % self.span, 1)

    def odd(self, step):
        return self.lane & step != 0

    def take(self, value, index):
        tiles = [value[:, k * LANES : (k + 1) * LANES] for k in range(self.tps + 1)]
        return jnp.concatenate([jnp.take_along_axis(tile, index, axis=1) for tile in tiles], 1)

    def pair(self, value, step):
        return value + self.take(value, self.lane1 ^ step)

    def with_halo(self, parts, outside):
        inside = jnp.where(self.first_half, pltpu.roll(parts[0], 7, 0), pltpu.roll(parts[-1], 1, 0))
        return parts + [jnp.where(self.outer, outside, inside)]

    def rotations(self, cor_ref, line):
        parts = [cor_ref[pl.ds(k, SEGS, stride=self.tps), :] for k in range(self.tps)]
        parts = [jnp.concatenate([part, -part], 0) for part in parts]
        line = jnp.broadcast_to(line, (8, LANES))
        rotation = jnp.concatenate(self.with_halo(parts, jnp.where(self.low, line, -line)), 1)
        result = []
        for level in range(LEVELS):
            result.append(rotation)
            rotation = 0.5 * self.pair(rotation, 1 << level)
        return result

    def around(self, now, x, field, east, rotation, step):
        north = now["north"][x]
        west_nb, w, east_nb = field
        return (
            east[1] * east_nb
            + east[0] * west_nb
            + north * self.roll(w, -step)
            + self.roll(north * w, step)
            + rotation * other(w)
        )

    def coefficients(self, now, first, group, step):
        east = [now["east"][first + j - 1] for j in range(group + 1)]

        def known(j):
            x = first + j
            north = now["north"][x]
            return north, now["mass"][x] + east[j + 1] + east[j] + north

        for j in range(0, group, 2):
            north, rest = known(j)
            if j + 1 < group:
                north2, rest2 = known(j + 1)
                north, rest = jnp.where(self.upper, north2, north), jnp.where(self.upper, rest2, rest)
            scale = self.weight / (rest + self.roll(north, step))
            scales = (scale,)
            if j + 1 < group:
                turned = other(scale)
                scales = (jnp.where(self.upper, turned, scale), jnp.where(self.upper, scale, turned))
            for k, scale in enumerate(scales):
                x = first + j + k
                now["scale"][x] = scale
                now["field"][x] = scale * now["right"][x]

    def restrict(self, now, coarse, fine, place, group, rotation, step):
        field = [now["field"][fine + j - 1] for j in range(2 * group + 2)]
        east = [now["east"][fine + j - 1] for j in range(2 * group + 1)]
        rest = [
            (1.0 - relax_weight) * now["right"][fine + j]
            + self.around(now, fine + j, field[j : j + 3], east[j : j + 2], rotation, step)
            for j in range(2 * group)
        ]
        for j in range(group):
            coarse["right"][place + j] = 0.25 * self.pair(rest[2 * j] + rest[2 * j + 1], step)

    def sweep(self, now, first, group, value, rotation, step, put):
        field = [value(first + j - 1) for j in range(group + 2)]
        east = [now["east"][first + j - 1] for j in range(group + 1)]
        for j in range(group):
            x = first + j
            near = now["right"][x] + self.around(
                now, x, field[j : j + 3], east[j : j + 2], rotation, step
            )
            put(x, (1.0 - relax_weight) * field[j + 1] + now["scale"][x] * near)


def other(value):
    return pltpu.roll(value, SEGS, 0)


def loop(start, count, body, group=GROUP):
    whole, rest = divmod(count, group)
    if whole == 1:
        body(start, group)
    elif whole:
        lax.fori_loop(0, whole, lambda g, c: (body(start + g * group, group), c)[1], 0)
    if rest:
        body(start + whole * group, rest)


FIRST = ("north", "east", "scale", "right", "field")
STATE = FIRST + ("mass",)
COARSE = ("right", "east", "north", "mass")
AHEAD = ("done", "same", "side", "up", "down", "turn")


def faces(visc, east, first, group):
    value = [visc[first + j] for j in range(group + 1)]
    for j in range(group):
        east[first + j] = 0.5 * (value[j] + value[j + 1])


def unpack(move, visc, top, load, base, ext, index, x):
    tps = move.tps
    rows = [jnp.broadcast_to(ext[4 * index + a : 4 * index + a + 1], (8, LANES)) for a in range(4)]
    both = move.with_halo(
        [load(pl.ds(base + 8 * k, 8)) for k in range(tps)], jnp.where(move.low, rows[0], rows[1])
    )
    turned = [other(part) for part in both]
    value = jnp.concatenate([jnp.where(move.low, a, b) for a, b in zip(both, turned)], 1)
    visc[x] = value
    top["mass"][x] = jnp.concatenate([jnp.where(move.low, b, a) for a, b in zip(both, turned)], 1)
    top["right"][x] = jnp.concatenate(
        move.with_halo(
            [load(pl.ds(base + 8 * (tps + k), 8)) for k in range(tps)],
            jnp.where(move.low, rows[2], rows[3]),
        ),
        1,
    )
    top["north"][x] = 0.5 * (value + move.roll(value, -1))


def coarsen(move, now, coarse, first, group, skip, step, with_east=True, with_sums=True):
    def norths(j):
        x = 2 * (first + j) + skip
        return now["north"][x] + now["north"][x + 1]

    for j in range(group):
        x = 2 * (first + j) + skip
        east = now["east"][x + 1] if with_east else None
        mass = now["mass"][x] + now["mass"][x + 1] if with_sums else None
        if with_east and with_sums:
            both = 0.25 * move.pair(jnp.where(move.upper, mass, east), step)
            turned = other(both)
            coarse["east"][first + j] = jnp.where(move.upper, turned, both)
            coarse["mass"][first + j] = jnp.where(move.upper, both, turned)
        elif with_east:
            coarse["east"][first + j] = 0.25 * move.pair(east, step)
        else:
            coarse["mass"][first + j] = 0.25 * move.pair(mass, step)
        if with_sums and j % 2 == 0:
            if j + 1 < group:
                both = jnp.where(move.upper, norths(j + 1), norths(j))
                both = 0.25 * move.take(both, move.lane1 | step)
                turned = other(both)
                coarse["north"][first + j] = jnp.where(move.upper, turned, both)
                coarse["north"][first + j + 1] = jnp.where(move.upper, both, turned)
            else:
                coarse["north"][first + j] = 0.25 * move.take(norths(j), move.lane1 | step)


def evens_of(move, value):
    return move.take(value, move.lane1 & ~1)


def odds_of(move, value):
    return move.take(value, move.lane1 | 1)


def coarse_packed(move, bottom, base, count):
    bit0, bit1 = move.odd(1), move.odd(2)
    values = []
    for n in range(count // 2):
        first, second = base + 2 * n, base + min(2 * n + 1, count - 2)
        east, north, mass = (
            jnp.where(move.upper, bottom[name][second], bottom[name][first]) for name in COARSE[1:]
        )
        right = bottom["right"][base + n + 1]
        values.append(jnp.where(bit1, jnp.where(bit0, mass, north), jnp.where(bit0, east, right)))
    rights = [bottom["right"][base + count // 2 + 1 + n] for n in range(2)]
    return values + [jnp.where(bit0, rights[1], rights[0])]


def coarse_unpacked(move, bottom, base, count, load, first_too):
    for n in range(count // 2):
        value = load(n)
        bottom["right"][base + n + 1] = move.take(value, move.lane1 & ~3)
        for place, name in enumerate(COARSE[1:]):
            part = move.take(value, (move.lane1 & ~3) | (place + 1))
            turned = other(part)
            if n or first_too:
                bottom[name][base + 2 * n] = jnp.where(move.upper, turned, part)
            if 2 * n + 1 < count - 1:
                bottom[name][base + 2 * n + 1] = jnp.where(move.upper, part, turned)
    value = load(count // 2)
    bottom["right"][base + count // 2 + 1] = evens_of(move, value)
    bottom["right"][base + count // 2 + 2] = odds_of(move, value)


def middle_packed(move, level1, column):
    bit0 = move.odd(1)
    values = []
    for x in (column, column + 1):
        coefficients = jnp.where(move.upper, level1["north"][x], level1["east"][x])
        values.append(jnp.where(bit0, coefficients, level1["right"][x]))
    masses = jnp.where(move.upper, level1["mass"][column + 1], level1["mass"][column])
    return values + [jnp.where(bit0, level1["east"][column - 1], masses)]


def middle_unpacked(move, level1, column, values, west):
    for x, value in zip((column, column + 1), values):
        level1["right"][x] = evens_of(move, value)
        both = odds_of(move, value)
        turned = other(both)
        level1["east"][x] = jnp.where(move.upper, turned, both)
        level1["north"][x] = jnp.where(move.upper, both, turned)
    both = evens_of(move, values[2])
    turned = other(both)
    level1["mass"][column] = jnp.where(move.upper, turned, both)
    level1["mass"][column + 1] = jnp.where(move.upper, both, turned)
    if west:
        level1["east"][column - 1] = odds_of(move, values[2])


def grouped(refs):
    levels = [dict(zip(STATE, refs[6 * n : 6 * n + 6])) for n in range(SPLIT)]
    levels.append(dict(zip(COARSE, refs[6 * SPLIT : 6 * SPLIT + 4])))
    return levels, refs[6 * SPLIT + 4]


KEPT = 6 * SPLIT + 5


def own_kernel(own_ref, swap_ref, folded_ref, wall_ref, cor_ref, *refs):
    tps = cor_ref.shape[0] // SEGS
    move = Shifts(tps)
    (top, level1, bottom), visc = grouped(refs)
    rot_ref, odd_ref, even_ref, ext_ref = refs[KEPT:]
    main = swap_ref.shape[0] - 8
    width = main // 4
    is_top = lax.axis_index("gy") == lax.axis_size("gy") - 1
    north = iota(swap_ref.shape, 1) < HALF
    swap = swap_ref[...]
    ext_ref[...] = jnp.where(
        north, jnp.where(is_top, folded_ref[...], swap), jnp.where(is_top, swap, wall_ref[...])
    )
    even = is_even()
    each = 2 * tps * 8
    side, total = FINE * each, width * each
    parts = (
        (slice(0, side), own_ref[0:side, :], own_ref[total - side : total, :]),
        (
            slice(side, side + 4 * FINE),
            ext_ref[0 : 4 * FINE, :],
            ext_ref[main - 4 * FINE : main, :],
        ),
    )
    for rows, low, high in parts:
        odd_ref[rows, :] = jnp.where(even, low, high)
        even_ref[rows, :] = jnp.where(even, high, low)
    rotations = move.rotations(cor_ref, ext_ref[main : main + 1, :])
    for level in range(LEVELS):
        rot_ref[level] = rotations[level]

    def own(first, group):
        for j in range(0, group, 2):
            x = first + j
            ext = ext_ref[pl.ds(pl.multiple_of(4 * x, 8), 8), :]
            for index in range(2):
                base = pl.multiple_of((x + index) * each, 8)
                unpack(
                    move, visc, top, lambda rows: own_ref[rows, :], base, ext, index, FINE + x + index
                )

    loop(0, width, own, width)
    loop(FINE, width - 1, lambda x, n: faces(visc, top["east"], x, n), 31)
    loop(FINE + 1, width - 2, lambda x, n: move.coefficients(top, x, n, 1), width - 2)
    skip, half, count = FINE - 2 * LEAD, width // 2, width >> SPLIT
    loop(LEAD, half - 1, lambda x, n: coarsen(move, top, level1, x, n, skip, 1), 15)
    coarsen(move, top, level1, LEAD + half - 1, 1, skip, 1, with_east=False)
    loop(
        LEAD + 1,
        half - 2,
        lambda x, n: move.restrict(top, level1, 2 * x + skip, x, n, rotations[0], 1),
        14,
    )
    move.coefficients(level1, LEAD + 1, half - 2, 2)
    skip = LEAD - 2 * count
    coarsen(move, level1, bottom, count, count - 1, skip, 2)
    coarsen(move, level1, bottom, 2 * count - 1, 1, skip, 2, with_east=False)
    move.restrict(level1, bottom, LEAD + 2, count + 1, count - 2, rotations[1], 2)

    def put(ref, column, value):
        for k in range(tps + 1):
            row = side + 4 * FINE + (column * (tps + 1) + k) * 8
            ref[row : row + 8, :] = value[:, k * LANES : (k + 1) * LANES]

    lows = middle_packed(move, level1, LEAD + 1)
    highs = middle_packed(move, level1, LEAD + half - 3)
    for n, (low, high) in enumerate(zip(lows, highs)):
        put(odd_ref, n, jnp.where(even, low, high))
        put(even_ref, n, jnp.where(even, high, low))
    for n, value in enumerate(coarse_packed(move, bottom, count, count)):
        put(odd_ref, 3 + n, value)
        put(even_ref, 3 + n, value)


def ahead_columns(move, now, ahead, rotation, level, place, group, parity=None):
    step = 1 << level
    parity = place % 2 if parity is None else parity
    x0 = place + (FINE, LEAD - 1)[level]
    field = [now["field"][x0 + j - 1] for j in range(group + 2)]
    east = [now["east"][x0 + j - 1] for j in range(group + 1)]
    for j in range(group):
        x, at = x0 + j, place + j
        scale = now["scale"][x]
        north = now["north"][x]
        near = now["right"][x] + move.around(now, x, field[j : j + 3], east[j : j + 2], rotation, step)
        ahead["done"][at] = (1.0 - relax_weight) * field[j + 1] + scale * near
        inner, outer = east[j + 1], east[j]
        if (parity + j + level) % 2:
            inner, outer = outer, inner
        ahead["same"][at] = (1.0 - relax_weight) + scale * inner
        ahead["side"][at] = scale * outer
        ahead["up"][at] = scale * north
        ahead["down"][at] = scale * move.roll(north, step)
        ahead["turn"][at] = scale * rotation


def aheads_of(refs):
    return [dict(zip(AHEAD, refs[6 * n : 6 * n + 6])) for n in range(SPLIT)]


def ahead_kernel(rot_ref, *refs):
    levels = [dict(zip(FIRST, refs[5 * n : 5 * n + 5])) for n in range(SPLIT)]
    aheads = aheads_of(refs[5 * SPLIT :])
    move = Shifts(rot_ref.shape[2] // LANES - 1)
    width = aheads[0]["done"].shape[0]
    loop(
        2,
        width - 4,
        lambda x, n: ahead_columns(move, levels[0], aheads[0], rot_ref[0], 0, x, n, parity=0),
        14,
    )
    loop(
        3,
        width // 2 - 4,
        lambda x, n: ahead_columns(move, levels[1], aheads[1], rot_ref[1], 1, x, n, parity=1),
        6,
    )


SECOND = ("scale", "field")
THIRD = ("right", "east", "north", "mass", "scale", "field")


def second_kernel(odd_ref, even_ref, rot_ref, *refs):
    out_hbm = refs[KEPT + 12]
    refs = list(refs[KEPT + 13 :])
    levels, visc = grouped(refs)
    aheads = aheads_of(refs[KEPT:])
    rest = refs[KEPT + 12 :]
    flat, out_ref, sems = rest[:3]
    levels[SPLIT].update(zip(SECOND, rest[3:5]))
    rest = rest[5:]
    for _ in range(SPLIT + 1, LEVELS):
        levels.append(dict(zip(THIRD, rest[:6])))
        rest = rest[6:]
    done = rest
    width = out_ref.shape[1]
    tps = out_ref.shape[2] // LANES // SEGS
    tiles = tps * SEGS
    move = Shifts(tps)
    rotations = [rot_ref[level] for level in range(LEVELS)]
    each = 2 * tps * 8
    even = is_even()
    columns, count, half = visc.shape[0], width >> SPLIT, width // 2
    top, level1, now = levels[: SPLIT + 1]

    def from_left(rows):
        return jnp.where(even, odd_ref[rows, :], even_ref[rows, :])

    def from_right(rows):
        return jnp.where(even, even_ref[rows, :], odd_ref[rows, :])

    for load, start in ((from_left, 0), (from_right, FINE + width)):
        for j in range(0, FINE, 2):
            ext = load(pl.ds(FINE * each + 4 * j, 8))
            for index in range(2):
                unpack(move, visc, top, load, (j + index) * each, ext, index, start + j + index)

    def received(load, column):
        row = FINE * (each + 4) + column * (tps + 1) * 8
        return jnp.concatenate([load(pl.ds(row + 8 * k, 8)) for k in range(tps + 1)], 1)

    middle_unpacked(move, level1, 1, [received(from_left, n) for n in range(3)], True)
    middle_unpacked(
        move, level1, LEAD + half + 1, [received(from_right, n) for n in range(3)], False
    )
    for load, start in ((from_left, 0), (from_right, 2 * count)):
        coarse_unpacked(
            move, now, start, count, lambda n, load=load: received(load, 3 + n), start == 0
        )
    for start in (0, columns - 1 - FINE):
        faces(visc, top["east"], start, FINE)
    for start in (1, columns - 1 - FINE):
        move.coefficients(top, start, FINE, 1)
    skip = FINE - 2 * LEAD
    for column in (LEAD - 1, LEAD + half):
        coarsen(move, top, level1, column, 1, skip, 1)
    coarsen(move, top, level1, LEAD + half - 1, 1, skip, 1, with_sums=False)
    for column in (LEAD - 1, LEAD + half - 1):
        move.restrict(top, level1, 2 * column + skip, column, 2, rotations[0], 1)
    for column in (1, LEAD + half - 1):
        move.coefficients(level1, column, 4, 2)
    skip = LEAD - 2 * count
    for column in (count - 1, 2 * count):
        coarsen(move, level1, now, column, 1, skip, 2)
    coarsen(move, level1, now, 2 * count - 1, 1, skip, 2, with_sums=False)
    for column in (count - 1, 2 * count - 1):
        move.restrict(level1, now, 2 * column + skip, column, 2, rotations[1], 2)
    for place in (0, width - 2):
        ahead_columns(move, top, aheads[0], rotations[0], 0, place, 2)
    for place in (0, width // 2 - 1):
        ahead_columns(move, level1, aheads[1], rotations[1], 1, place, 3)
    total = 3 * count
    move.coefficients(now, 1, total - 2, 1 << SPLIT)
    for level in range(SPLIT, LEVELS - 1):
        now, coarse = levels[level], levels[level + 1]
        step = 1 << level
        half = total // 2
        coarsen(move, now, coarse, 0, 1, 0, step, with_sums=False)
        coarsen(move, now, coarse, 1, half - 2, 0, step)
        move.restrict(now, coarse, 2, 1, half - 2, rotations[level], step)
        total = half
        move.coefficients(coarse, 1, total - 2, 2 * step)

    def keep(target):
        def put(x, value):
            target[x] = value

        return put

    level = LEVELS - 1
    last, solved = levels[level], done.pop(0)
    own = width >> level
    move.sweep(
        last, own - 2, own + 4, lambda x: last["field"][x], rotations[level], 1 << level, keep(solved)
    )
    move.sweep(
        last, own - 1, own + 2, lambda x: solved[x], rotations[level], 1 << level, keep(last["field"])
    )
    solved, before = last["field"], own
    for level in reversed(range(SPLIT, LEVELS - 1)):
        now = levels[level]
        own = width >> level

        def value(x, now=now, solved=solved):
            return now["field"][x] + solved[lax.div(x, 2)]

        target = done.pop(0)
        move.sweep(now, own - 1, own + 2, value, rotations[level], 1 << level, keep(target))
        solved, before = target, own

    def correct(ahead, solved, first, count, place, step, put):
        for j in range(count):
            middle = solved[first + j]
            moved = (move.roll(middle, -step), move.roll(middle, step), other(middle))
            for child in range(2):
                x = place + 2 * j + child
                if isinstance(x, int) and not 0 <= x < ahead["done"].shape[0]:
                    continue
                result = (
                    ahead["done"][x]
                    + ahead["same"][x] * middle
                    + ahead["side"][x] * solved[first + j + 2 * child - 1]
                    + ahead["up"][x] * moved[0]
                    + ahead["down"][x] * moved[1]
                    + ahead["turn"][x] * moved[2]
                )
                put(x, result)

    target = done.pop(0)
    correct(aheads[1], solved, before - 1, (width >> SPLIT) + 2, -1, 2, keep(target))

    def put(x, result):
        for k in range(tps):
            row = pl.multiple_of((x * tps + k) * 8, 8)
            flat[pl.ds(row, 8), :] = result[:, k * LANES : (k + 1) * LANES]

    copies = []
    for i in range(width // 8):
        correct(aheads[0], target, 4 * i + 1, 4, 8 * i, 1, put)
        rows = pl.ds(8 * i, 8)
        for c in range(2):
            for t in range(tiles):
                s, k = divmod(t, tps)
                row = (8 * i * tps + k) * 8 + c * SEGS + s
                out_ref[c, rows, t * LANES : (t + 1) * LANES] = flat[pl.ds(row, 8, stride=tps * 8), :]
        copies.append(pltpu.make_async_copy(out_ref.at[:, rows, :], out_hbm.at[:, rows, :], sems.at[i]))
        copies[-1].start()
    for copy in copies:
        copy.wait()


def local(forcing, viscosity, mass, coriolis, land, ice_tiles):
    width, height = viscosity.shape
    tiles = height // LANES
    tps = tiles // SEGS
    each = 2 * tps * 8
    outside = 4 * width + 8
    gx, gy = lax.axis_size("gx"), lax.axis_size("gy")
    lines = coriolis.reshape(tiles, LANES)

    def here(*shape):
        return pltpu.VMEM(shape, f32)

    def call(kernel, outs, args, scratch=(), space=pltpu.VMEM, out_spaces=None, aliases={}):
        return pl.pallas_call(
            kernel,
            out_shape=outs,
            in_specs=[pl.BlockSpec(memory_space=space)] * len(args),
            out_specs=jax.tree.map(
                lambda _, where: pl.BlockSpec(memory_space=where),
                outs,
                out_spaces or jax.tree.map(lambda _: pltpu.VMEM, outs),
            ),
            scratch_shapes=scratch,
            input_output_aliases=aliases,
            compiler_params=pltpu.CompilerParams(vmem_limit_bytes=24 * 1024 * 1024),
        )(*(pltpu.with_memory_space_constraint(arg, space) for arg in args))

    sources = (ice_tiles.T, forcing, viscosity, mass, land, lines)
    edge, mirror, wall, *fields, lines, ice = call(
        prepare_kernel,
        (here(outside, LANES),) * 3
        + tuple(pltpu.VMEM(source.shape, source.dtype) for source in sources[1:])
        + (here(8 * tiles, LANES),),
        sources,
        scratch=[
            pltpu.SMEM(sources[0].shape, sources[0].dtype),
            pltpu.SemaphoreType.DMA((len(sources),)),
        ],
        space=pltpu.HBM,
    )
    top = gy - 1
    folded = lax.ppermute(
        mirror, ("gx", "gy"), [(i * gy + top, (gx - 1 - i) * gy + top) for i in range(gx)]
    )
    swap = lax.ppermute(edge, "gy", [(i, gy - 1 - i) for i in range(gy)])
    packed = call(pack_kernel, here(width * each, LANES), (*fields, ice))
    odd_pairs = [(i, (i + (1 if i % 2 else gx - 1)) % gx) for i in range(gx)]
    even_pairs = [(i, i ^ 1) for i in range(gx)]
    span = (tps + 1) * LANES
    columns = [2 * FINE + width, 2 * LEAD + width // 2]
    columns += [3 * width >> level for level in range(SPLIT, LEVELS)]
    count = width >> SPLIT

    def lines_of(number):
        return here(number, 8, span)

    kept = tuple(lines_of(columns[level]) for level in range(SPLIT) for _ in STATE)
    kept += (lines_of(columns[SPLIT]),) * len(COARSE) + (lines_of(columns[0]),)
    message = here(FINE * (each + 4) + (count // 2 + 4) * (tps + 1) * 8, LANES)
    *state, rotation, odd, even = call(
        own_kernel,
        kept + (lines_of(LEVELS), message, message),
        (packed, swap, folded, wall, lines),
        scratch=[here(outside, LANES)],
    )
    by_odd = lax.ppermute(odd, "gx", odd_pairs)
    by_even = lax.ppermute(even, "gx", even_pairs)
    ahead_shapes = (lines_of(width),) * len(AHEAD) + (lines_of(width // 2 + 2),) * len(AHEAD)
    ahead = call(
        ahead_kernel,
        ahead_shapes,
        (rotation, *(state[len(STATE) * level + n] for level in range(SPLIT) for n in range(len(FIRST)))),
    )
    out = jax.ShapeDtypeStruct((2, width, height), f32)
    return call(
        second_kernel,
        (out,) + kept + ahead_shapes,
        (by_odd, by_even, rotation, *state, *ahead),
        scratch=[
            pltpu.VMEM((width * tps * 8, LANES), f32),
            pltpu.VMEM((2, width, height), f32),
            pltpu.SemaphoreType.DMA((width // 8,)),
        ]
        + [lines_of(columns[SPLIT]) for _ in SECOND]
        + [lines_of(columns[level]) for level in range(SPLIT + 1, LEVELS) for _ in THIRD]
        + [lines_of(columns[level]) for level in reversed(range(SPLIT, LEVELS))]
        + [lines_of(width // 2 + 2)],
        out_spaces=(pltpu.HBM,) + (pltpu.VMEM,) * (KEPT + 12),
        aliases={3 + n: 1 + n for n in range(KEPT + 12)},
    )[0]


def solution(mesh):
    return jax.shard_map(
        local,
        mesh=mesh,
        in_specs=(
            P(None, ("groups", "gx"), "gy"),
            P(("groups", "gx"), "gy"),
            P(("groups", "gx"), "gy"),
            P("gy"),
            P("gx", "gy"),
            P("groups", None),
        ),
        out_specs=P(None, ("groups", "gx"), "gy"),
        check_vma=False,
    )
```

```python
import jax
import jax.numpy as jnp
from jax import lax
from jax.experimental import pallas as pl
from jax.experimental.pallas import tpu as pltpu
from jax.sharding import PartitionSpec as P


TILE = 128
LEVELS = 4
LANES = 128
SEGS = 4
HALF = LANES // 2
GROUP = 8

relax_weight = 0.8
land_mass = 4.0
f32 = jnp.float32
exact = lax.Precision.HIGHEST


FINE = 4
LEAD = 4
SPLIT = 2


def iota(shape, axis):
    return lax.broadcasted_iota(jnp.int32, shape, axis)


def is_even():
    return lax.axis_index("gx") & 1 == 0


def masked(ice, visc, mass, land, forcing):
    land = land.astype(f32)
    ocean = 1.0 - land
    return (
        visc * ice * ocean,
        mass * ocean + land_mass * land,
        forcing[0] * ocean,
        forcing[1] * ocean,
    )


def fetch(sources, held, sems):
    copies = [pltpu.make_async_copy(a, b, sems.at[n]) for n, (a, b) in enumerate(zip(sources, held))]
    for copy in copies:
        copy.start()
    return copies


def prepare_kernel(*refs):
    hbm, sems = refs[:6], refs[20]
    edge_ref, mirror_ref, wall_ref, ice_ref = refs[6:9] + refs[14:15]
    _, visc_ref, _, _, cor_ref = refs[9:14]
    ice_place, forcing_end, visc_end, mass_end, land_end = refs[15:20]
    last_tile = visc_ref.shape[1] - LANES
    sources, held = [hbm[0], hbm[5]], [ice_place, cor_ref]
    for n in range(2):
        cols = pl.ds(n * last_tile, LANES)
        sources += [hbm[1].at[:, :, cols]] + [ref.at[:, cols] for ref in hbm[2:5]]
        held += [ref.at[n] for ref in (forcing_end, visc_end, mass_end, land_end)]
    copies = fetch(sources, held, sems)
    bulk = [
        pltpu.make_async_copy(a, b, sems.at[len(copies) + n])
        for n, (a, b) in enumerate(zip(hbm[1:5], refs[9:13]))
    ]
    for copy in bulk:
        copy.start()
    width = visc_ref.shape[0]
    tiles = visc_ref.shape[1] // LANES
    tile_x = lax.axis_index("gx") * width // TILE
    tile_y = lax.axis_index("gy") * tiles
    lane = iota((8, LANES), 1)
    main = 4 * width
    flip = (iota((LANES, LANES), 0) + iota((LANES, LANES), 1) == LANES - 1).astype(f32)
    row, col = iota((main, main), 0), iota((main, main), 1)
    sign = jnp.where(row & 2 == 0, 1.0, -1.0)
    turn = jnp.where((row & 3 == col & 3) & ((row >> 2) + (col >> 2) == width - 1), sign, 0.0)
    wall_ref[main : main + 8, :] = jnp.zeros((8, LANES), f32)
    for copy in copies:
        copy.wait()
    for t in range(tiles):
        ice_ref[8 * t : 8 * t + 8, :] = jnp.full((8, LANES), ice_place[tile_y + t, tile_x].astype(f32), f32)
    for i in range(width // 8):
        rows = slice(8 * i, 8 * i + 8)
        ends = []
        for n, t in enumerate((0, tiles - 1)):
            ends.append(
                masked(
                    ice_place[tile_y + t, tile_x].astype(f32),
                    visc_end[n, rows, :],
                    mass_end[n, rows, :],
                    land_end[n, rows, :],
                    [forcing_end[n, c, rows, :] for c in range(2)],
                )
            )
        for a in range(4):
            start = 8 * i * 4 + a
            edge_ref[pl.ds(start, 8, stride=4), :] = jnp.where(lane < HALF, ends[0][a], ends[1][a])
            if a == 0:
                wall = jnp.broadcast_to(ends[0][0][:, :1], (8, LANES))
            else:
                wall = jnp.full((8, LANES), 1.0 if a == 1 else 0.0, f32)
            wall_ref[pl.ds(start, 8, stride=4), :] = wall
    first, last = cor_ref[0:1, :], cor_ref[tiles - 1 : tiles, :]
    edge_ref[main : main + 8, :] = jnp.broadcast_to(
        jnp.where(lane[:1] < HALF, first, last), (8, LANES)
    )
    turned = jnp.dot(turn, edge_ref[0:main, :], precision=exact, preferred_element_type=f32)
    mirror_ref[0:main, :] = jnp.dot(turned, flip, precision=exact, preferred_element_type=f32)
    mirror_ref[main : main + 8, :] = jnp.dot(
        edge_ref[main : main + 8, :], flip, precision=exact, preferred_element_type=f32
    )
    for copy in bulk:
        copy.wait()


def pack_kernel(forcing_ref, visc_ref, mass_ref, land_ref, ice_ref, packed_ref):
    width = visc_ref.shape[0]
    tiles = visc_ref.shape[1] // LANES
    tps = tiles // SEGS
    for i in range(width // 8):
        rows = slice(8 * i, 8 * i + 8)
        for t in range(tiles):
            s, k = divmod(t, tps)
            cols = slice(t * LANES, (t + 1) * LANES)
            values = masked(
                ice_ref[8 * t : 8 * t + 8, :],
                visc_ref[rows, cols],
                mass_ref[rows, cols],
                land_ref[rows, cols],
                [forcing_ref[c, rows, cols] for c in range(2)],
            )
            for a, value in enumerate(values):
                tile = 8 * i * 2 * tps + (a // 2) * tps + k
                start = tile * 8 + (a % 2) * SEGS + s
                packed_ref[pl.ds(start, 8, stride=2 * tps * 8), :] = value


class Shifts:
    def __init__(self, tps):
        self.tps = tps
        self.span = (tps + 1) * LANES
        self.shape = (8, self.span)
        self.lane = iota(self.shape, 1)
        self.upper = iota(self.shape, 0) >= SEGS
        lane = self.lane1 = iota((8, LANES), 1)
        row = iota((8, LANES), 0) & (SEGS - 1)
        self.first_half = lane < HALF
        self.low = iota((8, LANES), 0) < SEGS
        self.outer = ((row == SEGS - 1) & (lane < HALF)) | ((row == 0) & (lane >= HALF))
        bottom = lax.axis_index("gy") == 0
        wall = (iota(self.shape, 0) & (SEGS - 1) == 0) & (self.lane >= tps * LANES + HALF) & bottom
        self.weight = jnp.where(wall, 0.0, relax_weight)

    def roll(self, value, shift):
        return pltpu.roll(value, shift % self.span, 1)

    def odd(self, step):
        return self.lane & step != 0

    def take(self, value, index):
        tiles = [value[:, k * LANES : (k + 1) * LANES] for k in range(self.tps + 1)]
        return jnp.concatenate([jnp.take_along_axis(tile, index, axis=1) for tile in tiles], 1)

    def pair(self, value, step):
        return value + self.take(value, self.lane1 ^ step)

    def with_halo(self, parts, outside):
        inside = jnp.where(self.first_half, pltpu.roll(parts[0], 7, 0), pltpu.roll(parts[-1], 1, 0))
        return parts + [jnp.where(self.outer, outside, inside)]

    def rotations(self, cor_ref, line):
        parts = [cor_ref[pl.ds(k, SEGS, stride=self.tps), :] for k in range(self.tps)]
        parts = [jnp.concatenate([part, -part], 0) for part in parts]
        line = jnp.broadcast_to(line, (8, LANES))
        rotation = jnp.concatenate(self.with_halo(parts, jnp.where(self.low, line, -line)), 1)
        result = []
        for level in range(LEVELS):
            result.append(rotation)
            rotation = 0.5 * self.pair(rotation, 1 << level)
        return result

    def around(self, now, x, field, east, rotation, step):
        north = now["north"][x]
        west_nb, w, east_nb = field
        return (
            east[1] * east_nb
            + east[0] * west_nb
            + north * self.roll(w, -step)
            + self.roll(north * w, step)
            + rotation * other(w)
        )

    def coefficients(self, now, first, group, step):
        east = [now["east"][first + j - 1] for j in range(group + 1)]

        def known(j):
            x = first + j
            north = now["north"][x]
            return north, now["mass"][x] + east[j + 1] + east[j] + north

        for j in range(0, group, 2):
            north, rest = known(j)
            if j + 1 < group:
                north2, rest2 = known(j + 1)
                north, rest = jnp.where(self.upper, north2, north), jnp.where(self.upper, rest2, rest)
            scale = self.weight / (rest + self.roll(north, step))
            scales = (scale,)
            if j + 1 < group:
                turned = other(scale)
                scales = (jnp.where(self.upper, turned, scale), jnp.where(self.upper, scale, turned))
            for k, scale in enumerate(scales):
                x = first + j + k
                now["scale"][x] = scale
                now["field"][x] = scale * now["right"][x]

    def restrict(self, now, coarse, fine, place, group, rotation, step):
        field = [now["field"][fine + j - 1] for j in range(2 * group + 2)]
        east = [now["east"][fine + j - 1] for j in range(2 * group + 1)]
        rest = [
            (1.0 - relax_weight) * now["right"][fine + j]
            + self.around(now, fine + j, field[j : j + 3], east[j : j + 2], rotation, step)
            for j in range(2 * group)
        ]
        for j in range(group):
            coarse["right"][place + j] = 0.25 * self.pair(rest[2 * j] + rest[2 * j + 1], step)

    def sweep(self, now, first, group, value, rotation, step, put):
        field = [value(first + j - 1) for j in range(group + 2)]
        east = [now["east"][first + j - 1] for j in range(group + 1)]
        for j in range(group):
            x = first + j
            near = now["right"][x] + self.around(
                now, x, field[j : j + 3], east[j : j + 2], rotation, step
            )
            put(x, (1.0 - relax_weight) * field[j + 1] + now["scale"][x] * near)


def other(value):
    return pltpu.roll(value, SEGS, 0)


def loop(start, count, body, group=GROUP):
    whole, rest = divmod(count, group)
    if whole == 1:
        body(start, group)
    elif whole:
        lax.fori_loop(0, whole, lambda g, c: (body(start + g * group, group), c)[1], 0)
    if rest:
        body(start + whole * group, rest)


FIRST = ("north", "east", "scale", "right", "field")
STATE = FIRST + ("mass",)
COARSE = ("right", "east", "north", "mass")
AHEAD = ("done", "same", "side", "up", "down", "turn")


def faces(visc, east, first, group):
    value = [visc[first + j] for j in range(group + 1)]
    for j in range(group):
        east[first + j] = 0.5 * (value[j] + value[j + 1])


def unpack(move, visc, top, load, bases, ext, x, with_right=(True, True)):
    tps = move.tps
    for index, base in enumerate(bases):
        rows = [jnp.broadcast_to(ext[4 * index + a : 4 * index + a + 1], (8, LANES)) for a in range(4)]
        both = move.with_halo(
            [load(pl.ds(base + 8 * k, 8)) for k in range(tps)], jnp.where(move.low, rows[0], rows[1])
        )
        turned = [other(part) for part in both]
        value = jnp.concatenate([jnp.where(move.low, a, b) for a, b in zip(both, turned)], 1)
        visc[x + index] = value
        top["north"][x + index] = 0.5 * (value + move.roll(value, -1))
        top["mass"][x + index] = jnp.concatenate(
            [jnp.where(move.low, b, a) for a, b in zip(both, turned)], 1
        )
        if with_right[index]:
            top["right"][x + index] = jnp.concatenate(
                move.with_halo(
                    [load(pl.ds(base + 8 * (tps + k), 8)) for k in range(tps)],
                    jnp.where(move.low, rows[2], rows[3]),
                ),
                1,
            )


def fine_rows(tps):
    return (FINE - 1) * 2 * tps * 8 + tps * 8


def coarsen(move, now, coarse, first, group, skip, step, with_east=True, with_sums=True):
    def norths(j):
        x = 2 * (first + j) + skip
        return now["north"][x] + now["north"][x + 1]

    for j in range(group):
        x = 2 * (first + j) + skip
        east = now["east"][x + 1] if with_east else None
        mass = now["mass"][x] + now["mass"][x + 1] if with_sums else None
        if with_east and with_sums:
            both = 0.25 * move.pair(jnp.where(move.upper, mass, east), step)
            turned = other(both)
            coarse["east"][first + j] = jnp.where(move.upper, turned, both)
            coarse["mass"][first + j] = jnp.where(move.upper, both, turned)
        elif with_east:
            coarse["east"][first + j] = 0.25 * move.pair(east, step)
        else:
            coarse["mass"][first + j] = 0.25 * move.pair(mass, step)
        if with_sums and j % 2 == 0:
            if j + 1 < group:
                both = jnp.where(move.upper, norths(j + 1), norths(j))
                both = 0.25 * move.take(both, move.lane1 | step)
                turned = other(both)
                coarse["north"][first + j] = jnp.where(move.upper, turned, both)
                coarse["north"][first + j + 1] = jnp.where(move.upper, both, turned)
            else:
                coarse["north"][first + j] = 0.25 * move.take(norths(j), move.lane1 | step)


def evens_of(move, value):
    return move.take(value, move.lane1 & ~1)


def odds_of(move, value):
    return move.take(value, move.lane1 | 1)


def coarse_packed(move, bottom, base, count):
    bit0, bit1 = move.odd(1), move.odd(2)
    values = []
    for n in range(count // 2):
        first, second = base + 2 * n, base + min(2 * n + 1, count - 2)
        east, north, mass = (
            jnp.where(move.upper, bottom[name][second], bottom[name][first]) for name in COARSE[1:]
        )
        right = bottom["right"][base + n + 1]
        values.append(jnp.where(bit1, jnp.where(bit0, mass, north), jnp.where(bit0, east, right)))
    rights = [bottom["right"][base + count // 2 + 1 + n] for n in range(2)]
    return values + [jnp.where(bit0, rights[1], rights[0])]


def coarse_unpacked(move, bottom, base, count, load, first_too):
    for n in range(count // 2):
        value = load(n)
        bottom["right"][base + n + 1] = move.take(value, move.lane1 & ~3)
        for place, name in enumerate(COARSE[1:]):
            part = move.take(value, (move.lane1 & ~3) | (place + 1))
            turned = other(part)
            if n or first_too:
                bottom[name][base + 2 * n] = jnp.where(move.upper, turned, part)
            if 2 * n + 1 < count - 1:
                bottom[name][base + 2 * n + 1] = jnp.where(move.upper, part, turned)
    value = load(count // 2)
    bottom["right"][base + count // 2 + 1] = evens_of(move, value)
    bottom["right"][base + count // 2 + 2] = odds_of(move, value)


def middle_packed(move, level1, column):
    bit0 = move.odd(1)
    values = []
    for x in (column, column + 1):
        coefficients = jnp.where(move.upper, level1["north"][x], level1["east"][x])
        values.append(jnp.where(bit0, coefficients, level1["right"][x]))
    masses = jnp.where(move.upper, level1["mass"][column + 1], level1["mass"][column])
    return values + [jnp.where(bit0, level1["east"][column - 1], masses)]


def middle_unpacked(move, level1, column, values, west):
    for x, value in zip((column, column + 1), values):
        level1["right"][x] = evens_of(move, value)
        both = odds_of(move, value)
        turned = other(both)
        level1["east"][x] = jnp.where(move.upper, turned, both)
        level1["north"][x] = jnp.where(move.upper, both, turned)
    both = evens_of(move, values[2])
    turned = other(both)
    level1["mass"][column] = jnp.where(move.upper, turned, both)
    level1["mass"][column + 1] = jnp.where(move.upper, both, turned)
    if west:
        level1["east"][column - 1] = odds_of(move, values[2])


def grouped(refs):
    levels = [dict(zip(STATE, refs[6 * n : 6 * n + 6])) for n in range(SPLIT)]
    levels.append(dict(zip(COARSE, refs[6 * SPLIT : 6 * SPLIT + 4])))
    return levels, refs[6 * SPLIT + 4]


KEPT = 6 * SPLIT + 5


def own_kernel(own_ref, swap_ref, folded_ref, wall_ref, cor_ref, *refs):
    tps = cor_ref.shape[0] // SEGS
    move = Shifts(tps)
    (top, level1, bottom), visc = grouped(refs)
    rot_ref, odd_ref, even_ref, ext_ref = refs[KEPT:]
    main = swap_ref.shape[0] - 8
    width = main // 4
    is_top = lax.axis_index("gy") == lax.axis_size("gy") - 1
    north = iota(swap_ref.shape, 1) < HALF
    swap = swap_ref[...]
    ext_ref[...] = jnp.where(
        north, jnp.where(is_top, folded_ref[...], swap), jnp.where(is_top, swap, wall_ref[...])
    )
    even = is_even()
    each = 2 * tps * 8
    side = fine_rows(tps)
    parts = [
        (slice(side, side + 4 * FINE), ext_ref[0 : 4 * FINE, :], ext_ref[main - 4 * FINE : main, :])
    ]
    for q in range(FINE):
        size = each if q < FINE - 1 else tps * 8
        start = (width - 1 - q) * each
        parts.append(
            (
                slice(q * each, q * each + size),
                own_ref[q * each : q * each + size, :],
                own_ref[start : start + size, :],
            )
        )
    for rows, low, high in parts:
        odd_ref[rows, :] = jnp.where(even, low, high)
        even_ref[rows, :] = jnp.where(even, high, low)
    rotations = move.rotations(cor_ref, ext_ref[main : main + 1, :])
    for level in range(LEVELS):
        rot_ref[level] = rotations[level]

    def own(first, group):
        for j in range(0, group, 2):
            x = first + j
            ext = ext_ref[pl.ds(pl.multiple_of(4 * x, 8), 8), :]
            bases = [pl.multiple_of((x + index) * each, 8) for index in range(2)]
            unpack(move, visc, top, lambda rows: own_ref[rows, :], bases, ext, FINE + x)

    loop(0, width, own, width)
    loop(FINE, width - 1, lambda x, n: faces(visc, top["east"], x, n), 31)
    loop(FINE + 1, width - 2, lambda x, n: move.coefficients(top, x, n, 1), width - 2)
    skip, half, count = FINE - 2 * LEAD, width // 2, width >> SPLIT
    loop(LEAD, half - 1, lambda x, n: coarsen(move, top, level1, x, n, skip, 1), 15)
    coarsen(move, top, level1, LEAD + half - 1, 1, skip, 1, with_east=False)
    loop(
        LEAD + 1,
        half - 2,
        lambda x, n: move.restrict(top, level1, 2 * x + skip, x, n, rotations[0], 1),
        14,
    )
    move.coefficients(level1, LEAD + 1, half - 2, 2)
    skip = LEAD - 2 * count
    coarsen(move, level1, bottom, count, count - 1, skip, 2)
    coarsen(move, level1, bottom, 2 * count - 1, 1, skip, 2, with_east=False)
    move.restrict(level1, bottom, LEAD + 2, count + 1, count - 2, rotations[1], 2)

    def put(ref, column, value):
        for k in range(tps + 1):
            row = side + 4 * FINE + (column * (tps + 1) + k) * 8
            ref[row : row + 8, :] = value[:, k * LANES : (k + 1) * LANES]

    lows = middle_packed(move, level1, LEAD + 1)
    highs = middle_packed(move, level1, LEAD + half - 3)
    for n, (low, high) in enumerate(zip(lows, highs)):
        put(odd_ref, n, jnp.where(even, low, high))
        put(even_ref, n, jnp.where(even, high, low))
    for n, value in enumerate(coarse_packed(move, bottom, count, count)):
        put(odd_ref, 3 + n, value)
        put(even_ref, 3 + n, value)


def ahead_columns(move, now, ahead, rotation, level, place, group, parity=None):
    step = 1 << level
    parity = place % 2 if parity is None else parity
    x0 = place + (FINE, LEAD - 1)[level]
    field = [now["field"][x0 + j - 1] for j in range(group + 2)]
    east = [now["east"][x0 + j - 1] for j in range(group + 1)]
    for j in range(group):
        x, at = x0 + j, place + j
        scale = now["scale"][x]
        north = now["north"][x]
        near = now["right"][x] + move.around(now, x, field[j : j + 3], east[j : j + 2], rotation, step)
        ahead["done"][at] = (1.0 - relax_weight) * field[j + 1] + scale * near
        inner, outer = east[j + 1], east[j]
        if (parity + j + level) % 2:
            inner, outer = outer, inner
        ahead["same"][at] = (1.0 - relax_weight) + scale * inner
        ahead["side"][at] = scale * outer
        ahead["up"][at] = scale * north
        ahead["down"][at] = scale * move.roll(north, step)
        ahead["turn"][at] = scale * rotation


def aheads_of(refs):
    return [dict(zip(AHEAD, refs[6 * n : 6 * n + 6])) for n in range(SPLIT)]


def ahead_kernel(rot_ref, *refs):
    levels = [dict(zip(FIRST, refs[5 * n : 5 * n + 5])) for n in range(SPLIT)]
    aheads = aheads_of(refs[5 * SPLIT :])
    move = Shifts(rot_ref.shape[2] // LANES - 1)
    width = aheads[0]["done"].shape[0]
    loop(
        2,
        width - 4,
        lambda x, n: ahead_columns(move, levels[0], aheads[0], rot_ref[0], 0, x, n, parity=0),
        14,
    )
    loop(
        3,
        width // 2 - 4,
        lambda x, n: ahead_columns(move, levels[1], aheads[1], rot_ref[1], 1, x, n, parity=1),
        6,
    )


SECOND = ("scale", "field")
THIRD = ("right", "east", "north", "mass", "scale", "field")


def second_kernel(odd_ref, even_ref, rot_ref, *refs):
    out_hbm = refs[KEPT + 12]
    refs = list(refs[KEPT + 13 :])
    levels, visc = grouped(refs)
    aheads = aheads_of(refs[KEPT:])
    rest = refs[KEPT + 12 :]
    flat, out_ref, sems = rest[:3]
    levels[SPLIT].update(zip(SECOND, rest[3:5]))
    rest = rest[5:]
    for _ in range(SPLIT + 1, LEVELS):
        levels.append(dict(zip(THIRD, rest[:6])))
        rest = rest[6:]
    done = rest
    width = out_ref.shape[1]
    tps = out_ref.shape[2] // LANES // SEGS
    tiles = tps * SEGS
    move = Shifts(tps)
    rotations = [rot_ref[level] for level in range(LEVELS)]
    each = 2 * tps * 8
    even = is_even()
    columns, count, half = visc.shape[0], width >> SPLIT, width // 2
    top, level1, now = levels[: SPLIT + 1]

    def from_left(rows):
        return jnp.where(even, odd_ref[rows, :], even_ref[rows, :])

    def from_right(rows):
        return jnp.where(even, even_ref[rows, :], odd_ref[rows, :])

    side = fine_rows(tps)
    for load, start in ((from_left, 0), (from_right, FINE + width)):
        for j in range(0, FINE, 2):
            ext = load(pl.ds(side + 4 * j, 8))
            places = [j + index if start else FINE - 1 - j - index for index in range(2)]
            unpack(
                move,
                visc,
                top,
                load,
                [place * each for place in places],
                ext,
                start + j,
                [place < FINE - 1 for place in places],
            )

    def received(load, column):
        row = side + 4 * FINE + column * (tps + 1) * 8
        return jnp.concatenate([load(pl.ds(row + 8 * k, 8)) for k in range(tps + 1)], 1)

    middle_unpacked(move, level1, 1, [received(from_left, n) for n in range(3)], True)
    middle_unpacked(
        move, level1, LEAD + half + 1, [received(from_right, n) for n in range(3)], False
    )
    for load, start in ((from_left, 0), (from_right, 2 * count)):
        coarse_unpacked(
            move, now, start, count, lambda n, load=load: received(load, 3 + n), start == 0
        )
    for start in (0, columns - 1 - FINE):
        faces(visc, top["east"], start, FINE)
    for start in (1, columns - 1 - FINE):
        move.coefficients(top, start, FINE, 1)
    skip = FINE - 2 * LEAD
    for column in (LEAD - 1, LEAD + half):
        coarsen(move, top, level1, column, 1, skip, 1)
    coarsen(move, top, level1, LEAD + half - 1, 1, skip, 1, with_sums=False)
    for column in (LEAD - 1, LEAD + half - 1):
        move.restrict(top, level1, 2 * column + skip, column, 2, rotations[0], 1)
    for column in (1, LEAD + half - 1):
        move.coefficients(level1, column, 4, 2)
    skip = LEAD - 2 * count
    for column in (count - 1, 2 * count):
        coarsen(move, level1, now, column, 1, skip, 2)
    coarsen(move, level1, now, 2 * count - 1, 1, skip, 2, with_sums=False)
    for column in (count - 1, 2 * count - 1):
        move.restrict(level1, now, 2 * column + skip, column, 2, rotations[1], 2)
    for place in (0, width - 2):
        ahead_columns(move, top, aheads[0], rotations[0], 0, place, 2)
    for place in (0, width // 2 - 1):
        ahead_columns(move, level1, aheads[1], rotations[1], 1, place, 3)
    total = 3 * count
    move.coefficients(now, 1, total - 2, 1 << SPLIT)
    for level in range(SPLIT, LEVELS - 1):
        now, coarse = levels[level], levels[level + 1]
        step = 1 << level
        half = total // 2
        coarsen(move, now, coarse, 0, 1, 0, step, with_sums=False)
        coarsen(move, now, coarse, 1, half - 2, 0, step)
        move.restrict(now, coarse, 2, 1, half - 2, rotations[level], step)
        total = half
        move.coefficients(coarse, 1, total - 2, 2 * step)

    def keep(target):
        def put(x, value):
            target[x] = value

        return put

    level = LEVELS - 1
    last, solved = levels[level], done.pop(0)
    own = width >> level
    move.sweep(
        last, own - 2, own + 4, lambda x: last["field"][x], rotations[level], 1 << level, keep(solved)
    )
    move.sweep(
        last, own - 1, own + 2, lambda x: solved[x], rotations[level], 1 << level, keep(last["field"])
    )
    solved, before = last["field"], own
    for level in reversed(range(SPLIT, LEVELS - 1)):
        now = levels[level]
        own = width >> level

        def value(x, now=now, solved=solved):
            return now["field"][x] + solved[lax.div(x, 2)]

        target = done.pop(0)
        move.sweep(now, own - 1, own + 2, value, rotations[level], 1 << level, keep(target))
        solved, before = target, own

    def correct(ahead, solved, first, count, place, step, put):
        for j in range(count):
            middle = solved[first + j]
            moved = (move.roll(middle, -step), move.roll(middle, step), other(middle))
            for child in range(2):
                x = place + 2 * j + child
                if isinstance(x, int) and not 0 <= x < ahead["done"].shape[0]:
                    continue
                result = (
                    ahead["done"][x]
                    + ahead["same"][x] * middle
                    + ahead["side"][x] * solved[first + j + 2 * child - 1]
                    + ahead["up"][x] * moved[0]
                    + ahead["down"][x] * moved[1]
                    + ahead["turn"][x] * moved[2]
                )
                put(x, result)

    target = done.pop(0)
    correct(aheads[1], solved, before - 1, (width >> SPLIT) + 2, -1, 2, keep(target))

    def put(x, result):
        for k in range(tps):
            row = pl.multiple_of((x * tps + k) * 8, 8)
            flat[pl.ds(row, 8), :] = result[:, k * LANES : (k + 1) * LANES]

    copies = []
    for i in range(width // 8):
        correct(aheads[0], target, 4 * i + 1, 4, 8 * i, 1, put)
        rows = pl.ds(8 * i, 8)
        for c in range(2):
            for t in range(tiles):
                s, k = divmod(t, tps)
                row = (8 * i * tps + k) * 8 + c * SEGS + s
                out_ref[c, rows, t * LANES : (t + 1) * LANES] = flat[pl.ds(row, 8, stride=tps * 8), :]
        copies.append(pltpu.make_async_copy(out_ref.at[:, rows, :], out_hbm.at[:, rows, :], sems.at[i]))
        copies[-1].start()
    for copy in copies:
        copy.wait()


def local(forcing, viscosity, mass, coriolis, land, ice_tiles):
    width, height = viscosity.shape
    tiles = height // LANES
    tps = tiles // SEGS
    each = 2 * tps * 8
    outside = 4 * width + 8
    gx, gy = lax.axis_size("gx"), lax.axis_size("gy")
    lines = coriolis.reshape(tiles, LANES)

    def here(*shape):
        return pltpu.VMEM(shape, f32)

    def call(kernel, outs, args, scratch=(), space=pltpu.VMEM, out_spaces=None, aliases={}):
        return pl.pallas_call(
            kernel,
            out_shape=outs,
            in_specs=[pl.BlockSpec(memory_space=space)] * len(args),
            out_specs=jax.tree.map(
                lambda _, where: pl.BlockSpec(memory_space=where),
                outs,
                out_spaces or jax.tree.map(lambda _: pltpu.VMEM, outs),
            ),
            scratch_shapes=scratch,
            input_output_aliases=aliases,
            compiler_params=pltpu.CompilerParams(vmem_limit_bytes=24 * 1024 * 1024),
        )(*(pltpu.with_memory_space_constraint(arg, space) for arg in args))

    sources = (ice_tiles.T, forcing, viscosity, mass, land, lines)
    edge, mirror, wall, *fields, lines, ice = call(
        prepare_kernel,
        (here(outside, LANES),) * 3
        + tuple(pltpu.VMEM(source.shape, source.dtype) for source in sources[1:])
        + (here(8 * tiles, LANES),),
        sources,
        scratch=[
            pltpu.SMEM(sources[0].shape, sources[0].dtype),
            pltpu.VMEM((2, 2, width, LANES), f32),
            *(pltpu.VMEM((2, width, LANES), source.dtype) for source in sources[2:5]),
            pltpu.SemaphoreType.DMA((14,)),
        ],
        space=pltpu.HBM,
    )
    top = gy - 1
    folded = lax.ppermute(
        mirror, ("gx", "gy"), [(i * gy + top, (gx - 1 - i) * gy + top) for i in range(gx)]
    )
    swap = lax.ppermute(edge, "gy", [(i, gy - 1 - i) for i in range(gy)])
    packed = call(pack_kernel, here(width * each, LANES), (*fields, ice))
    odd_pairs = [(i, (i + (1 if i % 2 else gx - 1)) % gx) for i in range(gx)]
    even_pairs = [(i, i ^ 1) for i in range(gx)]
    span = (tps + 1) * LANES
    columns = [2 * FINE + width, 2 * LEAD + width // 2]
    columns += [3 * width >> level for level in range(SPLIT, LEVELS)]
    count = width >> SPLIT

    def lines_of(number):
        return here(number, 8, span)

    kept = tuple(lines_of(columns[level]) for level in range(SPLIT) for _ in STATE)
    kept += (lines_of(columns[SPLIT]),) * len(COARSE) + (lines_of(columns[0]),)
    message = here(fine_rows(tps) + 4 * FINE + (count // 2 + 4) * (tps + 1) * 8, LANES)
    *state, rotation, odd, even = call(
        own_kernel,
        kept + (lines_of(LEVELS), message, message),
        (packed, swap, folded, wall, lines),
        scratch=[here(outside, LANES)],
    )
    by_odd = lax.ppermute(odd, "gx", odd_pairs)
    by_even = lax.ppermute(even, "gx", even_pairs)
    ahead_shapes = (lines_of(width),) * len(AHEAD) + (lines_of(width // 2 + 2),) * len(AHEAD)
    ahead = call(
        ahead_kernel,
        ahead_shapes,
        (rotation, *(state[len(STATE) * level + n] for level in range(SPLIT) for n in range(len(FIRST)))),
    )
    out = jax.ShapeDtypeStruct((2, width, height), f32)
    return call(
        second_kernel,
        (out,) + kept + ahead_shapes,
        (by_odd, by_even, rotation, *state, *ahead),
        scratch=[
            pltpu.VMEM((width * tps * 8, LANES), f32),
            pltpu.VMEM((2, width, height), f32),
            pltpu.SemaphoreType.DMA((width // 8,)),
        ]
        + [lines_of(columns[SPLIT]) for _ in SECOND]
        + [lines_of(columns[level]) for level in range(SPLIT + 1, LEVELS) for _ in THIRD]
        + [lines_of(columns[level]) for level in reversed(range(SPLIT, LEVELS))]
        + [lines_of(width // 2 + 2)],
        out_spaces=(pltpu.HBM,) + (pltpu.VMEM,) * (KEPT + 12),
        aliases={3 + n: 1 + n for n in range(KEPT + 12)},
    )[0]


def solution(mesh):
    return jax.shard_map(
        local,
        mesh=mesh,
        in_specs=(
            P(None, ("groups", "gx"), "gy"),
            P(("groups", "gx"), "gy"),
            P(("groups", "gx"), "gy"),
            P("gy"),
            P("gx", "gy"),
            P("groups", None),
        ),
        out_specs=P(None, ("groups", "gx"), "gy"),
        check_vma=False,
    )
```
